8 devices in a mesh: dp: 1 (over z), tp: 8 (over y, x, core).
Axes of the slice: x: 2, y: 2, z: 1, core: 2. Of those that a mesh axis runs over, the one named last changes fastest.
Arguments:
- x_in: bfloat16 [256, 4096], P('dp')
- tok_pos: int32 [256], P('dp')
- conv_state: bfloat16 [2, 256, 3, 5632], P(None, 'dp', None, 'tp')
- lru_state: float32 [2, 256, 5632], P(None, 'dp', 'tp')
- k_cache: bfloat16 [256, 1024, 128], P('dp')
- v_cache: bfloat16 [256, 1024, 128], P('dp')
- slot_pos: int32 [256, 1024], P('dp')
- norm_scale: bfloat16 [3, 2, 4096], replicated
- rec_wx: bfloat16 [2, 4096, 5632], P(None, None, 'tp')
- rec_bx: bfloat16 [2, 5632], P(None, 'tp')
- rec_wy: bfloat16 [2, 4096, 5632], P(None, None, 'tp')
- rec_by: bfloat16 [2, 5632], P(None, 'tp')
- conv_w: bfloat16 [2, 4, 5632], P(None, None, 'tp')
- conv_b: bfloat16 [2, 5632], P(None, 'tp')
- gate_wa: bfloat16 [2, 32, 176, 176], P(None, 'tp')
- gate_ba: bfloat16 [2, 5632], P(None, 'tp')
- gate_wi: bfloat16 [2, 32, 176, 176], P(None, 'tp')
- gate_bi: bfloat16 [2, 5632], P(None, 'tp')
- a_param: float32 [2, 5632], P(None, 'tp')
- rec_wout: bfloat16 [2, 5632, 4096], P(None, 'tp')
- rec_bout: bfloat16 [2, 4096], replicated
- attn_wq: bfloat16 [4096, 4096], P(None, 'tp')
- attn_wk: bfloat16 [4096, 128], replicated
- attn_wv: bfloat16 [4096, 128], replicated
- attn_wo: bfloat16 [4096, 4096], P('tp')
- attn_bo: bfloat16 [4096], replicated
- mlp_w1: bfloat16 [3, 4096, 12288], P(None, None, 'tp')
- mlp_b1: bfloat16 [3, 12288], P(None, 'tp')
- mlp_w2: bfloat16 [3, 4096, 12288], P(None, None, 'tp')
- mlp_b2: bfloat16 [3, 12288], P(None, 'tp')
- mlp_wd: bfloat16 [3, 12288, 4096], P(None, 'tp')
- mlp_bd: bfloat16 [3, 4096], replicated
Outputs:
- output 1: bfloat16 [256, 4096], P('dp')
- output 2: bfloat16 [2, 256, 3, 5632], P(None, 'dp', None, 'tp')
- output 3: float32 [2, 256, 5632], P(None, 'dp', 'tp')
- output 4: bfloat16 [256, 1024, 128], P('dp')
- output 5: bfloat16 [256, 1024, 128], P('dp')
- output 6: int32 [256, 1024], P('dp')
All inputs are finite; a program needn't handle non-finite values.
Results may differ from the reference program's by a relative error of at most 0.02.
Values are sent between devices in bfloat16 or wider.
A program may use at most 1.75 GiB of HBM per device.

```python
import jax
import jax.numpy as jnp
from jax import lax

D = 4096
L = 5632
H = 32
F = 12288
HEAD = 128
WINDOW = 1024
BATCH = 256

ROPE_BASE = 10000.0
NORM_EPS = 1e-6


def draw_positions(key):
    key_kind, key_low, key_mid, key_high, key_old = jax.random.split(key, 5)
    pos_kind = jax.random.permutation(key_kind, jnp.arange(BATCH, dtype=jnp.int32) % 4)
    pos_low = jax.random.randint(key_low, (BATCH,), 1, 8, dtype=jnp.int32)
    pos_mid = jax.random.randint(key_mid, (BATCH,), 8, WINDOW, dtype=jnp.int32)
    pos_high = jax.random.randint(key_high, (BATCH,), WINDOW, 4 * WINDOW, dtype=jnp.int32)
    tok_pos = jnp.where(pos_kind == 0, 0, jnp.where(pos_kind == 1, pos_low, jnp.where(pos_kind == 2, pos_mid, pos_high)))
    old_len = jax.random.randint(key_old, (BATCH,), 0, 4 * WINDOW, dtype=jnp.int32)
    written = jnp.where(tok_pos > 0, tok_pos, old_len)
    slot_ids = jnp.arange(WINDOW, dtype=jnp.int32)
    behind = written[:, None] - 1 - slot_ids[None, :]
    slot_pos = jnp.where(behind >= 0, slot_ids[None, :] + WINDOW * (behind // WINDOW), -1)
    return tok_pos.astype(jnp.int32), slot_pos.astype(jnp.int32)


def normal_draw(key, shape, scale):
    return (jax.random.normal(key, shape, jnp.float32) * scale).astype(jnp.bfloat16)


def setup_inputs(seed: int = 0, part: int = 0) -> dict:
    root_key = jax.random.key(seed)
    part_root, shared_root = jax.random.split(root_key)
    part_keys = jax.random.split(jax.random.fold_in(part_root, part), 8)
    weight_keys = jax.random.split(shared_root, 32)
    tok_pos, slot_pos = draw_positions(part_keys[0])
    v_mean = jax.random.normal(part_keys[6], (BATCH, 1, HEAD), jnp.float32)
    v_noise = jax.random.normal(part_keys[5], (BATCH, WINDOW, HEAD), jnp.float32)
    a_root = jax.random.uniform(weight_keys[11], (2, L), jnp.float32, 0.9, 0.999)
    a_soft = -jnp.log(a_root) / 8.0
    block_width = L // H
    return {
        'x_in': normal_draw(part_keys[1], (BATCH, D), 1.0),
        'tok_pos': tok_pos,
        'conv_state': normal_draw(part_keys[2], (2, BATCH, 3, L), 1.0),
        'lru_state': jax.random.normal(part_keys[3], (2, BATCH, L), jnp.float32) * 0.35,
        'k_cache': normal_draw(part_keys[4], (BATCH, WINDOW, HEAD), 1.0),
        'v_cache': (v_mean + v_noise).astype(jnp.bfloat16),
        'slot_pos': slot_pos,
        'norm_scale': normal_draw(weight_keys[0], (3, 2, D), 0.3),
        'rec_wx': normal_draw(weight_keys[1], (2, D, L), D ** -0.5),
        'rec_bx': normal_draw(weight_keys[2], (2, L), 0.3),
        'rec_wy': normal_draw(weight_keys[3], (2, D, L), D ** -0.5),
        'rec_by': normal_draw(weight_keys[4], (2, L), 0.3),
        'conv_w': normal_draw(weight_keys[5], (2, 4, L), 0.5),
        'conv_b': normal_draw(weight_keys[6], (2, L), 0.3),
        'gate_wa': normal_draw(weight_keys[7], (2, H, block_width, block_width), 2.0 * block_width ** -0.5),
        'gate_ba': normal_draw(weight_keys[8], (2, L), 1.5),
        'gate_wi': normal_draw(weight_keys[9], (2, H, block_width, block_width), block_width ** -0.5),
        'gate_bi': normal_draw(weight_keys[10], (2, L), 0.5),
        'a_param': jnp.log(jnp.expm1(a_soft)),
        'rec_wout': normal_draw(weight_keys[12], (2, L, D), L ** -0.5),
        'rec_bout': normal_draw(weight_keys[13], (2, D), 0.2),
        'attn_wq': normal_draw(weight_keys[14], (D, H * HEAD), D ** -0.5),
        'attn_wk': normal_draw(weight_keys[15], (D, HEAD), D ** -0.5),
        'attn_wv': normal_draw(weight_keys[16], (D, HEAD), D ** -0.5),
        'attn_wo': normal_draw(weight_keys[17], (H * HEAD, D), (H * HEAD) ** -0.5),
        'attn_bo': normal_draw(weight_keys[18], (D,), 0.2),
        'mlp_w1': normal_draw(weight_keys[19], (3, D, F), D ** -0.5),
        'mlp_b1': normal_draw(weight_keys[20], (3, F), 0.3),
        'mlp_w2': normal_draw(weight_keys[21], (3, D, F), D ** -0.5),
        'mlp_b2': normal_draw(weight_keys[22], (3, F), 0.3),
        'mlp_wd': normal_draw(weight_keys[23], (3, F, D), F ** -0.5),
        'mlp_bd': normal_draw(weight_keys[24], (3, D), 0.2),
    }


def rms_norm(residual, scale):
    res_f = residual.astype(jnp.float32)
    mean_sq = jnp.mean(res_f * res_f, axis=-1, keepdims=True)
    return (res_f * lax.rsqrt(mean_sq + NORM_EPS) * (1.0 + scale.astype(jnp.float32))).astype(jnp.bfloat16)


def add_update(residual, update, out_bias):
    return (residual.astype(jnp.float32) + update.astype(jnp.bfloat16).astype(jnp.float32) + out_bias.astype(jnp.float32)).astype(jnp.bfloat16)


def rope_tables(tok_pos, head_dim):
    quarter = head_dim // 4
    inv_freq = ROPE_BASE ** (-jnp.arange(quarter, dtype=jnp.float32) / quarter)
    angles = tok_pos.astype(jnp.float32)[:, None] * inv_freq[None, :]
    return jnp.cos(angles), jnp.sin(angles)


def apply_rope(vectors, cosine, sine):
    quarter = vectors.shape[-1] // 4
    first = vectors[..., :quarter]
    second = vectors[..., quarter:2 * quarter]
    return jnp.concatenate([first * cosine - second * sine, second * cosine + first * sine, vectors[..., 2 * quarter:]], axis=-1)


def mlp_update(normed, w_up, b_up, w_lin, b_lin, w_down):
    gate_pre = jnp.dot(normed, w_up, preferred_element_type=jnp.float32) + b_up.astype(jnp.float32)
    lin_pre = jnp.dot(normed, w_lin, preferred_element_type=jnp.float32) + b_lin.astype(jnp.float32)
    hidden = (jax.nn.gelu(gate_pre, approximate=True) * lin_pre).astype(jnp.bfloat16)
    return jnp.dot(hidden, w_down, preferred_element_type=jnp.float32)


def recurrent_update(normed, tok_pos, conv_prev, lru_prev, rec_wx, rec_bx, rec_wy, rec_by, conv_w, conv_b, gate_wa, gate_ba, gate_wi, gate_bi, a_param, rec_wout):
    n_rows = normed.shape[0]
    n_blocks = gate_wa.shape[0]
    block_width = gate_wa.shape[1]
    x_branch = (jnp.dot(normed, rec_wx, preferred_element_type=jnp.float32) + rec_bx.astype(jnp.float32)).astype(jnp.bfloat16)
    y_branch = jax.nn.gelu(jnp.dot(normed, rec_wy, preferred_element_type=jnp.float32) + rec_by.astype(jnp.float32), approximate=True)
    tap_keep = tok_pos[:, None, None] >= jnp.arange(3, 0, -1, dtype=jnp.int32)[None, :, None]
    history = jnp.where(tap_keep, conv_prev.astype(jnp.float32), 0.0)
    tap_w = conv_w.astype(jnp.float32)
    conv_sum = conv_b.astype(jnp.float32) + tap_w[0] * x_branch.astype(jnp.float32) + jnp.sum(history * tap_w[:0:-1][None], axis=1)
    conv_x = conv_sum.astype(jnp.bfloat16)
    blocks = conv_x.reshape(n_rows, n_blocks, block_width).astype(jnp.float32)
    r_pre = jnp.einsum('bhi,hij->bhj', blocks, gate_wa.astype(jnp.float32)).reshape(n_rows, -1) + gate_ba.astype(jnp.float32)
    i_pre = jnp.einsum('bhi,hij->bhj', blocks, gate_wi.astype(jnp.float32)).reshape(n_rows, -1) + gate_bi.astype(jnp.float32)
    log_a = -8.0 * jax.nn.sigmoid(r_pre) * jax.nn.softplus(a_param)
    decay_gate = jnp.exp(log_a)
    in_scale = jnp.sqrt(1.0 - decay_gate * decay_gate)
    is_reset = (tok_pos == 0)[:, None]
    decay_gate = jnp.where(is_reset, 0.0, decay_gate)
    in_scale = jnp.where(is_reset, 1.0, in_scale)
    lru_new = decay_gate * lru_prev + in_scale * jax.nn.sigmoid(i_pre) * conv_x.astype(jnp.float32)
    gated_h = (lru_new * y_branch).astype(jnp.bfloat16)
    update = jnp.dot(gated_h, rec_wout, preferred_element_type=jnp.float32)
    conv_new = jnp.concatenate([conv_prev[:, 1:], x_branch[:, None, :]], axis=1)
    return update, conv_new, lru_new


def attention_update(normed, tok_pos, k_cache, v_cache, slot_pos, attn_wq, attn_wk, attn_wv, attn_wo):
    n_rows = normed.shape[0]
    head_dim = attn_wk.shape[1]
    window = k_cache.shape[1]
    cosine, sine = rope_tables(tok_pos, head_dim)
    q_heads = jnp.dot(normed, attn_wq, preferred_element_type=jnp.float32).reshape(n_rows, -1, head_dim)
    q_heads = apply_rope(q_heads, cosine[:, None, :], sine[:, None, :]).astype(jnp.bfloat16)
    k_new = apply_rope(jnp.dot(normed, attn_wk, preferred_element_type=jnp.float32), cosine, sine).astype(jnp.bfloat16)
    v_new = jnp.dot(normed, attn_wv, preferred_element_type=jnp.float32).astype(jnp.bfloat16)
    target = jnp.arange(window, dtype=jnp.int32)[None, :] == (tok_pos % window)[:, None]
    k_next = jnp.where(target[:, :, None], k_new[:, None, :], k_cache)
    v_next = jnp.where(target[:, :, None], v_new[:, None, :], v_cache)
    slot_next = jnp.where(target, tok_pos[:, None], slot_pos)
    slot_age = tok_pos[:, None] - slot_next
    slot_valid = (slot_next >= 0) & (slot_age >= 0) & (slot_age < window)

    def attend_row(row_args):
        q_row, k_row, v_row, valid_row = row_args
        scores = jnp.einsum('hd,sd->hs', q_row.astype(jnp.float32), k_row.astype(jnp.float32)) * (head_dim ** -0.5)
        scores = jnp.where(valid_row[None, :], scores, -jnp.inf)
        probs_bf = jax.nn.softmax(scores, axis=-1).astype(jnp.bfloat16)
        return jnp.einsum('hs,sd->hd', probs_bf.astype(jnp.float32), v_row.astype(jnp.float32)).astype(jnp.bfloat16)

    heads_out = lax.map(attend_row, (q_heads, k_next, v_next, slot_valid))
    update = jnp.dot(heads_out.reshape(n_rows, -1), attn_wo, preferred_element_type=jnp.float32)
    return update, k_next, v_next, slot_next


def reference(x_in, tok_pos, conv_state, lru_state, k_cache, v_cache, slot_pos, norm_scale, rec_wx, rec_bx, rec_wy, rec_by, conv_w, conv_b, gate_wa, gate_ba, gate_wi, gate_bi, a_param, rec_wout, rec_bout, attn_wq, attn_wk, attn_wv, attn_wo, attn_bo, mlp_w1, mlp_b1, mlp_w2, mlp_b2, mlp_wd, mlp_bd):
    residual = x_in
    conv_list = []
    lru_list = []
    for layer_idx in range(3):
        normed = rms_norm(residual, norm_scale[layer_idx, 0])
        if layer_idx < 2:
            update, conv_new, lru_new = recurrent_update(normed, tok_pos, conv_state[layer_idx], lru_state[layer_idx], rec_wx[layer_idx], rec_bx[layer_idx], rec_wy[layer_idx], rec_by[layer_idx], conv_w[layer_idx], conv_b[layer_idx], gate_wa[layer_idx], gate_ba[layer_idx], gate_wi[layer_idx], gate_bi[layer_idx], a_param[layer_idx], rec_wout[layer_idx])
            conv_list.append(conv_new)
            lru_list.append(lru_new)
            out_bias = rec_bout[layer_idx]
        else:
            update, k_next, v_next, slot_next = attention_update(normed, tok_pos, k_cache, v_cache, slot_pos, attn_wq, attn_wk, attn_wv, attn_wo)
            out_bias = attn_bo
        residual = add_update(residual, update, out_bias)
        normed = rms_norm(residual, norm_scale[layer_idx, 1])
        update = mlp_update(normed, mlp_w1[layer_idx], mlp_b1[layer_idx], mlp_w2[layer_idx], mlp_b2[layer_idx], mlp_wd[layer_idx])
        residual = add_update(residual, update, mlp_bd[layer_idx])
    return (residual, jnp.stack(conv_list), jnp.stack(lru_list), k_next, v_next, slot_next)
```

```python
import functools

import jax
import jax.numpy as jnp
from jax import lax
from jax.experimental import pallas as pl
from jax.experimental.pallas import tpu as pltpu
from jax.sharding import PartitionSpec as P

ROPE_BASE = 10000.0
NORM_EPS = 1e-6
MESH = pl.DeviceIdType.MESH
BF = jnp.bfloat16
F32 = jnp.float32
ANY = pl.BlockSpec(memory_space=pl.ANY)
VM = pl.BlockSpec(memory_space=pltpu.VMEM)
B = 256
D = 4096
LC = 704
FC = 1536
W = 1024
HD = 128
G = 4
GC = D // G


def rms(x, scale):
    xf = x.astype(F32)
    mean_sq = jnp.mean(xf * xf, axis=-1, keepdims=True)
    return (xf * lax.rsqrt(mean_sq + NORM_EPS) * (1.0 + scale.astype(F32))).astype(BF)


def norm_into(n_s, x_ref, scale):
    for r in range(0, B, 32):
        n_s[r:r + 32, :] = rms(x_ref[r:r + 32, :], scale)


def ar_kernel(layer, part_ref, x_ref, b_ref, out_ref, xbuf, xown, recv1, send2, recv2, own,
              s1s, s1r, s2s, s2r, s3s, s3r, s4s, s4r, lsem, osem):
    t = lax.axis_index('tp')
    y = t // 4
    x = (t // 2) % 2
    c = t % 2
    q = 2 * y + x
    partner = 2 * q + 1 - c
    chips = [2 * y + (1 - x), 2 * (1 - y) + x, 2 * (1 - y) + (1 - x)]
    peers = [2 * qd + c for qd in chips]
    barrier = pltpu.get_barrier_semaphore()
    for dev in [partner] + peers:
        pl.semaphore_signal(barrier, inc=1, device_id={'tp': dev}, device_id_type=MESH)
    load_x = pltpu.make_async_copy(x_ref.at[q, c], xown, lsem)
    load_x.start()
    pl.semaphore_wait(barrier, 4)

    def remote(src, dst, ss, rs, dev):
        cp = pltpu.make_async_remote_copy(src_ref=src, dst_ref=dst, send_sem=ss, recv_sem=rs, device_id={'tp': dev}, device_id_type=MESH)
        cp.start()
        return cp

    cols = [pl.ds(g * GC, GC) for g in range(G)]
    cp1 = [remote(part_ref.at[:, 1 - c, :, cols[g]], recv1.at[:, :, cols[g]], s1s.at[g], s1r.at[g], partner) for g in range(G)]
    cp2 = []
    for g in range(G):
        cp1[g].wait_recv()
        row = []
        for k in (2, 0, 1):
            s = part_ref[chips[k], c, :, cols[g]].astype(F32) + recv1[chips[k], :, cols[g]].astype(F32)
            send2[k, :, cols[g]] = s.astype(BF)
            row.append((k, remote(send2.at[k, :, cols[g]], recv2.at[k, :, cols[g]], s2s.at[g, k], s2r.at[g, k], peers[k])))
        own[:, cols[g]] = part_ref[q, c, :, cols[g]].astype(F32) + recv1[q, :, cols[g]].astype(F32)
        cp2.append([cp for _, cp in sorted(row, key=lambda e: e[0])])
    load_x.wait()
    cp3 = []
    ocp = []
    for g in range(G):
        for k in range(3):
            cp2[g][k].wait_recv()
        tot = own[:, cols[g]]
        for k in range(3):
            tot = tot + recv2[k, :, cols[g]].astype(F32)
        bias = b_ref[...].astype(F32)[layer:layer + 1, g * GC:(g + 1) * GC]
        xn = (xown[:, cols[g]].astype(F32) + tot.astype(BF).astype(F32) + bias).astype(BF)
        xbuf[q, c, :, cols[g]] = xn
        place = xbuf.at[q, c, :, cols[g]]
        row = {}
        for k in (2, 0, 1):
            row[k] = remote(place, place, s3s.at[g, k], s3r.at[g, k], peers[k])
        row[3] = remote(place, place, s3s.at[g, 3], s3r.at[g, 3], partner)
        cp3.append(row)
    cp4 = []
    for g in range(G):
        for k in range(3):
            cp3[g][k].wait_recv()
            place = xbuf.at[chips[k], c, :, cols[g]]
            cp4.append(remote(place, place, s4s.at[g, k], s4r.at[g, k], partner))
    for g in range(G):
        cp3[g][3].wait_recv()
    for cp in cp4:
        cp.wait_recv()
    store = pltpu.make_async_copy(xbuf, out_ref, osem)
    store.start()
    for g in range(G):
        cp1[g].wait_send()
        for k in range(3):
            cp2[g][k].wait_send()
        for k in range(4):
            cp3[g][k].wait_send()
    for cp in cp4:
        cp.wait_send()
    store.wait()


def all_reduce(part, x, bias, layer, cid):
    out = pl.pallas_call(
        functools.partial(ar_kernel, layer),
        name=f'ar{cid}',
        out_shape=jax.ShapeDtypeStruct((4, 2, 32, D), BF),
        in_specs=[VM, ANY, VM],
        out_specs=ANY,
        scratch_shapes=[
            pltpu.VMEM((4, 2, 32, D), BF), pltpu.VMEM((32, D), BF), pltpu.VMEM((4, 32, D), BF),
            pltpu.VMEM((3, 32, D), BF), pltpu.VMEM((3, 32, D), BF), pltpu.VMEM((32, D), F32),
            pltpu.SemaphoreType.DMA((G,)), pltpu.SemaphoreType.DMA((G,)),
            pltpu.SemaphoreType.DMA((G, 3)), pltpu.SemaphoreType.DMA((G, 3)),
            pltpu.SemaphoreType.DMA((G, 4)), pltpu.SemaphoreType.DMA((G, 4)),
            pltpu.SemaphoreType.DMA((G, 3)), pltpu.SemaphoreType.DMA((G, 3)),
            pltpu.SemaphoreType.DMA, pltpu.SemaphoreType.DMA,
        ],
        compiler_params=pltpu.CompilerParams(collective_id=cid, has_side_effects=True),
        cost_estimate=pl.CostEstimate(flops=10**9, bytes_accessed=80 * 10**6, transcendentals=0),
    )(part.reshape(4, 2, 32, D), x.reshape(4, 2, 32, D), bias)
    return out.reshape(B, D)


def mlp_kernel(layer, nb, x_ref, sc_ref, w1_ref, b1_ref, w2_ref, b2_ref, wd_ref, out_ref, n_s, h_s):
    i = pl.program_id(0)

    @pl.when(i == 0)
    def _():
        norm_into(n_s, x_ref, sc_ref[...].astype(F32)[layer, 1:2, :])

    @pl.when(i < nb)
    def _():
        n = n_s[...]
        lanes = pl.ds(pl.multiple_of(i * 256, 256), 256)
        g = jnp.dot(n, w1_ref[0], preferred_element_type=F32) + b1_ref[:, lanes].astype(F32)[layer:layer + 1]
        u = jnp.dot(n, w2_ref[0], preferred_element_type=F32) + b2_ref[:, lanes].astype(F32)[layer:layer + 1]
        h_s[:, lanes] = (jax.nn.gelu(g, approximate=True) * u).astype(BF)

    @pl.when(i >= nb)
    def _():
        out_ref[...] = jnp.dot(h_s[...], wd_ref[0], preferred_element_type=F32).astype(BF)


def mlp(x, scale, w1, b1, w2, b2, wd, layer):
    nb = FC // 256
    nd = D // 512
    up = pl.BlockSpec((1, D, 256), lambda i: (layer, 0, jnp.minimum(i, nb - 1)))
    return pl.pallas_call(
        functools.partial(mlp_kernel, layer, nb),
        name=f'mlp{layer}',
        grid=(nb + nd,),
        out_shape=jax.ShapeDtypeStruct((B, D), BF),
        in_specs=[pl.BlockSpec((B, D), lambda i: (0, 0)), pl.BlockSpec(scale.shape, lambda i: (0, 0, 0)),
                  up, pl.BlockSpec(b1.shape, lambda i: (0, 0)), up, pl.BlockSpec(b2.shape, lambda i: (0, 0)),
                  pl.BlockSpec((1, FC, 512), lambda i: (layer, 0, jnp.maximum(i - nb, 0)))],
        out_specs=pl.BlockSpec((B, 512), lambda i: (0, jnp.maximum(i - nb, 0))),
        scratch_shapes=[pltpu.VMEM((B, D), BF), pltpu.VMEM((B, FC), BF)],
        cost_estimate=pl.CostEstimate(flops=2 * B * D * FC * 3, bytes_accessed=6 * D * FC, transcendentals=0),
    )(x, scale, w1, b1, w2, b2, wd)


RB = 352


def rec_kernel(layer, x_ref, sc_ref, wx_ref, wy_ref, conv_ref, lru_ref, wa_ref, wi_ref, pc_ref, tok_ref, wo_ref,
               out_ref, conv_out, lru_out, n_s, ht_s, hy_s):
    i = pl.program_id(0)
    nb = LC // RB

    @pl.when(i == 0)
    def _():
        norm_into(n_s, x_ref, sc_ref[...].astype(F32)[layer, 0:1, :])

    @pl.when(i < nb)
    def _():
        n = n_s[...]
        nt = (((1,), (1,)), ((), ()))
        pc = pc_ref[0]
        col = lambda k: pc[:, k:k + 1]
        tok = tok_ref[...]
        xb = (lax.dot_general(wx_ref[0], n, nt, preferred_element_type=F32) + col(0)).astype(BF)
        yb = jax.nn.gelu(lax.dot_general(wy_ref[0], n, nt, preferred_element_type=F32) + col(1), approximate=True)
        hist = jnp.zeros((RB, B), F32)
        for j in range(3):
            hj = jnp.where(tok >= 3 - j, conv_ref[0, j].astype(F32), 0.0)
            hist = hist + hj * col(5 - j)
        xc = (col(6) + col(2) * xb.astype(F32) + hist).astype(BF)
        conv_out[0, 0] = conv_ref[0, 1]
        conv_out[0, 1] = conv_ref[0, 2]
        conv_out[0, 2] = xb
        tn = (((0,), (0,)), ((), ()))
        fresh = tok == 0
        for h in range(RB // 176):
            rows = slice(176 * h, 176 * h + 176)
            xh = xc[rows]
            ph = pc[rows]
            rg = jax.nn.sigmoid(lax.dot_general(wa_ref[0, h], xh, tn, preferred_element_type=F32) + ph[:, 7:8])
            ig = jax.nn.sigmoid(lax.dot_general(wi_ref[0, h], xh, tn, preferred_element_type=F32) + ph[:, 8:9])
            a = jnp.exp(rg * ph[:, 9:10])
            sc = jnp.sqrt(1.0 - a * a)
            a = jnp.where(fresh, 0.0, a)
            sc = jnp.where(fresh, 1.0, sc)
            hn = a * lru_ref[0, rows, :] + sc * ig * xh.astype(F32)
            lru_out[0, rows, :] = hn
            ht_s[pl.ds(pl.multiple_of(i * RB, 16) + 176 * h, 176), :] = (hn * yb[rows]).astype(BF)

    @pl.when(i == nb)
    def _():
        ht_s[LC:, :] = jnp.zeros((64, B), BF)
        hy_s[...] = ht_s[...].T

    @pl.when(i >= nb)
    def _():
        out_ref[...] = jnp.dot(hy_s[:, :LC], wo_ref[0], preferred_element_type=F32).astype(BF)


def rec(x, scale, wxt, wyt, convt, lrut, wa, wi, pcols, tok, wout, layer):
    nb = LC // RB
    nd = D // 512
    up = pl.BlockSpec((1, RB, D), lambda i: (layer, jnp.minimum(i, nb - 1), 0))
    gate = pl.BlockSpec((1, RB // 176, 176, 176), lambda i: (layer, jnp.minimum(i, nb - 1), 0, 0))
    return pl.pallas_call(
        functools.partial(rec_kernel, layer),
        name=f'rec{layer}',
        grid=(nb + nd,),
        out_shape=(jax.ShapeDtypeStruct((B, D), BF), jax.ShapeDtypeStruct((1, 3, LC, B), BF), jax.ShapeDtypeStruct((1, LC, B), F32)),
        in_specs=[pl.BlockSpec((B, D), lambda i: (0, 0)), pl.BlockSpec(scale.shape, lambda i: (0, 0, 0)), up, up,
                  pl.BlockSpec((1, 3, RB, B), lambda i: (layer, 0, jnp.minimum(i, nb - 1), 0)),
                  pl.BlockSpec((1, RB, B), lambda i: (layer, jnp.minimum(i, nb - 1), 0)),
                  gate, gate, pl.BlockSpec((1, RB, pcols.shape[2]), lambda i: (layer, jnp.minimum(i, nb - 1), 0)),
                  pl.BlockSpec((1, B), lambda i: (0, 0)),
                  pl.BlockSpec((1, LC, 512), lambda i: (layer, 0, jnp.maximum(i - nb, 0)))],
        out_specs=(pl.BlockSpec((B, 512), lambda i: (0, jnp.maximum(i - nb, 0))),
                   pl.BlockSpec((1, 3, RB, B), lambda i: (0, 0, jnp.minimum(i, nb - 1), 0)),
                   pl.BlockSpec((1, RB, B), lambda i: (0, jnp.minimum(i, nb - 1), 0))),
        scratch_shapes=[pltpu.VMEM((B, D), BF), pltpu.VMEM((LC + 64, B), BF), pltpu.VMEM((B, LC + 64), BF)],
        cost_estimate=pl.CostEstimate(flops=2 * B * D * LC * 3, bytes_accessed=6 * D * LC, transcendentals=0),
    )(x, scale, wxt, wyt, convt, lrut, wa, wi, pcols, tok, wout)


def rope(v, tab_ref):
    return v * tab_ref[0] + pltpu.roll(v, 96, 1) * tab_ref[1] + pltpu.roll(v, 32, 1) * tab_ref[2]


def qkv_kernel(x_ref, sc_ref, wq_ref, wk_ref, wv_ref, tab_ref, q_ref, k_ref, v_ref, n_s):
    i = pl.program_id(0)

    @pl.when(i == 0)
    def _():
        norm_into(n_s, x_ref, sc_ref[...].astype(F32)[2, 0:1, :])

    @pl.when(i < 2)
    def _():
        qf = jnp.dot(n_s[...], wq_ref[...], preferred_element_type=F32)
        for h in range(2):
            q_ref[h] = rope(qf[:, 128 * h:128 * h + 128], tab_ref).astype(BF)

    @pl.when(i == 2)
    def _():
        k_ref[...] = rope(jnp.dot(n_s[...], wk_ref[...], preferred_element_type=F32), tab_ref).astype(BF)
        v_ref[...] = jnp.dot(n_s[...], wv_ref[...], preferred_element_type=F32).astype(BF)


def qkv(x, scale, wq, wk, wv, tab):
    return pl.pallas_call(
        qkv_kernel,
        name='qkv',
        grid=(3,),
        out_shape=(jax.ShapeDtypeStruct((4, B, HD), BF), jax.ShapeDtypeStruct((B, HD), BF), jax.ShapeDtypeStruct((B, HD), BF)),
        in_specs=[pl.BlockSpec((B, D), lambda i: (0, 0)), pl.BlockSpec(scale.shape, lambda i: (0, 0, 0)),
                  pl.BlockSpec((D, 256), lambda i: (0, jnp.minimum(i, 1))),
                  pl.BlockSpec((D, HD), lambda i: (0, 0)), pl.BlockSpec((D, HD), lambda i: (0, 0)),
                  pl.BlockSpec((3, B, HD), lambda i: (0, 0, 0))],
        out_specs=(pl.BlockSpec((2, B, HD), lambda i: (jnp.minimum(i, 1), 0, 0)),
                   pl.BlockSpec((B, HD), lambda i: (0, 0)), pl.BlockSpec((B, HD), lambda i: (0, 0))),
        scratch_shapes=[pltpu.VMEM((B, D), BF)],
        cost_estimate=pl.CostEstimate(flops=2 * B * D * 768, bytes_accessed=2 * D * 768, transcendentals=0),
    )(x, scale, wq, wk, wv, tab)


RA = 8


def attn_kernel(tok_ref, q_ref, kn_ref, vn_ref, slot_ref, k_ref, v_ref, o_ref, ko_ref, vo_ref, so_ref):
    i = pl.program_id(0)
    lane = lax.broadcasted_iota(jnp.int32, (1, W), 1)
    sub = lax.broadcasted_iota(jnp.int32, (16, HD), 0)
    for r in range(RA):
        tp = tok_ref[i * RA + r]
        slot = lax.rem(tp, W)
        base = pl.multiple_of((slot // 16) * 16, 16)
        hit = sub == (slot - base)
        ko_ref[r] = k_ref[r]
        vo_ref[r] = v_ref[r]
        kn = kn_ref[...].astype(F32)[r:r + 1]
        vn = vn_ref[...].astype(F32)[r:r + 1]
        ko_ref[r, pl.ds(base, 16), :] = jnp.where(hit, kn, k_ref[r, pl.ds(base, 16), :].astype(F32)).astype(BF)
        vo_ref[r, pl.ds(base, 16), :] = jnp.where(hit, vn, v_ref[r, pl.ds(base, 16), :].astype(F32)).astype(BF)
        sn = jnp.where(lane == slot, tp, slot_ref[r:r + 1, :])
        so_ref[r:r + 1, :] = sn
        age = tp - sn
        valid = (sn >= 0) & (age >= 0) & (age < W)
        s = lax.dot_general(q_ref[r], ko_ref[r], (((1,), (1,)), ((), ())), preferred_element_type=F32) * (HD ** -0.5)
        s = jnp.where(valid, s, -jnp.inf)
        m = jnp.max(s, axis=-1, keepdims=True)
        e = jnp.exp(s - m)
        p = (e / jnp.sum(e, axis=-1, keepdims=True)).astype(BF)
        o_ref[r] = jnp.dot(p, vo_ref[r], preferred_element_type=F32).astype(BF)


def attend(tok, q, kn, vn, slot_pos, kc, vc):
    cache = pl.BlockSpec((RA, W, HD), lambda i, t: (i, 0, 0))
    row = pl.BlockSpec((RA, HD), lambda i, t: (i, 0))
    slots = pl.BlockSpec((RA, W), lambda i, t: (i, 0))
    heads = pl.BlockSpec((RA, 4, HD), lambda i, t: (i, 0, 0))
    return pl.pallas_call(
        attn_kernel,
        name='attend',
        grid_spec=pltpu.PrefetchScalarGridSpec(
            num_scalar_prefetch=1,
            grid=(B // RA,),
            in_specs=[heads, row, row, slots, cache, cache],
            out_specs=(heads, cache, cache, slots),
        ),
        out_shape=(jax.ShapeDtypeStruct((B, 4, HD), BF), jax.ShapeDtypeStruct(kc.shape, BF), jax.ShapeDtypeStruct(vc.shape, BF), jax.ShapeDtypeStruct(slot_pos.shape, jnp.int32)),
        cost_estimate=pl.CostEstimate(flops=4 * B * 4 * W * HD, bytes_accessed=8 * B * W * HD, transcendentals=0),
    )(tok, q, kn, vn, slot_pos, kc, vc)


def wo_kernel(o_ref, w_ref, out_ref):
    out_ref[...] = jnp.dot(o_ref[...], w_ref[...], preferred_element_type=F32).astype(BF)


def out_proj(o, wo):
    return pl.pallas_call(
        wo_kernel,
        name='wo',
        grid=(D // 1024,),
        out_shape=jax.ShapeDtypeStruct((B, D), BF),
        in_specs=[pl.BlockSpec((B, 512), lambda i: (0, 0)), pl.BlockSpec((512, 1024), lambda i: (0, i))],
        out_specs=pl.BlockSpec((B, 1024), lambda i: (0, i)),
        cost_estimate=pl.CostEstimate(flops=2 * B * D * 512, bytes_accessed=2 * D * 512, transcendentals=0),
    )(o, wo)


def rope_tables(tok_pos):
    quarter = HD // 4
    inv_freq = ROPE_BASE ** (-jnp.arange(quarter, dtype=F32) / quarter)
    angles = tok_pos.astype(F32)[:, None] * inv_freq[None, :]
    cos, sin = jnp.cos(angles), jnp.sin(angles)
    one = jnp.ones_like(cos)
    zero = jnp.zeros_like(cos)
    keep = jnp.concatenate([cos, cos, one, one], axis=1)
    up = jnp.concatenate([-sin, zero, zero, zero], axis=1)
    down = jnp.concatenate([zero, sin, zero, zero], axis=1)
    return jnp.stack([keep, up, down])


def io_specs():
    in_specs = (P('dp', None), P('dp'), P(None, 'dp', None, 'tp'), P(None, 'dp', 'tp'), P('dp', None, None), P('dp', None, None), P('dp', None),
                P(), P(None, None, 'tp'), P(None, 'tp'), P(None, None, 'tp'), P(None, 'tp'), P(None, None, 'tp'), P(None, 'tp'),
                P(None, 'tp', None, None), P(None, 'tp'), P(None, 'tp', None, None), P(None, 'tp'), P(None, 'tp'), P(None, 'tp', None), P(),
                P(None, 'tp'), P(), P(), P('tp', None), P(),
                P(None, None, 'tp'), P(None, 'tp'), P(None, None, 'tp'), P(None, 'tp'), P(None, 'tp', None), P())
    out_specs = (P('dp', None), P(None, 'dp', None, 'tp'), P(None, 'dp', 'tp'), P('dp', None, None), P('dp', None, None), P('dp', None))
    return in_specs, out_specs


def solution(mesh):
    in_specs, out_specs = io_specs()

    def local_step(x_in, tok_pos, conv_state, lru_state, k_cache, v_cache, slot_pos, norm_scale, rec_wx, rec_bx, rec_wy, rec_by, conv_w, conv_b, gate_wa, gate_ba, gate_wi, gate_bi, a_param, rec_wout, rec_bout, attn_wq, attn_wk, attn_wv, attn_wo, attn_bo, mlp_w1, mlp_b1, mlp_w2, mlp_b2, mlp_wd, mlp_bd):
        wxt = jnp.swapaxes(rec_wx, 1, 2)
        wyt = jnp.swapaxes(rec_wy, 1, 2)
        convt = jnp.transpose(conv_state, (0, 2, 3, 1))
        lrut = jnp.swapaxes(lru_state, 1, 2)
        f = lambda v: v.astype(F32)
        pcols = jnp.stack([f(rec_bx), f(rec_by), f(conv_w[:, 0]), f(conv_w[:, 1]), f(conv_w[:, 2]), f(conv_w[:, 3]), f(conv_b), f(gate_ba), f(gate_bi), -8.0 * jax.nn.softplus(a_param)], axis=-1)
        tok_row = tok_pos[None, :]
        tab = rope_tables(tok_pos)

        x = x_in
        convs = []
        lrus = []
        for layer in range(2):
            part, conv_new, lru_new = rec(x, norm_scale, wxt, wyt, convt, lrut, gate_wa, gate_wi, pcols, tok_row, rec_wout, layer)
            convs.append(conv_new)
            lrus.append(lru_new)
            x = all_reduce(part, x, rec_bout, layer, 2 * layer)
            part = mlp(x, norm_scale, mlp_w1, mlp_b1, mlp_w2, mlp_b2, mlp_wd, layer)
            x = all_reduce(part, x, mlp_bd, layer, 2 * layer + 1)
        q, kn, vn = qkv(x, norm_scale, attn_wq, attn_wk, attn_wv, tab)
        o, k_next, v_next, slot_next = attend(tok_pos, jnp.swapaxes(q, 0, 1), kn, vn, slot_pos, k_cache, v_cache)
        part = out_proj(o.reshape(B, 512), attn_wo)
        x = all_reduce(part, x, attn_bo[None, :], 0, 4)
        part = mlp(x, norm_scale, mlp_w1, mlp_b1, mlp_w2, mlp_b2, mlp_wd, 2)
        x = all_reduce(part, x, mlp_bd, 2, 5)
        conv_out = jnp.transpose(jnp.concatenate(convs), (0, 3, 1, 2))
        lru_out = jnp.swapaxes(jnp.concatenate(lrus), 1, 2)
        return (x, conv_out, lru_out, k_next, v_next, slot_next)

    return jax.shard_map(local_step, mesh=mesh, in_specs=in_specs, out_specs=out_specs, check_vma=False)
```

```python
import functools

import jax
import jax.numpy as jnp
from jax import lax
from jax.experimental import pallas as pl
from jax.experimental.pallas import tpu as pltpu
from jax.sharding import PartitionSpec as P

ROPE_BASE = 10000.0
NORM_EPS = 1e-6
MESH = pl.DeviceIdType.MESH
BF = jnp.bfloat16
F32 = jnp.float32
ANY = pl.BlockSpec(memory_space=pl.ANY)
VM = pl.BlockSpec(memory_space=pltpu.VMEM)
B = 256
D = 4096
LC = 704
FC = 1536
W = 1024
HD = 128
G = 4
GC = D // G


def rms(x, scale):
    xf = x.astype(F32)
    mean_sq = jnp.mean(xf * xf, axis=-1, keepdims=True)
    return (xf * lax.rsqrt(mean_sq + NORM_EPS) * (1.0 + scale.astype(F32))).astype(BF)


ROPE_DN = (((1,), (1,)), ((), ()))
TN = (((0,), (0,)), ((), ()))
COLS = [pl.ds(g * GC, GC) for g in range(G)]


class Links:
    def __init__(self, part, recv1, recv2, own, n, xown, s1s, s1r, s2s, s2r, s3s, s3r, s4s, s4r):
        self.part, self.recv1, self.recv2, self.own, self.n, self.xown = part, recv1, recv2, own, n, xown
        self.s1s, self.s1r, self.s2s, self.s2r, self.s3s, self.s3r, self.s4s, self.s4r = s1s, s1r, s2s, s2r, s3s, s3r, s4s, s4r
        t = lax.axis_index('tp')
        y, x = t // 4, (t // 2) % 2
        self.c = t % 2
        self.q = 2 * y + x
        self.partner = 2 * self.q + 1 - self.c
        self.chips = [2 * y + (1 - x), 2 * (1 - y) + x, 2 * (1 - y) + (1 - x)]
        self.peers = [2 * qd + self.c for qd in self.chips]

    def enter(self):
        barrier = pltpu.get_barrier_semaphore()
        for dev in [self.partner] + self.peers:
            pl.semaphore_signal(barrier, inc=1, device_id={'tp': dev}, device_id_type=MESH)
        pl.semaphore_wait(barrier, 4)

    def remote(self, src, dst, ss, rs, dev):
        cp = pltpu.make_async_remote_copy(src_ref=src, dst_ref=dst, send_sem=ss, recv_sem=rs, device_id={'tp': dev}, device_id_type=MESH)
        cp.start()
        return cp

    def dots(self, g, lhs, rhs):
        def body(p, carry):
            out = jnp.dot(lhs[...], rhs[:, pl.ds(pl.multiple_of(p * 512, 512), 512)], preferred_element_type=F32)
            self.part[:, :, :, pl.ds(pl.multiple_of(g * GC + p * 512, 512), 512)] = out.astype(BF).reshape(4, 2, 32, 512)
            return carry

        lax.fori_loop(0, GC // 512, body, 0)

    def reduce_scatter(self, produce, bias_row):
        c, q, chips, cp1, cp2 = self.c, self.q, self.chips, [], []

        def pair(g):
            cols = COLS[g]
            cp1[g].wait_recv()
            row = {}
            for k in (2, 0, 1):
                s = self.part[chips[k], c, :, cols].astype(F32) + self.recv1[chips[k], :, cols].astype(F32)
                self.part[chips[k], c, :, cols] = s.astype(BF)
                row[k] = self.remote(self.part.at[chips[k], c, :, cols], self.recv2.at[k, :, cols], self.s2s.at[g, k], self.s2r.at[g, k], self.peers[k])
            self.own[:, cols] = self.part[q, c, :, cols].astype(F32) + self.recv1[q, :, cols].astype(F32)
            cp2.append(row)

        for g in range(G):
            produce(g)
            cp1.append(self.remote(self.part.at[:, 1 - c, :, COLS[g]], self.recv1.at[:, :, COLS[g]], self.s1s.at[g], self.s1r.at[g], self.partner))
            if g >= 1:
                pair(g - 1)
        pair(G - 1)
        for g in range(G):
            cols = COLS[g]
            for k in range(3):
                cp2[g][k].wait_recv()
            tot = self.own[:, cols]
            for k in range(3):
                tot = tot + self.recv2[k, :, cols].astype(F32)
            bias = bias_row[:, g * GC:(g + 1) * GC]
            self.xown[:, cols] = (self.xown[:, cols].astype(F32) + tot.astype(BF).astype(F32) + bias).astype(BF)
        for g in range(G):
            cp1[g].wait_send()
            for k in range(3):
                cp2[g][k].wait_send()

    def place(self, dev, g):
        return self.n.at[pl.ds(pl.multiple_of(dev * 32, 32), 32), COLS[g]]

    def gather_start(self, rows):
        me = 2 * self.q + self.c
        self.n[pl.ds(pl.multiple_of(me * 32, 32), 32), :] = rows
        self.cp3, self.cp4 = [], []
        for g in range(G):
            ref = self.place(me, g)
            row = {}
            for k in (2, 0, 1):
                row[k] = self.remote(ref, ref, self.s3s.at[g, k], self.s3r.at[g, k], self.peers[k])
            row[3] = self.remote(ref, ref, self.s3s.at[g, 3], self.s3r.at[g, 3], self.partner)
            self.cp3.append(row)

    def gather_forward(self, g):
        row = []
        for k in range(3):
            self.cp3[g][k].wait_recv()
            ref = self.place(self.peers[k], g)
            row.append(self.remote(ref, ref, self.s4s.at[g, k], self.s4r.at[g, k], self.partner))
        self.cp4.append(row)

    def gather_ready(self, g):
        self.cp3[g][3].wait_recv()
        for k in range(3):
            self.cp4[g][k].wait_recv()

    def gather_finish(self):
        for g in range(G):
            for k in range(4):
                self.cp3[g][k].wait_send()
            for k in range(3):
                self.cp4[g][k].wait_send()

    def gathered(self, use, fresh=False):
        for g in range(G):
            if not fresh:
                self.gather_forward(g)
            if g >= 1:
                if not fresh:
                    self.gather_ready(g - 1)
                use(g - 1)
        if not fresh:
            self.gather_ready(G - 1)
        use(G - 1)
        if not fresh:
            self.gather_finish()


LINK_SCRATCH = [
    pltpu.VMEM((4, 2, 32, D), BF), pltpu.VMEM((4, 32, D), BF), pltpu.VMEM((3, 32, D), BF),
    pltpu.VMEM((32, D), F32), pltpu.VMEM((B, D), BF), pltpu.VMEM((32, D), BF),
    pltpu.SemaphoreType.DMA((G,)), pltpu.SemaphoreType.DMA((G,)), pltpu.SemaphoreType.DMA((G, 3)), pltpu.SemaphoreType.DMA((G, 3)),
    pltpu.SemaphoreType.DMA((G, 4)), pltpu.SemaphoreType.DMA((G, 4)), pltpu.SemaphoreType.DMA((G, 3)), pltpu.SemaphoreType.DMA((G, 3)),
]
NLINK = len(LINK_SCRATCH)


class Ring:
    def __init__(self, groups, depth):
        self.groups, self.depth, self.issued = groups, depth, 0

    def fill(self, used):
        while self.issued < min(used + self.depth, len(self.groups)):
            for cp in self.groups[self.issued]:
                cp.start()
            self.issued += 1

    def wait(self, k):
        for cp in self.groups[k]:
            cp.wait()


SLOTS = 3


def up_group(k, layer, g, w1, w2, wu, sems):
    s = k % SLOTS
    rows = pl.ds(g * GC, GC)
    return [pltpu.make_async_copy(w1.at[layer, rows, :], wu.at[s, 0], sems.at[s, 0]), pltpu.make_async_copy(w2.at[layer, rows, :], wu.at[s, 1], sems.at[s, 1])]


def down_group(k, layer, g, wd, wdb, sems):
    s = k % SLOTS
    return [pltpu.make_async_copy(wd.at[layer, :, COLS[g]], wdb.at[s], sems.at[s])]


def mlp_up(net, ring, k0, wu, acc, h_s, b1, b2):
    def use(g):
        k = k0 + g
        s = k % SLOTS
        ring.wait(k)
        ng = net.n[:, COLS[g]]

        def body(j, carry):
            lanes = pl.ds(pl.multiple_of(j * 512, 512), 512)
            for half in range(2):
                a = jnp.dot(ng, wu[s, half, :, lanes], preferred_element_type=F32)
                for p in range(2):
                    piece = a[:, 256 * p:256 * p + 256]
                    at = 6 * half + 2 * j + p
                    acc[at] = piece if g == 0 else acc[at] + piece
            return carry

        lax.fori_loop(0, FC // 512, body, 0)
        ring.fill(k + 1)

    net.gathered(use)

    for j in range(FC // 256):
        lanes = slice(256 * j, 256 * j + 256)
        h_s[:, lanes] = (jax.nn.gelu(acc[j] + b1[:, lanes], approximate=True) * (acc[6 + j] + b2[:, lanes])).astype(BF)


def mlp_down(net, ring, k0, wdb, h_s, bias_row):
    def produce(g):
        k = k0 + g
        s = k % SLOTS
        ring.wait(k)
        net.dots(g, h_s, wdb.at[s])
        ring.fill(k + 1)

    net.reduce_scatter(produce, bias_row)


def rope(v, tab_ref):
    return v * tab_ref[0] + pltpu.roll(v, 96, 1) * tab_ref[1] + pltpu.roll(v, 32, 1) * tab_ref[2]


def kernel_a(x_ref, sc_ref, wx, wy, conv, lru, wa_ref, wi_ref, pc_ref, tok_ref, wout, rb_ref, w1, b1_ref, w2, b2_ref, wd, mb_ref, wq, wk, wv, tab_ref,
             q_ref, k_ref, v_ref, xo_ref, conv_out, lru_out, *scratch):
    net = Links(*scratch[:NLINK])
    wu, wdb, wxb, wob, acc, h_s, conv_s, xb_s, lru_s, ht_s, us, ds, xs, os, ss, ts, ls = scratch[NLINK:]
    f = lambda ref: ref[...].astype(F32)

    load_x = pltpu.make_async_copy(x_ref, net.part, ls)
    load_x.start()
    rec_in = [Ring([[pltpu.make_async_copy(wx.at[l, :, COLS[g]], wxb.at[0, :, COLS[g]], xs.at[0, g]), pltpu.make_async_copy(wy.at[l, :, COLS[g]], wxb.at[1, :, COLS[g]], xs.at[1, g])] for g in range(G)], G) for l in range(2)]
    rec_out = [Ring([[pltpu.make_async_copy(wout.at[l, :, COLS[g]], wob.at[:, COLS[g]], os.at[g])] for g in range(G)], G) for l in range(2)]
    state_in = [[pltpu.make_async_copy(conv.at[l], conv_s, ss.at[0]), pltpu.make_async_copy(lru.at[l], lru_s, ss.at[1])] for l in range(2)]
    state_out = [[pltpu.make_async_copy(conv_s.at[1:3], conv_out.at[l, 0:2], ts.at[0]), pltpu.make_async_copy(xb_s, conv_out.at[l, 2], ts.at[1]), pltpu.make_async_copy(lru_s, lru_out.at[l], ts.at[2])] for l in range(2)]
    ups = [up_group(4 * l + g, l, g, w1, w2, wu, us) for l in range(2) for g in range(G)]
    for g in range(G):
        s = (8 + g) % SLOTS
        rows = pl.ds(g * GC, GC)
        ups.append([pltpu.make_async_copy(wq.at[rows, :], wu.at[s, 0, :, 0:512], us.at[s, 0]), pltpu.make_async_copy(wk.at[rows, :], wu.at[s, 0, :, 512:640], us.at[s, 1]),
                    pltpu.make_async_copy(wv.at[rows, :], wu.at[s, 0, :, 640:768], us.at[s, 2])])
    up = Ring(ups, SLOTS)
    down = Ring([down_group(4 * l + g, l, g, wd, wdb, ds) for l in range(2) for g in range(G)], SLOTS)

    rec_in[0].fill(0)
    for cp in state_in[0]:
        cp.start()
    rec_out[0].fill(0)
    net.enter()
    load_x.wait()
    for j in range(8):
        net.n[32 * j:32 * j + 32, :] = rms(net.part[j // 2, j % 2], f(sc_ref)[0, 0:1, :])
    net.xown[...] = net.part[net.q, net.c]
    tok = tok_ref[...]
    fresh = tok == 0

    for layer in range(2):
        def use(g):
            rec_in[layer].wait(g)
            ng = net.n[:, COLS[g]]
            for half in range(2):
                r = lax.dot_general(wxb[half, :, COLS[g]], ng, ROPE_DN, preferred_element_type=F32)
                for h in range(4):
                    piece = r[176 * h:176 * h + 176]
                    acc[4 * half + h, 0:176, :] = piece if g == 0 else acc[4 * half + h, 0:176, :] + piece

        net.gathered(use, fresh=layer == 0)
        if layer == 0:
            up.fill(0)
            down.fill(0)
            rec_in[1].fill(0)
        for cp in state_in[layer]:
            cp.wait()
        for h in range(4):
            rows = slice(176 * h, 176 * h + 176)
            pc = pc_ref[layer, rows, :]
            col = lambda k: pc[:, k:k + 1]
            xb = (acc[h, 0:176, :] + col(0)).astype(BF)
            yb = jax.nn.gelu(acc[4 + h, 0:176, :] + col(1), approximate=True)
            xb_s[rows, :] = xb
            hist = jnp.zeros((176, B), F32)
            for j in range(3):
                hist = hist + jnp.where(tok >= 3 - j, conv_s[j, rows, :].astype(F32), 0.0) * col(5 - j)
            xc = (col(6) + col(2) * xb.astype(F32) + hist).astype(BF)
            rg = jax.nn.sigmoid(lax.dot_general(wa_ref[layer, h], xc, TN, preferred_element_type=F32) + col(7))
            ig = jax.nn.sigmoid(lax.dot_general(wi_ref[layer, h], xc, TN, preferred_element_type=F32) + col(8))
            a = jnp.exp(rg * col(9))
            sc = jnp.sqrt(1.0 - a * a)
            a = jnp.where(fresh, 0.0, a)
            sc = jnp.where(fresh, 1.0, sc)
            hn = a * lru_s[rows, :] + sc * ig * xc.astype(F32)
            lru_s[rows, :] = hn
            ht_s[rows, :] = (hn * yb).astype(BF)
        for cp in state_out[layer]:
            cp.start()
        ht_s[LC:, :] = jnp.zeros((64, B), BF)
        h_s[:, :LC + 64] = ht_s[...].T

        def produce(g):
            rec_out[layer].wait(g)
            net.dots(g, h_s.at[:, :LC], wob.at[:, COLS[g]])

        net.reduce_scatter(produce, f(rb_ref)[layer:layer + 1])
        net.gather_start(rms(net.xown[...], f(sc_ref)[layer, 1:2, :]))
        for cp in state_out[layer]:
            cp.wait()
        if layer == 0:
            rec_out[1].fill(0)
            for cp in state_in[1]:
                cp.start()
        mlp_up(net, up, 4 * layer, wu, acc, h_s, f(b1_ref)[layer:layer + 1], f(b2_ref)[layer:layer + 1])
        mlp_down(net, down, 4 * layer, wdb, h_s, f(mb_ref)[layer:layer + 1])
        net.gather_start(rms(net.xown[...], f(sc_ref)[layer + 1, 0:1, :]))

    xo_ref[...] = net.xown[...]

    def use_q(g):
        k = 8 + g
        up.wait(k)
        ng = net.n[:, COLS[g]]
        for j in range(3):
            a = jnp.dot(ng, wu[k % SLOTS, 0, :, 256 * j:256 * j + 256], preferred_element_type=F32)
            acc[j] = a if g == 0 else acc[j] + a
        up.fill(k + 1)

    net.gathered(use_q)
    for h in range(4):
        q_ref[h] = rope(acc[h // 2, :, 128 * (h % 2):128 * (h % 2) + 128], tab_ref).astype(BF)
    k_ref[...] = rope(acc[2, :, 0:128], tab_ref).astype(BF)
    v_ref[...] = acc[2, :, 128:256].astype(BF)


def first_layers(x, scale, wxt, wyt, convt, lrut, wa, wi, pcols, tok, wout, rb, w1, b1, w2, b2, wd, mb, wq, wk, wv, tab):
    return pl.pallas_call(
        kernel_a,
        name='first_layers',
        out_shape=(jax.ShapeDtypeStruct((4, B, HD), BF), jax.ShapeDtypeStruct((B, HD), BF), jax.ShapeDtypeStruct((B, HD), BF), jax.ShapeDtypeStruct((32, D), BF),
                   jax.ShapeDtypeStruct(convt.shape, BF), jax.ShapeDtypeStruct(lrut.shape, F32)),
        in_specs=[ANY, VM, ANY, ANY, ANY, ANY, VM, VM, VM, VM, ANY, VM, ANY, VM, ANY, VM, ANY, VM, ANY, ANY, ANY, VM],
        out_specs=(VM, VM, VM, VM, ANY, ANY),
        scratch_shapes=LINK_SCRATCH + [
            pltpu.VMEM((SLOTS, 2, GC, FC), BF), pltpu.VMEM((SLOTS, FC, GC), BF), pltpu.VMEM((2, LC, D), BF), pltpu.VMEM((LC, D), BF),
            pltpu.VMEM((12, B, 256), F32), pltpu.VMEM((B, FC), BF), pltpu.VMEM((3, LC, B), BF), pltpu.VMEM((LC, B), BF), pltpu.VMEM((LC, B), F32),
            pltpu.VMEM((LC + 64, B), BF),
            pltpu.SemaphoreType.DMA((SLOTS, 3)), pltpu.SemaphoreType.DMA((SLOTS,)), pltpu.SemaphoreType.DMA((2, G)), pltpu.SemaphoreType.DMA((G,)),
            pltpu.SemaphoreType.DMA((2,)), pltpu.SemaphoreType.DMA((3,)), pltpu.SemaphoreType.DMA,
        ],
        compiler_params=pltpu.CompilerParams(collective_id=0, has_side_effects=True, vmem_limit_bytes=67043328),
        cost_estimate=pl.CostEstimate(flops=30 * 10**9, bytes_accessed=400 * 10**6, transcendentals=0),
    )(x.reshape(4, 2, 32, D), scale, wxt, wyt, convt, lrut, wa, wi, pcols, tok, wout, rb, w1, b1, w2, b2, wd, mb, wq, wk, wv, tab)


def kernel_b(o_ref, x_ref, wo, bo_ref, sc_ref, w1, b1_ref, w2, b2_ref, wd, mb_ref, out_ref, *scratch):
    net = Links(*scratch[:NLINK])
    wu, wdb, wob, acc, h_s, us, ds, os, ls = scratch[NLINK:]
    f = lambda ref: ref[...].astype(F32)
    load_o = Ring([[pltpu.make_async_copy(wo.at[:, COLS[g]], wob.at[:, COLS[g]], os.at[g])] for g in range(G)], G)
    up = Ring([up_group(g, 2, g, w1, w2, wu, us) for g in range(G)], SLOTS)
    down = Ring([down_group(g, 2, g, wd, wdb, ds) for g in range(G)], SLOTS)
    load_o.fill(0)
    up.fill(0)
    down.fill(0)
    net.enter()
    net.xown[...] = x_ref[...]

    def produce(g):
        load_o.wait(g)
        net.dots(g, o_ref, wob.at[:, COLS[g]])

    net.reduce_scatter(produce, f(bo_ref))
    net.gather_start(rms(net.xown[...], f(sc_ref)[2, 1:2, :]))
    mlp_up(net, up, 0, wu, acc, h_s, f(b1_ref)[2:3], f(b2_ref)[2:3])
    mlp_down(net, down, 0, wdb, h_s, f(mb_ref)[2:3])
    net.gather_start(net.xown[...])
    stores = []

    def use(g):
        cp = pltpu.make_async_copy(net.n.at[:, COLS[g]], out_ref.at[:, COLS[g]], ls.at[g])
        cp.start()
        stores.append(cp)

    net.gathered(use)
    for cp in stores:
        cp.wait()


def last_layer(o, x_own, wo, bo, scale, w1, b1, w2, b2, wd, mb):
    return pl.pallas_call(
        kernel_b,
        name='last_layer',
        out_shape=jax.ShapeDtypeStruct((B, D), BF),
        in_specs=[VM, VM, ANY, VM, VM, ANY, VM, ANY, VM, ANY, VM],
        out_specs=ANY,
        scratch_shapes=LINK_SCRATCH + [
            pltpu.VMEM((SLOTS, 2, GC, FC), BF), pltpu.VMEM((SLOTS, FC, GC), BF), pltpu.VMEM((512, D), BF),
            pltpu.VMEM((12, B, 256), F32), pltpu.VMEM((B, FC), BF),
            pltpu.SemaphoreType.DMA((SLOTS, 3)), pltpu.SemaphoreType.DMA((SLOTS,)), pltpu.SemaphoreType.DMA((G,)), pltpu.SemaphoreType.DMA((G,)),
        ],
        compiler_params=pltpu.CompilerParams(collective_id=1, has_side_effects=True, vmem_limit_bytes=67043328),
        cost_estimate=pl.CostEstimate(flops=12 * 10**9, bytes_accessed=200 * 10**6, transcendentals=0),
    )(o, x_own, wo, bo, scale, w1, b1, w2, b2, wd, mb)


RA = 8


def attn_kernel(tok_ref, q_ref, kn_ref, vn_ref, slot_ref, k_ref, v_ref, o_ref, ko_ref, vo_ref, so_ref, s_s):
    i = pl.program_id(0)
    lane = lax.broadcasted_iota(jnp.int32, (1, W), 1)
    sub = lax.broadcasted_iota(jnp.int32, (16, HD), 0)
    kn = kn_ref[...].astype(F32)
    vn = vn_ref[...].astype(F32)
    ko_ref[...] = k_ref[...]
    vo_ref[...] = v_ref[...]
    for r in range(RA):
        tp = tok_ref[i * RA + r]
        slot = lax.rem(tp, W)
        base = pl.multiple_of((slot // 16) * 16, 16)
        hit = sub == (slot - base)
        ko_ref[r, pl.ds(base, 16), :] = jnp.where(hit, kn[r:r + 1], k_ref[r, pl.ds(base, 16), :].astype(F32)).astype(BF)
        vo_ref[r, pl.ds(base, 16), :] = jnp.where(hit, vn[r:r + 1], v_ref[r, pl.ds(base, 16), :].astype(F32)).astype(BF)
        so_ref[r:r + 1, :] = jnp.where(lane == slot, tp, slot_ref[r:r + 1, :])
    for r in range(RA):
        tp = tok_ref[i * RA + r]
        sn = so_ref[r:r + 1, :]
        age = tp - sn
        valid = (sn >= 0) & (age >= 0) & (age < W)
        s = lax.dot_general(q_ref[r], ko_ref[r], (((1,), (1,)), ((), ())), preferred_element_type=F32) * (HD ** -0.5)
        s_s[4 * r:4 * r + 4, :] = jnp.where(valid, s, -jnp.inf)
    s = s_s[...]
    e = jnp.exp(s - jnp.max(s, axis=-1, keepdims=True))
    s_s[...] = e / jnp.sum(e, axis=-1, keepdims=True)
    for r in range(RA):
        o_ref[r] = jnp.dot(s_s[4 * r:4 * r + 4, :].astype(BF), vo_ref[r], preferred_element_type=F32).astype(BF)


def attend(tok, q, kn, vn, slot_pos, kc, vc):
    cache = pl.BlockSpec((RA, W, HD), lambda i, t: (i, 0, 0))
    row = pl.BlockSpec((RA, HD), lambda i, t: (i, 0))
    slots = pl.BlockSpec((RA, W), lambda i, t: (i, 0))
    heads = pl.BlockSpec((RA, 4, HD), lambda i, t: (i, 0, 0))
    return pl.pallas_call(
        attn_kernel,
        name='attend',
        grid_spec=pltpu.PrefetchScalarGridSpec(
            num_scalar_prefetch=1,
            grid=(B // RA,),
            in_specs=[heads, row, row, slots, cache, cache],
            out_specs=(heads, cache, cache, slots),
            scratch_shapes=[pltpu.VMEM((4 * RA, W), F32)],
        ),
        out_shape=(jax.ShapeDtypeStruct((B, 4, HD), BF), jax.ShapeDtypeStruct(kc.shape, BF), jax.ShapeDtypeStruct(vc.shape, BF), jax.ShapeDtypeStruct(slot_pos.shape, jnp.int32)),
        cost_estimate=pl.CostEstimate(flops=4 * B * 4 * W * HD, bytes_accessed=8 * B * W * HD, transcendentals=0),
    )(tok, q, kn, vn, slot_pos, kc, vc)


def rope_tables(tok_pos):
    quarter = HD // 4
    inv_freq = ROPE_BASE ** (-jnp.arange(quarter, dtype=F32) / quarter)
    angles = tok_pos.astype(F32)[:, None] * inv_freq[None, :]
    cos, sin = jnp.cos(angles), jnp.sin(angles)
    one = jnp.ones_like(cos)
    zero = jnp.zeros_like(cos)
    keep = jnp.concatenate([cos, cos, one, one], axis=1)
    up = jnp.concatenate([-sin, zero, zero, zero], axis=1)
    down = jnp.concatenate([zero, sin, zero, zero], axis=1)
    return jnp.stack([keep, up, down])


def io_specs():
    in_specs = (P('dp', None), P('dp'), P(None, 'dp', None, 'tp'), P(None, 'dp', 'tp'), P('dp', None, None), P('dp', None, None), P('dp', None),
                P(), P(None, None, 'tp'), P(None, 'tp'), P(None, None, 'tp'), P(None, 'tp'), P(None, None, 'tp'), P(None, 'tp'),
                P(None, 'tp', None, None), P(None, 'tp'), P(None, 'tp', None, None), P(None, 'tp'), P(None, 'tp'), P(None, 'tp', None), P(),
                P(None, 'tp'), P(), P(), P('tp', None), P(),
                P(None, None, 'tp'), P(None, 'tp'), P(None, None, 'tp'), P(None, 'tp'), P(None, 'tp', None), P())
    out_specs = (P('dp', None), P(None, 'dp', None, 'tp'), P(None, 'dp', 'tp'), P('dp', None, None), P('dp', None, None), P('dp', None))
    return in_specs, out_specs


def solution(mesh):
    in_specs, out_specs = io_specs()

    def local_step(x_in, tok_pos, conv_state, lru_state, k_cache, v_cache, slot_pos, norm_scale, rec_wx, rec_bx, rec_wy, rec_by, conv_w, conv_b, gate_wa, gate_ba, gate_wi, gate_bi, a_param, rec_wout, rec_bout, attn_wq, attn_wk, attn_wv, attn_wo, attn_bo, mlp_w1, mlp_b1, mlp_w2, mlp_b2, mlp_wd, mlp_bd):
        wxt = jnp.swapaxes(rec_wx, 1, 2)
        wyt = jnp.swapaxes(rec_wy, 1, 2)
        convt = jnp.transpose(conv_state, (0, 2, 3, 1))
        lrut = jnp.swapaxes(lru_state, 1, 2)
        f = lambda v: v.astype(F32)
        pcols = jnp.stack([f(rec_bx), f(rec_by), f(conv_w[:, 0]), f(conv_w[:, 1]), f(conv_w[:, 2]), f(conv_w[:, 3]), f(conv_b), f(gate_ba), f(gate_bi), -8.0 * jax.nn.softplus(a_param)], axis=-1)
        tok_row = tok_pos[None, :]
        tab = rope_tables(tok_pos)

        q, kn, vn, x_own, convs, lrus = first_layers(x_in, norm_scale, wxt, wyt, convt, lrut, gate_wa, gate_wi, pcols, tok_row, rec_wout, rec_bout, mlp_w1, mlp_b1, mlp_w2, mlp_b2, mlp_wd, mlp_bd, attn_wq, attn_wk, attn_wv, tab)
        o, k_next, v_next, slot_next = attend(tok_pos, jnp.swapaxes(q, 0, 1), kn, vn, slot_pos, k_cache, v_cache)
        x = last_layer(o.reshape(B, 512), x_own, attn_wo, attn_bo[None, :], norm_scale, mlp_w1, mlp_b1, mlp_w2, mlp_b2, mlp_wd, mlp_bd)
        conv_out = jnp.transpose(convs, (0, 3, 1, 2))
        lru_out = jnp.swapaxes(lrus, 1, 2)
        return (x, conv_out, lru_out, k_next, v_next, slot_next)

    return jax.shard_map(local_step, mesh=mesh, in_specs=in_specs, out_specs=out_specs, check_vma=False)
```

```python
import functools

import jax
import jax.numpy as jnp
from jax import lax
from jax.experimental import pallas as pl
from jax.experimental.pallas import tpu as pltpu
from jax.sharding import PartitionSpec as P

ROPE_BASE = 10000.0
NORM_EPS = 1e-6
MESH = pl.DeviceIdType.MESH
BF = jnp.bfloat16
F32 = jnp.float32
ANY = pl.BlockSpec(memory_space=pl.ANY)
VM = pl.BlockSpec(memory_space=pltpu.VMEM)
B = 256
D = 4096
LC = 704
FC = 1536
W = 1024
HD = 128
G = 8
KC = 1024
NK = D // KC
GC = D // G


def rms(x, scale):
    xf = x.astype(F32)
    mean_sq = jnp.mean(xf * xf, axis=-1, keepdims=True)
    return (xf * lax.rsqrt(mean_sq + NORM_EPS) * (1.0 + scale.astype(F32))).astype(BF)


NT = (((1,), (1,)), ((), ()))
TN = (((0,), (0,)), ((), ()))
COLS = [pl.ds(g * GC, GC) for g in range(G)]
KCOLS = [pl.ds(k * KC, KC) for k in range(NK)]
PIECES = {1: (0, 1024), 3: (1024, 1024), 5: (2048, 1024), 6: (3072, 512), 7: (3584, 512)}


def chunk(g):
    return pl.ds(pl.multiple_of(g * GC, GC), GC)


class Links:
    def __init__(self, part, recv1, recv2, own, n, xown, s1s, s1r, s2s, s2r, s3s, s3r, s4s, s4r):
        self.part, self.recv1, self.recv2, self.own, self.n, self.xown = part, recv1, recv2, own, n, xown
        self.s1s, self.s1r, self.s2s, self.s2r, self.s3s, self.s3r, self.s4s, self.s4r = s1s, s1r, s2s, s2r, s3s, s3r, s4s, s4r
        t = lax.axis_index('tp')
        y, x = t // 4, (t // 2) % 2
        self.c = t % 2
        self.q = 2 * y + x
        self.partner = 2 * self.q + 1 - self.c
        self.chips = [2 * y + (1 - x), 2 * (1 - y) + x, 2 * (1 - y) + (1 - x)]
        self.peers = [2 * qd + self.c for qd in self.chips]

    def enter(self):
        barrier = pltpu.get_barrier_semaphore()
        for dev in [self.partner] + self.peers:
            pl.semaphore_signal(barrier, inc=1, device_id={'tp': dev}, device_id_type=MESH)
        pl.semaphore_wait(barrier, 4)

    def remote(self, src, dst, ss, rs, dev):
        return pltpu.make_async_remote_copy(src_ref=src, dst_ref=dst, send_sem=ss, recv_sem=rs, device_id={'tp': dev}, device_id_type=MESH)

    def dots(self, g, lhs, rhs):
        out = jnp.dot(lhs[...], rhs[...], preferred_element_type=F32)
        self.part[:, :, :, chunk(g)] = out.astype(BF).reshape(4, 2, 32, GC)

    def to_partner(self, g):
        return self.remote(self.part.at[:, 1 - self.c, :, chunk(g)], self.recv1.at[:, :, chunk(g)], self.s1s.at[g], self.s1r.at[g], self.partner)

    def to_owner(self, g, k):
        return self.remote(self.part.at[self.chips[k], self.c, :, chunk(g)], self.recv2.at[k, :, chunk(g)], self.s2s.at[g, k], self.s2r.at[g, k], self.peers[k])

    def reduce_scatter(self, produce, bias_ref, layer):
        c, q, chips = self.c, self.q, self.chips

        def pair(g):
            cols = chunk(g)
            self.to_partner(g).wait_recv()
            for k in (2, 0, 1):
                s = self.part[chips[k], c, :, cols].astype(F32) + self.recv1[chips[k], :, cols].astype(F32)
                self.part[chips[k], c, :, cols] = s.astype(BF)
                self.to_owner(g, k).start()
            self.own[:, cols] = self.part[q, c, :, cols].astype(F32) + self.recv1[q, :, cols].astype(F32)

        def step(k, carry):
            produce(k, 0)
            self.to_partner(2 * k).start()

            @pl.when(k > 0)
            def _():
                pair(2 * k - 1)

            produce(k, 1)
            self.to_partner(2 * k + 1).start()
            pair(2 * k)
            return carry

        lax.fori_loop(0, NK, step, 0)
        pair(G - 1)

        def final(g, carry):
            cols = chunk(g)
            for k in range(3):
                self.to_owner(g, k).wait_recv()
            tot = self.own[:, cols]
            for k in range(3):
                tot = tot + self.recv2[k, :, cols].astype(F32)
            bias = bias_ref[:, cols].astype(F32)[layer:layer + 1]
            self.xown[:, cols] = (self.xown[:, cols].astype(F32) + tot.astype(BF).astype(F32) + bias).astype(BF)
            return carry

        lax.fori_loop(0, G, final, 0)

        def sent(g, carry):
            self.to_partner(g).wait_send()
            for k in range(3):
                self.to_owner(g, k).wait_send()
            return carry

        lax.fori_loop(0, G, sent, 0)

    def place(self, dev, g):
        return self.n.at[pl.ds(pl.multiple_of(dev * 32, 32), 32), chunk(g)]

    def from_own(self, g, k):
        ref = self.place(2 * self.q + self.c, g)
        return self.remote(ref, ref, self.s3s.at[g, k], self.s3r.at[g, k], self.peers[k] if k < 3 else self.partner)

    def pass_on(self, g, k):
        ref = self.place(self.peers[k], g)
        return self.remote(ref, ref, self.s4s.at[g, k], self.s4r.at[g, k], self.partner)

    def gather_start(self, rows):
        self.n[pl.ds(pl.multiple_of((2 * self.q + self.c) * 32, 32), 32), :] = rows

        def send(g, carry):
            for k in (2, 0, 1, 3):
                self.from_own(g, k).start()
            return carry

        lax.fori_loop(0, G, send, 0)

    def gather_forward(self, g):
        for k in range(3):
            self.from_own(g, k).wait_recv()
            self.pass_on(g, k).start()

    def gather_ready(self, g):
        self.from_own(g, 3).wait_recv()
        for k in range(3):
            self.pass_on(g, k).wait_recv()

    def gather_finish(self):
        def sent(g, carry):
            for k in range(4):
                self.from_own(g, k).wait_send()
            for k in range(3):
                self.pass_on(g, k).wait_send()
            return carry

        lax.fori_loop(0, G, sent, 0)

    def gathered(self, use_piece, fresh=False):
        def use(g):
            if g in PIECES:
                use_piece(*PIECES[g])

        for g in range(G):
            if not fresh:
                self.gather_forward(g)
            if g >= 1:
                if not fresh:
                    self.gather_ready(g - 1)
                use(g - 1)
        if not fresh:
            self.gather_ready(G - 1)
        use(G - 1)
        if not fresh:
            self.gather_finish()


LINK_SCRATCH = [
    pltpu.VMEM((4, 2, 32, D), BF), pltpu.VMEM((4, 32, D), BF), pltpu.VMEM((3, 32, D), BF),
    pltpu.VMEM((32, D), F32), pltpu.VMEM((B, D), BF), pltpu.VMEM((32, D), BF),
    pltpu.SemaphoreType.DMA((G,)), pltpu.SemaphoreType.DMA((G,)), pltpu.SemaphoreType.DMA((G, 3)), pltpu.SemaphoreType.DMA((G, 3)),
    pltpu.SemaphoreType.DMA((G, 4)), pltpu.SemaphoreType.DMA((G, 4)), pltpu.SemaphoreType.DMA((G, 3)), pltpu.SemaphoreType.DMA((G, 3)),
]
NLINK = len(LINK_SCRATCH)


class Stream:
    def __init__(self, group, total, depth):
        self.group, self.total, self.depth = group, total, depth

    def begin(self):
        for k in range(self.depth):
            self.group(k).start()

    def wait(self, k):
        self.group(k).wait()

    def done(self, k):
        @pl.when(k + self.depth < self.total)
        def _():
            self.group(k + self.depth).start()


class Ring:
    def __init__(self, groups, depth):
        self.groups, self.depth, self.issued = groups, depth, 0

    def fill(self, used):
        while self.issued < min(used + self.depth, len(self.groups)):
            for cp in self.groups[self.issued]:
                cp.start()
            self.issued += 1

    def wait(self, k):
        for cp in self.groups[k]:
            cp.wait()


SLOTS = 3


def up_group(k, layer, g, w1, w2, wu, sems):
    s = k % SLOTS
    rows = KCOLS[g]
    return [pltpu.make_async_copy(w1.at[layer, rows, :], wu.at[s, 0], sems.at[s, 0]), pltpu.make_async_copy(w2.at[layer, rows, :], wu.at[s, 1], sems.at[s, 1])]


def down_stream(first, count, wd, wdb, sems):
    def group(k):
        s = lax.rem(k, SLOTS)
        return pltpu.make_async_copy(wd.at[first + k // NK, :, pl.ds(pl.multiple_of(lax.rem(k, NK) * KC, KC), KC)], wdb.at[s], sems.at[s])

    return Stream(group, count * NK, SLOTS)


def wide_stream(src, dst, sems):
    def group(k):
        cols = pl.ds(pl.multiple_of(k * KC, KC), KC)
        return pltpu.make_async_copy(src.at[:, cols], dst.at[:, cols], sems.at[k])

    return Stream(group, NK, NK)


def mlp_up(net, ring, k0, wu, acc, h_s, b1_ref, b2_ref, layer):
    def use(start, size):
        k = k0 + start // KC
        s = k % SLOTS
        off = start % KC
        if off == 0:
            ring.wait(k)
        ng = net.n[:, start:start + size]
        last = start + size == D

        def body(j, carry):
            lanes = pl.ds(pl.multiple_of(j * 512, 512), 512)
            for p in range(2):
                pieces = []
                for half in range(2):
                    sub = pl.ds(pl.multiple_of(j * 512 + p * 256, 256), 256)
                    a = jnp.dot(ng, wu[s, half, off:off + size, sub], preferred_element_type=F32)
                    at = 6 * half + 2 * j + p
                    a = a if start == 0 else acc[at] + a
                    if last:
                        pieces.append(a)
                    else:
                        acc[at] = a
                if last:
                    b1 = b1_ref[:, sub].astype(F32)[layer:layer + 1]
                    b2 = b2_ref[:, sub].astype(F32)[layer:layer + 1]
                    h_s[:, sub] = (jax.nn.gelu(pieces[0] + b1, approximate=True) * (pieces[1] + b2)).astype(BF)
            return carry

        lax.fori_loop(0, FC // 512, body, 0)
        if off + size == KC:
            ring.fill(k + 1)

    net.gathered(use)


def mlp_down(net, stream, k0, wdb, h_s, bias_ref, layer):
    def produce(k, u):
        if u == 0:
            stream.wait(k0 + k)
        net.dots(2 * k + u, h_s, wdb.at[lax.rem(k0 + k, SLOTS), :, u * GC:u * GC + GC])
        if u == 1:
            stream.done(k0 + k)

    net.reduce_scatter(produce, bias_ref, layer)


def rope(v, tab_ref):
    keep_ref, turn_ref = tab_ref
    lane = lax.broadcasted_iota(jnp.int32, v.shape, 1)
    return v * keep_ref[...] + jnp.where(lane < 32, pltpu.roll(v, 96, 1), pltpu.roll(v, 32, 1)) * turn_ref[...]


def kernel_a(x_ref, sc_ref, wx, wy, conv, lru, wa_ref, wi_ref, bx_ref, by_ref, cw_ref, cb_ref, ba_ref, bi_ref, sp_ref, tok_ref, wout, rb_ref, w1, b1_ref, w2, b2_ref, wd, mb_ref, wq, wk, wv, keep_ref, turn_ref,
             q_ref, k_ref, v_ref, xo_ref, conv_out, lru_out, *scratch):
    net = Links(*scratch[:NLINK])
    wu, wdb, wxb, wob, acc, h_s, conv_s, xb_s, lru_s, ht_s, prow, pcol, us, ds, xs, os, ss, ts, ls = scratch[NLINK:]
    f = lambda ref: ref[...].astype(F32)

    load_x = pltpu.make_async_copy(x_ref, net.part, ls)
    load_x.start()
    rec_in = [Ring([[pltpu.make_async_copy(wx.at[l, :, KCOLS[g]], wxb.at[0, :, KCOLS[g]], xs.at[0, g]), pltpu.make_async_copy(wy.at[l, :, KCOLS[g]], wxb.at[1, :, KCOLS[g]], xs.at[1, g])] for g in range(NK)], NK) for l in range(2)]
    rec_out = [wide_stream(wout.at[l], wob, os) for l in range(2)]
    state_in = [[pltpu.make_async_copy(conv.at[l], conv_s, ss.at[0]), pltpu.make_async_copy(lru.at[l], lru_s, ss.at[1])] for l in range(2)]
    state_out = [[pltpu.make_async_copy(conv_s.at[1:3], conv_out.at[l, 0:2], ts.at[0]), pltpu.make_async_copy(xb_s, conv_out.at[l, 2], ts.at[1]), pltpu.make_async_copy(lru_s, lru_out.at[l], ts.at[2])] for l in range(2)]
    ups = [up_group(4 * l + g, l, g, w1, w2, wu, us) for l in range(2) for g in range(NK)]
    for g in range(NK):
        s = (8 + g) % SLOTS
        rows = KCOLS[g]
        ups.append([pltpu.make_async_copy(wq.at[rows, :], wu.at[s, 0, :, 0:512], us.at[s, 0]), pltpu.make_async_copy(wk.at[rows, :], wu.at[s, 0, :, 512:640], us.at[s, 1]),
                    pltpu.make_async_copy(wv.at[rows, :], wu.at[s, 0, :, 640:768], us.at[s, 2])])
    up = Ring(ups, SLOTS)
    down = down_stream(0, 2, wd, wdb, ds)

    rec_in[0].fill(0)
    for cp in state_in[0]:
        cp.start()
    rec_out[0].begin()
    net.enter()
    load_x.wait()
    for j in range(8):
        net.n[32 * j:32 * j + 32, :] = rms(net.part[j // 2, j % 2], f(sc_ref)[0, 0:1, :])
    net.xown[...] = net.part[net.q, net.c]
    tok = tok_ref[...]
    fresh = tok == 0

    for layer in range(2):
        def use(start, size):
            if start % KC == 0:
                rec_in[layer].wait(start // KC)
            ng = net.n[:, start:start + size]
            for half in range(2):
                r = lax.dot_general(wxb[half, :, start:start + size], ng, NT, preferred_element_type=F32)
                for h in range(4):
                    piece = r[176 * h:176 * h + 176]
                    acc[4 * half + h, 0:176, :] = piece if start == 0 else acc[4 * half + h, 0:176, :] + piece

        net.gathered(use, fresh=layer == 0)
        if layer == 0:
            up.fill(0)
            down.begin()
            rec_in[1].fill(0)
        row = lambda ref: ref[...].astype(F32)[layer:layer + 1]
        cw = cw_ref[...].astype(F32)
        params = [row(bx_ref), row(by_ref)] + [cw[layer, j:j + 1, :] for j in range(4)] + [row(cb_ref), row(ba_ref), row(bi_ref), row(sp_ref)]
        for j, p in enumerate(params):
            prow[j:j + 1, 0:LC] = p
        pcol[...] = prow[...].T
        for cp in state_in[layer]:
            cp.wait()
        for h in range(4):
            rows = slice(176 * h, 176 * h + 176)
            pc = pcol[rows, :]
            col = lambda k: pc[:, k:k + 1]
            xb = (acc[h, 0:176, :] + col(0)).astype(BF)
            yb = jax.nn.gelu(acc[4 + h, 0:176, :] + col(1), approximate=True)
            xb_s[rows, :] = xb
            hist = jnp.zeros((176, B), F32)
            for j in range(3):
                hist = hist + jnp.where(tok >= 3 - j, conv_s[j, rows, :].astype(F32), 0.0) * col(5 - j)
            xc = (col(6) + col(2) * xb.astype(F32) + hist).astype(BF)
            rg = jax.nn.sigmoid(lax.dot_general(wa_ref[layer, h], xc, TN, preferred_element_type=F32) + col(7))
            ig = jax.nn.sigmoid(lax.dot_general(wi_ref[layer, h], xc, TN, preferred_element_type=F32) + col(8))
            a = jnp.exp(rg * col(9))
            sc = jnp.sqrt(1.0 - a * a)
            a = jnp.where(fresh, 0.0, a)
            sc = jnp.where(fresh, 1.0, sc)
            hn = a * lru_s[rows, :] + sc * ig * xc.astype(F32)
            lru_s[rows, :] = hn
            ht_s[rows, :] = (hn * yb).astype(BF)
        for cp in state_out[layer]:
            cp.start()
        ht_s[LC:, :] = jnp.zeros((64, B), BF)
        h_s[:, :LC + 64] = ht_s[...].T

        def produce(k, u):
            if u == 0:
                rec_out[layer].wait(k)
            net.dots(2 * k + u, h_s.at[:, :LC], wob.at[:, chunk(2 * k + u)])

        net.reduce_scatter(produce, rb_ref, layer)
        net.gather_start(rms(net.xown[...], f(sc_ref)[layer, 1:2, :]))
        for cp in state_out[layer]:
            cp.wait()
        if layer == 0:
            rec_out[1].begin()
            for cp in state_in[1]:
                cp.start()
        mlp_up(net, up, 4 * layer, wu, acc, h_s, b1_ref, b2_ref, layer)
        mlp_down(net, down, 4 * layer, wdb, h_s, mb_ref, layer)
        net.gather_start(rms(net.xown[...], f(sc_ref)[layer + 1, 0:1, :]))

    xo_ref[...] = net.xown[...]

    def use_q(start, size):
        k = 8 + start // KC
        off = start % KC
        if off == 0:
            up.wait(k)
        ng = net.n[:, start:start + size]
        for j in range(3):
            a = jnp.dot(ng, wu[k % SLOTS, 0, off:off + size, 256 * j:256 * j + 256], preferred_element_type=F32)
            acc[j] = a if start == 0 else acc[j] + a
        if off + size == KC:
            up.fill(k + 1)

    net.gathered(use_q)
    for h in range(4):
        q_ref[:, 128 * h:128 * h + 128] = rope(acc[h // 2, :, 128 * (h % 2):128 * (h % 2) + 128], (keep_ref, turn_ref)).astype(BF)
    k_ref[...] = rope(acc[2, :, 0:128], (keep_ref, turn_ref)).astype(BF)
    v_ref[...] = acc[2, :, 128:256].astype(BF)


def first_layers(x, scale, wxt, wyt, convt, lrut, wa, wi, bx, by, cw, cb, ba, bi, sp, tok, wout, rb, w1, b1, w2, b2, wd, mb, wq, wk, wv, keep, turn):
    return pl.pallas_call(
        kernel_a,
        name='first_layers',
        out_shape=(jax.ShapeDtypeStruct((B, 4 * HD), BF), jax.ShapeDtypeStruct((B, HD), BF), jax.ShapeDtypeStruct((B, HD), BF), jax.ShapeDtypeStruct((32, D), BF),
                   jax.ShapeDtypeStruct(convt.shape, BF), jax.ShapeDtypeStruct(lrut.shape, F32)),
        in_specs=[ANY, VM, ANY, ANY, ANY, ANY, VM, VM] + [VM] * 7 + [VM, ANY, VM, ANY, VM, ANY, VM, ANY, VM, ANY, ANY, ANY, VM, VM],
        out_specs=(VM, VM, VM, VM, ANY, ANY),
        scratch_shapes=LINK_SCRATCH + [
            pltpu.VMEM((SLOTS, 2, KC, FC), BF), pltpu.VMEM((SLOTS, FC, KC), BF), pltpu.VMEM((2, LC, D), BF), pltpu.VMEM((LC, D), BF),
            pltpu.VMEM((12, B, 256), F32), pltpu.VMEM((B, FC), BF), pltpu.VMEM((3, LC, B), BF), pltpu.VMEM((LC, B), BF), pltpu.VMEM((LC, B), F32),
            pltpu.VMEM((LC + 64, B), BF), pltpu.VMEM((16, LC + 64), F32), pltpu.VMEM((LC + 64, 16), F32),
            pltpu.SemaphoreType.DMA((SLOTS, 3)), pltpu.SemaphoreType.DMA((SLOTS,)), pltpu.SemaphoreType.DMA((2, NK)), pltpu.SemaphoreType.DMA((NK,)),
            pltpu.SemaphoreType.DMA((2,)), pltpu.SemaphoreType.DMA((3,)), pltpu.SemaphoreType.DMA,
        ],
        compiler_params=pltpu.CompilerParams(collective_id=0, has_side_effects=True, vmem_limit_bytes=67043328),
        cost_estimate=pl.CostEstimate(flops=30 * 10**9, bytes_accessed=400 * 10**6, transcendentals=0),
    )(x.reshape(4, 2, 32, D), scale, wxt, wyt, convt, lrut, wa, wi, bx, by, cw, cb, ba, bi, sp, tok, wout, rb, w1, b1, w2, b2, wd, mb, wq, wk, wv, keep, turn)


def kernel_b(o_ref, x_ref, wo, bo_ref, sc_ref, w1, b1_ref, w2, b2_ref, wd, mb_ref, out_ref, *scratch):
    net = Links(*scratch[:NLINK])
    wu, wdb, wob, acc, h_s, us, ds, os, ls = scratch[NLINK:]
    f = lambda ref: ref[...].astype(F32)
    load_o = wide_stream(wo, wob, os)
    up = Ring([up_group(g, 2, g, w1, w2, wu, us) for g in range(NK)], SLOTS)
    down = down_stream(2, 1, wd, wdb, ds)
    load_o.begin()
    up.fill(0)
    down.begin()
    net.enter()
    net.xown[...] = x_ref[...]

    def produce(k, u):
        if u == 0:
            load_o.wait(k)
        net.dots(2 * k + u, o_ref, wob.at[:, chunk(2 * k + u)])

    net.reduce_scatter(produce, bo_ref, 0)
    net.gather_start(rms(net.xown[...], f(sc_ref)[2, 1:2, :]))
    mlp_up(net, up, 0, wu, acc, h_s, b1_ref, b2_ref, 2)
    mlp_down(net, down, 0, wdb, h_s, mb_ref, 2)
    net.gather_start(net.xown[...])
    stores = []

    def use(start, size):
        cp = pltpu.make_async_copy(net.n.at[:, start:start + size], out_ref.at[:, start:start + size], ls.at[len(stores)])
        cp.start()
        stores.append(cp)

    net.gathered(use)
    for cp in stores:
        cp.wait()


def last_layer(o, x_own, wo, bo, scale, w1, b1, w2, b2, wd, mb):
    return pl.pallas_call(
        kernel_b,
        name='last_layer',
        out_shape=jax.ShapeDtypeStruct((B, D), BF),
        in_specs=[VM, VM, ANY, VM, VM, ANY, VM, ANY, VM, ANY, VM],
        out_specs=ANY,
        scratch_shapes=LINK_SCRATCH + [
            pltpu.VMEM((SLOTS, 2, KC, FC), BF), pltpu.VMEM((SLOTS, FC, KC), BF), pltpu.VMEM((512, D), BF),
            pltpu.VMEM((12, B, 256), F32), pltpu.VMEM((B, FC), BF),
            pltpu.SemaphoreType.DMA((SLOTS, 3)), pltpu.SemaphoreType.DMA((SLOTS,)), pltpu.SemaphoreType.DMA((G,)), pltpu.SemaphoreType.DMA((G,)),
        ],
        compiler_params=pltpu.CompilerParams(collective_id=1, has_side_effects=True, vmem_limit_bytes=67043328),
        cost_estimate=pl.CostEstimate(flops=12 * 10**9, bytes_accessed=200 * 10**6, transcendentals=0),
    )(o, x_own, wo, bo, scale, w1, b1, w2, b2, wd, mb)


RA = 8
NB = 6
STEPS = B // RA


def attn_kernel(tok_ref, q_ref, kn_ref, vn_ref, slot_ref, k_ref, v_ref, o_ref, ko_ref, vo_ref, so_ref, kb, vb, s_s, q_s, o_s, isem, osem):
    lane = lax.broadcasted_iota(jnp.int32, (1, W), 1)
    sub = lax.broadcasted_iota(jnp.int32, (16, HD), 0)

    def copies(step, out):
        b = lax.rem(step, NB)
        rows = pl.ds(pl.multiple_of(step * RA, RA), RA)
        if out:
            return [pltpu.make_async_copy(kb.at[b], ko_ref.at[rows], osem.at[0, b]), pltpu.make_async_copy(vb.at[b], vo_ref.at[rows], osem.at[1, b])]
        return [pltpu.make_async_copy(k_ref.at[rows], kb.at[b], isem.at[0, b]), pltpu.make_async_copy(v_ref.at[rows], vb.at[b], isem.at[1, b])]

    def start(step):
        for cp in copies(step, False):
            cp.start()

    lax.fori_loop(0, NB - 2, lambda step, c: (start(step), c)[1], 0)

    def step_fn(i, carry):
        b = lax.rem(i, NB)
        rows = pl.ds(pl.multiple_of(i * RA, RA), RA)
        ahead = i + NB - 2

        @pl.when(ahead < STEPS)
        def _():
            @pl.when(ahead >= NB)
            def _():
                for cp in copies(ahead - NB, True):
                    cp.wait()
            start(ahead)

        for cp in copies(i, False):
            cp.wait()
        kn = kn_ref[rows, :].astype(F32)
        vn = vn_ref[rows, :].astype(F32)
        for h in range(4):
            q_s[pl.ds(h, RA, stride=4), :] = q_ref[rows, 128 * h:128 * h + 128].astype(F32)
        slots = slot_ref[rows, :]
        new_rows = []
        for r in range(RA):
            tp = tok_ref[i * RA + r]
            slot = lax.rem(tp, W)
            base = pl.multiple_of((slot // 16) * 16, 16)
            hit = sub == (slot - base)
            spot = pl.ds(base, 16)
            kb[b, r, spot, :] = jnp.where(hit, kn[r:r + 1], kb[b, r, spot, :].astype(F32)).astype(BF)
            vb[b, r, spot, :] = jnp.where(hit, vn[r:r + 1], vb[b, r, spot, :].astype(F32)).astype(BF)
            sn = jnp.where(lane == slot, tp, slots[r:r + 1])
            new_rows.append((tp, sn))
        for r in range(RA):
            tp, sn = new_rows[r]
            so_ref[pl.ds(i * RA + r, 1), :] = sn
            age = tp - sn
            valid = (sn >= 0) & (age >= 0) & (age < W)
            s = lax.dot_general(q_s[4 * r:4 * r + 4, :].astype(BF), kb[b, r], NT, preferred_element_type=F32) * (HD ** -0.5)
            s_s[4 * r:4 * r + 4, :] = jnp.where(valid, s, -jnp.inf)
        s = s_s[...]
        e = jnp.exp(s - jnp.max(s, axis=-1, keepdims=True))
        s_s[...] = e / jnp.sum(e, axis=-1, keepdims=True)
        for r in range(RA):
            o_s[4 * r:4 * r + 4, :] = jnp.dot(s_s[4 * r:4 * r + 4, :].astype(BF), vb[b, r], preferred_element_type=F32)
        for h in range(4):
            o_ref[rows, 128 * h:128 * h + 128] = o_s[pl.ds(h, RA, stride=4), :].astype(BF)
        for cp in copies(i, True):
            cp.start()
        return carry

    lax.fori_loop(0, STEPS, step_fn, 0)
    for step in range(STEPS - NB, STEPS):
        for cp in copies(step, True):
            cp.wait()


def attend(tok, q, kn, vn, slot_pos, kc, vc):
    return pl.pallas_call(
        attn_kernel,
        name='attend',
        in_specs=[pl.BlockSpec(memory_space=pltpu.SMEM), VM, VM, VM, VM, ANY, ANY],
        out_specs=(VM, ANY, ANY, VM),
        out_shape=(jax.ShapeDtypeStruct((B, 4 * HD), BF), jax.ShapeDtypeStruct(kc.shape, BF), jax.ShapeDtypeStruct(vc.shape, BF), jax.ShapeDtypeStruct(slot_pos.shape, jnp.int32)),
        scratch_shapes=[pltpu.VMEM((NB, RA, W, HD), BF), pltpu.VMEM((NB, RA, W, HD), BF), pltpu.VMEM((4 * RA, W), F32), pltpu.VMEM((4 * RA, HD), F32), pltpu.VMEM((4 * RA, HD), F32),
                        pltpu.SemaphoreType.DMA((2, NB)), pltpu.SemaphoreType.DMA((2, NB))],
        cost_estimate=pl.CostEstimate(flops=4 * B * 4 * W * HD, bytes_accessed=8 * B * W * HD, transcendentals=0),
    )(tok, q, kn, vn, slot_pos, kc, vc)


def rope_tables(tok_pos):
    quarter = HD // 4
    lane = lax.broadcasted_iota(jnp.int32, (1, HD), 1)
    inv_freq = ROPE_BASE ** (-(lane % quarter).astype(F32) / quarter)
    angles = tok_pos.astype(F32)[:, None] * inv_freq
    cos, sin = jnp.cos(angles), jnp.sin(angles)
    return jnp.where(lane < 2 * quarter, cos, 1.0), jnp.where(lane < quarter, -sin, jnp.where(lane < 2 * quarter, sin, 0.0))


def io_specs():
    in_specs = (P('dp', None), P('dp'), P(None, 'dp', None, 'tp'), P(None, 'dp', 'tp'), P('dp', None, None), P('dp', None, None), P('dp', None),
                P(), P(None, None, 'tp'), P(None, 'tp'), P(None, None, 'tp'), P(None, 'tp'), P(None, None, 'tp'), P(None, 'tp'),
                P(None, 'tp', None, None), P(None, 'tp'), P(None, 'tp', None, None), P(None, 'tp'), P(None, 'tp'), P(None, 'tp', None), P(),
                P(None, 'tp'), P(), P(), P('tp', None), P(),
                P(None, None, 'tp'), P(None, 'tp'), P(None, None, 'tp'), P(None, 'tp'), P(None, 'tp', None), P())
    out_specs = (P('dp', None), P(None, 'dp', None, 'tp'), P(None, 'dp', 'tp'), P('dp', None, None), P('dp', None, None), P('dp', None))
    return in_specs, out_specs


def solution(mesh):
    in_specs, out_specs = io_specs()

    def local_step(x_in, tok_pos, conv_state, lru_state, k_cache, v_cache, slot_pos, norm_scale, rec_wx, rec_bx, rec_wy, rec_by, conv_w, conv_b, gate_wa, gate_ba, gate_wi, gate_bi, a_param, rec_wout, rec_bout, attn_wq, attn_wk, attn_wv, attn_wo, attn_bo, mlp_w1, mlp_b1, mlp_w2, mlp_b2, mlp_wd, mlp_bd):
        wxt = jnp.swapaxes(rec_wx, 1, 2)
        wyt = jnp.swapaxes(rec_wy, 1, 2)
        convt = jnp.transpose(conv_state, (0, 2, 3, 1))
        lrut = jnp.swapaxes(lru_state, 1, 2)
        tok_row = tok_pos[None, :]
        tab = rope_tables(tok_pos)

        q, kn, vn, x_own, convs, lrus = first_layers(x_in, norm_scale, wxt, wyt, convt, lrut, gate_wa, gate_wi, rec_bx, rec_by, conv_w, conv_b, gate_ba, gate_bi, -8.0 * jax.nn.softplus(a_param), tok_row, rec_wout, rec_bout, mlp_w1, mlp_b1, mlp_w2, mlp_b2, mlp_wd, mlp_bd, attn_wq, attn_wk, attn_wv, *tab)
        o, k_next, v_next, slot_next = attend(tok_pos, q, kn, vn, slot_pos, k_cache, v_cache)
        x = last_layer(o, x_own, attn_wo, attn_bo[None, :], norm_scale, mlp_w1, mlp_b1, mlp_w2, mlp_b2, mlp_wd, mlp_bd)
        conv_out = jnp.transpose(convs, (0, 3, 1, 2))
        lru_out = jnp.swapaxes(lrus, 1, 2)
        return (x, conv_out, lru_out, k_next, v_next, slot_next)

    return jax.shard_map(local_step, mesh=mesh, in_specs=in_specs, out_specs=out_specs, check_vma=False)
```

```python
import functools

import jax
import jax.numpy as jnp
from jax import lax
from jax.experimental import pallas as pl
from jax.experimental.pallas import tpu as pltpu
from jax.sharding import PartitionSpec as P

ROPE_BASE = 10000.0
NORM_EPS = 1e-6
MESH = pl.DeviceIdType.MESH
BF = jnp.bfloat16
F32 = jnp.float32
ANY = pl.BlockSpec(memory_space=pl.ANY)
VM = pl.BlockSpec(memory_space=pltpu.VMEM)
B = 256
D = 4096
LC = 704
FC = 1536
W = 1024
HD = 128
G = 4
HB = 128
OR = 16
GC = D // G


def rms(x, scale):
    xf = x.astype(F32)
    mean_sq = jnp.mean(xf * xf, axis=-1, keepdims=True)
    return (xf * lax.rsqrt(mean_sq + NORM_EPS) * (1.0 + scale.astype(F32))).astype(BF)


NT = (((1,), (1,)), ((), ()))
TN = (((0,), (0,)), ((), ()))
DMA = pltpu.SemaphoreType.DMA


def chunk(g):
    return pl.ds(pl.multiple_of(g * GC, GC), GC)


class Links:
    def __init__(self, part, recv1, recv2, own, n, xown, s1s, s1r, s2s, s2r, s3s, s3r, s4s, s4r):
        self.part, self.recv1, self.recv2, self.own, self.n, self.xown = part, recv1, recv2, own, n, xown
        self.s1s, self.s1r, self.s2s, self.s2r, self.s3s, self.s3r, self.s4s, self.s4r = s1s, s1r, s2s, s2r, s3s, s3r, s4s, s4r
        t = lax.axis_index('tp')
        y, x = t // 4, (t // 2) % 2
        self.c = t % 2
        self.q = 2 * y + x
        self.partner = 2 * self.q + 1 - self.c
        self.chips = [2 * y + (1 - x), 2 * (1 - y) + x, 2 * (1 - y) + (1 - x)]
        self.peers = [2 * qd + self.c for qd in self.chips]

    def enter(self):
        barrier = pltpu.get_barrier_semaphore()
        for dev in [self.partner] + self.peers:
            pl.semaphore_signal(barrier, inc=1, device_id={'tp': dev}, device_id_type=MESH)
        pl.semaphore_wait(barrier, 4)

    def remote(self, src, dst, ss, rs, dev):
        return pltpu.make_async_remote_copy(src_ref=src, dst_ref=dst, send_sem=ss, recv_sem=rs, device_id={'tp': dev}, device_id_type=MESH)

    def to_partner(self, h, g):
        return self.remote(self.part.at[h, :, 1 - self.c, :, chunk(g)], self.recv1.at[h, :, :, chunk(g)], self.s1s.at[h, g], self.s1r.at[h, g], self.partner)

    def to_owner(self, h, g, k):
        return self.remote(self.part.at[h, self.chips[k], self.c, :, chunk(g)], self.recv2.at[h, k, :, chunk(g)], self.s2s.at[h, g, k], self.s2r.at[h, g, k], self.peers[k])

    def place(self, h, dev, g):
        return self.n.at[h, pl.ds(pl.multiple_of(dev * OR, OR), OR), chunk(g)]

    def from_own(self, h, g, k):
        ref = self.place(h, 2 * self.q + self.c, g)
        return self.remote(ref, ref, self.s3s.at[h, g, k], self.s3r.at[h, g, k], self.peers[k] if k < 3 else self.partner)

    def pass_on(self, h, g, k):
        ref = self.place(h, self.peers[k], g)
        return self.remote(ref, ref, self.s4s.at[h, g, k], self.s4r.at[h, g, k], self.partner)

    def scatter(self, h, lhs, rhs, before=None, after=None):
        c, q, chips, part = self.c, self.q, self.chips, self.part

        def pair(g):
            cols = chunk(g)
            self.to_partner(h, g).wait_recv()
            for k in (2, 0, 1):
                s = part[h, chips[k], c, :, cols].astype(F32) + self.recv1[h, chips[k], :, cols].astype(F32)
                part[h, chips[k], c, :, cols] = s.astype(BF)
                self.to_owner(h, g, k).start()
            self.own[h, :, cols] = part[h, q, c, :, cols].astype(F32) + self.recv1[h, q, :, cols].astype(F32)

        def step(g, carry):
            if before is not None:
                before(g)
            left = lhs()
            for p in range(2):
                cols = pl.ds(pl.multiple_of(g * GC + p * 512, 512), 512)
                out = jnp.dot(left, rhs(g, p), preferred_element_type=F32)
                part[h, :, :, :, cols] = out.astype(BF).reshape(4, 2, OR, 512)
            if after is not None:
                after(g)
            self.to_partner(h, g).start()

            @pl.when(g > 0)
            def _():
                pair(g - 1)

            return carry

        lax.fori_loop(0, G, step, 0)
        pair(G - 1)

    def finish(self, h, bias_ref, layer, scale):
        def final(g, carry):
            cols = chunk(g)
            tot = self.own[h, :, cols]
            for k in range(3):
                self.to_owner(h, g, k).wait_recv()
                tot = tot + self.recv2[h, k, :, cols].astype(F32)
            bias = bias_ref[:, cols].astype(F32)[layer:layer + 1]
            self.xown[h, :, cols] = (self.xown[h, :, cols].astype(F32) + tot.astype(BF).astype(F32) + bias).astype(BF)
            return carry

        lax.fori_loop(0, G, final, 0)

        def sent(g, carry):
            self.to_partner(h, g).wait_send()
            for k in range(3):
                self.to_owner(h, g, k).wait_send()
            return carry

        lax.fori_loop(0, G, sent, 0)
        rows = self.xown[h]
        self.n[h, pl.ds(pl.multiple_of((2 * self.q + self.c) * OR, OR), OR), :] = rows if scale is None else rms(rows, scale)

        def send(i, carry):
            for k in (2, 0, 1, 3):
                self.from_own(h, order(h, i), k).start()
            return carry

        lax.fori_loop(0, G, send, 0)

    def gathered(self, h, use, fresh=False):
        def step(i, carry):
            if not fresh:
                @pl.when(i < G)
                def _():
                    g = order(h, i)
                    for k in range(3):
                        self.from_own(h, g, k).wait_recv()
                        self.pass_on(h, g, k).start()

            @pl.when(i > 0)
            def _():
                g = order(h, i - 1)
                if not fresh:
                    self.from_own(h, g, 3).wait_recv()
                    for k in range(3):
                        self.pass_on(h, g, k).wait_recv()
                use(i - 1, g)

            return carry

        lax.fori_loop(0, G + 1, step, 0)
        if fresh:
            return

        def sent(g, carry):
            for k in range(4):
                self.from_own(h, g, k).wait_send()
            for k in range(3):
                self.pass_on(h, g, k).wait_send()
            return carry

        lax.fori_loop(0, G, sent, 0)


def order(h, i):
    return lax.rem(i + 2 * h, G)


LINK_SCRATCH = [
    pltpu.VMEM((2, 4, 2, OR, D), BF), pltpu.VMEM((2, 4, OR, D), BF), pltpu.VMEM((2, 3, OR, D), BF),
    pltpu.VMEM((2, OR, D), F32), pltpu.VMEM((2, HB, D), BF), pltpu.VMEM((2, OR, D), BF),
    DMA((2, G)), DMA((2, G)), DMA((2, G, 3)), DMA((2, G, 3)), DMA((2, G, 4)), DMA((2, G, 4)), DMA((2, G, 3)), DMA((2, G, 3)),
]
NLINK = len(LINK_SCRATCH)

SLOTS = 5
SLAB = 512
LOADS = 12


class Slabs:
    def __init__(self, groups, wu):
        self.groups, self.wu = groups, wu

    def start(self, load):
        for j, group in enumerate(self.groups):
            @pl.when((load >= LOADS * j) & (load < LOADS * (j + 1)))
            def _():
                for cp in group(load - LOADS * j, load):
                    cp.start()

    def begin(self):
        def body(load, carry):
            self.start(load)
            return carry

        lax.fori_loop(0, SLOTS, body, 0)

    def use(self, h, j, i, body):
        load = LOADS * j + 4 * h + i

        @pl.when(i >= 4 * h)
        def _():
            for cp in self.groups[j](load - LOADS * j, load):
                cp.wait()

        body(lax.rem(load, SLOTS))

        @pl.when((i < 4) | (h == 1))
        def _():
            self.start(load + SLOTS)


def slab_rows(k):
    return pl.ds(pl.multiple_of(lax.rem(k, 8) * SLAB, SLAB), SLAB)


def mlp_slabs(layer, w1, w2, wu, sems):
    def group(k, load):
        s = lax.rem(load, SLOTS)
        return [pltpu.make_async_copy(w1.at[layer, slab_rows(k), :], wu.at[s, 0], sems.at[s, 0]), pltpu.make_async_copy(w2.at[layer, slab_rows(k), :], wu.at[s, 1], sems.at[s, 1])]

    return group


def qkv_slabs(wq, wk, wv, wu, sems):
    def group(k, load):
        s = lax.rem(load, SLOTS)
        return [pltpu.make_async_copy(w.at[slab_rows(k), :], wu.at[s, 0, :, lo:hi], sems.at[s, j]) for j, (w, lo, hi) in enumerate(((wq, 0, 512), (wk, 512, 640), (wv, 640, 768)))]

    return group


def wide(src, dst, sems, g):
    return pltpu.make_async_copy(src.at[:, chunk(g)], dst.at[:, chunk(g)], sems.at[g])


def mlp_up(net, h, slabs, j, acc, h_s, b1_ref, b2_ref, layer):
    acc[...] = jnp.zeros_like(acc)

    def use(i, g):
        for e in range(2):
            def body(slot):
                ng = net.n[h, :, pl.ds(pl.multiple_of(g * GC + e * SLAB, SLAB), SLAB)]
                for half in range(2):
                    for lo in range(0, FC, 512):
                        acc[half, :, lo:lo + 512] += jnp.dot(ng, slabs.wu[slot, half, :, lo:lo + 512], preferred_element_type=F32)

            slabs.use(h, j, 2 * i + e, body)

    net.gathered(h, use)
    b1 = b1_ref[...].astype(F32)[layer:layer + 1]
    b2 = b2_ref[...].astype(F32)[layer:layer + 1]
    for lo in range(0, FC, 256):
        lanes = slice(lo, lo + 256)
        h_s[:, lanes] = (jax.nn.gelu(acc[0, :, lanes] + b1[:, lanes], approximate=True) * (acc[1, :, lanes] + b2[:, lanes])).astype(BF)


def mlp(net, slabs, j, acc, h_s, b1_ref, b2_ref, wd, wdb, ds, layer, last):
    for h in range(2):
        mlp_up(net, h, slabs, j, acc, h_s, b1_ref, b2_ref, layer)

        def before(g):
            if h == 0:
                wide(wd.at[layer], wdb, ds, g).wait()

        def after(g):
            if h == 1 and not last:
                wide(wd.at[layer + 1], wdb, ds, g).start()

        net.scatter(h, lambda: h_s[...], lambda g, p: wdb[:, pl.ds(pl.multiple_of(g * GC + p * 512, 512), 512)], before, after)


def rope(v, keep, turn):
    lane = lax.broadcasted_iota(jnp.int32, v.shape, 1)
    return v * keep + jnp.where(lane < 32, pltpu.roll(v, 96, 1), pltpu.roll(v, 32, 1)) * turn


def kernel_a(x_ref, sc_ref, wx, wy, conv, lru, wa_ref, wi_ref, bx_ref, by_ref, cw_ref, cb_ref, ba_ref, bi_ref, sp_ref, tok_ref, wout, rb_ref, w1, b1_ref, w2, b2_ref, wd, mb_ref, wq, wk, wv, keep_ref, turn_ref,
             q_ref, k_ref, v_ref, xo_ref, conv_out, lru_out, *scratch):
    net = Links(*scratch[:NLINK])
    wu, wdb, wxb, wob, acc, accr, h_s, conv_s, xb_s, lru_s, ht_s, prow, pcol, us, ds, xs, os, ss, ts, ls = scratch[NLINK:]
    scale = lambda l, j: sc_ref[...].astype(F32)[l, j:j + 1, :]
    rec_in = lambda l, g: [pltpu.make_async_copy(w.at[l, :, chunk(g)], wxb.at[j, :, chunk(g)], xs.at[j, g]) for j, w in enumerate((wx, wy))]
    state_in = lambda l: [pltpu.make_async_copy(conv.at[l], conv_s, ss.at[0]), pltpu.make_async_copy(lru.at[l], lru_s, ss.at[1])]
    state_out = lambda l: [pltpu.make_async_copy(conv_s.at[1:3], conv_out.at[l, 0:2], ts.at[0]), pltpu.make_async_copy(xb_s, conv_out.at[l, 2], ts.at[1]), pltpu.make_async_copy(lru_s, lru_out.at[l], ts.at[2])]
    slabs = Slabs([mlp_slabs(0, w1, w2, wu, us), mlp_slabs(1, w1, w2, wu, us), qkv_slabs(wq, wk, wv, wu, us)], wu)

    load_x = pltpu.make_async_copy(x_ref, net.part, ls)
    load_x.start()

    def load_rec(l):
        for g in range(G):
            for cp in rec_in(l, g):
                cp.start()

    load_rec(0)
    for cp in state_in(0):
        cp.start()
    for g in range(G):
        wide(wout.at[0], wob, os, g).start()
    net.enter()
    load_x.wait()
    for h in range(2):
        for chip in range(4):
            net.n[h, 2 * OR * chip:2 * OR * (chip + 1), :] = rms(net.part[h, chip].reshape(2 * OR, D), scale(0, 0))
        net.xown[h] = net.part[h, net.q, net.c]
    tok = tok_ref[...]

    for layer in range(2):
        row = lambda ref: ref[...].astype(F32)[layer:layer + 1]
        cw = cw_ref[...].astype(F32)
        params = [row(bx_ref), row(by_ref)] + [cw[layer, j:j + 1, :] for j in range(4)] + [row(cb_ref), row(ba_ref), row(bi_ref), row(sp_ref)]
        for j, p in enumerate(params):
            prow[j:j + 1, 0:LC] = p
        pcol[...] = prow[...].T

        for h in range(2):
            lanes = slice(HB * h, HB * (h + 1))
            accr[...] = jnp.zeros_like(accr)

            def use(i, g):
                if h == 0:
                    for cp in rec_in(layer, g):
                        cp.wait()
                ng = net.n[h, :, chunk(g)]
                for half in range(2):
                    accr[half] += lax.dot_general(wxb[half, :, chunk(g)], ng, NT, preferred_element_type=F32)

            net.gathered(h, use, fresh=layer == 0)
            if h == 0:
                for cp in state_in(layer):
                    cp.wait()
            elif layer == 0:
                slabs.begin()
                for g in range(G):
                    wide(wd.at[0], wdb, ds, g).start()
            tk = tok[:, lanes]
            fresh = tk == 0
            for b in range(4):
                rows = slice(176 * b, 176 * b + 176)
                pc = pcol[rows, :]
                col = lambda k: pc[:, k:k + 1]
                xb = (accr[0, rows, :] + col(0)).astype(BF)
                yb = jax.nn.gelu(accr[1, rows, :] + col(1), approximate=True)
                xb_s[rows, lanes] = xb
                hist = jnp.zeros((176, HB), F32)
                for j in range(3):
                    hist = hist + jnp.where(tk >= 3 - j, conv_s[j, rows, lanes].astype(F32), 0.0) * col(5 - j)
                xc = (col(6) + col(2) * xb.astype(F32) + hist).astype(BF)
                rg = jax.nn.sigmoid(lax.dot_general(wa_ref[layer, b], xc, TN, preferred_element_type=F32) + col(7))
                ig = jax.nn.sigmoid(lax.dot_general(wi_ref[layer, b], xc, TN, preferred_element_type=F32) + col(8))
                a = jnp.exp(rg * col(9))
                sc = jnp.sqrt(1.0 - a * a)
                a = jnp.where(fresh, 0.0, a)
                sc = jnp.where(fresh, 1.0, sc)
                hn = a * lru_s[rows, lanes] + sc * ig * xc.astype(F32)
                lru_s[rows, lanes] = hn
                ht_s[rows, :] = (hn * yb).astype(BF)
            ht_s[LC:, :] = jnp.zeros((64, HB), BF)
            h_s[:, :LC + 64] = ht_s[...].T

            def before(g):
                if h == 0:
                    wide(wout.at[layer], wob, os, g).wait()

            net.scatter(h, lambda: h_s[:, :LC], lambda g, p: wob[:, pl.ds(pl.multiple_of(g * GC + p * 512, 512), 512)], before)
        for cp in state_out(layer):
            cp.start()
        if layer == 0:
            load_rec(1)
            for g in range(G):
                wide(wout.at[1], wob, os, g).start()
        for h in range(2):
            net.finish(h, rb_ref, layer, scale(layer, 1))
        for cp in state_out(layer):
            cp.wait()
        if layer == 0:
            for cp in state_in(1):
                cp.start()
        mlp(net, slabs, layer, acc, h_s, b1_ref, b2_ref, wd, wdb, ds, layer, layer == 1)
        for h in range(2):
            net.finish(h, mb_ref, layer, scale(layer + 1, 0))

    xo_ref[...] = net.xown[...]
    for h in range(2):
        acc[...] = jnp.zeros_like(acc)

        def use_q(i, g):
            for e in range(2):
                def body(slot):
                    ng = net.n[h, :, pl.ds(pl.multiple_of(g * GC + e * SLAB, SLAB), SLAB)]
                    acc[0, :, 0:768] += jnp.dot(ng, wu[slot, 0, :, 0:768], preferred_element_type=F32)

                slabs.use(h, 2, 2 * i + e, body)

        net.gathered(h, use_q)
        keep, turn = keep_ref[h], turn_ref[h]
        for b in range(4):
            q_ref[h, :, HD * b:HD * (b + 1)] = rope(acc[0, :, HD * b:HD * (b + 1)], keep, turn).astype(BF)
        k_ref[h] = rope(acc[0, :, 512:640], keep, turn).astype(BF)
        v_ref[h] = acc[0, :, 640:768].astype(BF)


def first_layers(x, scale, wxt, wyt, convt, lrut, wa, wi, bx, by, cw, cb, ba, bi, sp, tok, wout, rb, w1, b1, w2, b2, wd, mb, wq, wk, wv, keep, turn):
    return pl.pallas_call(
        kernel_a,
        name='first_layers',
        out_shape=(jax.ShapeDtypeStruct((2, HB, 4 * HD), BF), jax.ShapeDtypeStruct((2, HB, HD), BF), jax.ShapeDtypeStruct((2, HB, HD), BF), jax.ShapeDtypeStruct((2, OR, D), BF),
                   jax.ShapeDtypeStruct(convt.shape, BF), jax.ShapeDtypeStruct(lrut.shape, F32)),
        in_specs=[ANY, VM, ANY, ANY, ANY, ANY, VM, VM] + [VM] * 7 + [VM, ANY, VM, ANY, VM, ANY, VM, ANY, VM, ANY, ANY, ANY, VM, VM],
        out_specs=(VM, VM, VM, VM, ANY, ANY),
        scratch_shapes=LINK_SCRATCH + [
            pltpu.VMEM((SLOTS, 2, SLAB, FC), BF), pltpu.VMEM((FC, D), BF), pltpu.VMEM((2, LC, D), BF), pltpu.VMEM((LC, D), BF),
            pltpu.VMEM((2, HB, FC), F32), pltpu.VMEM((2, LC, HB), F32), pltpu.VMEM((HB, FC), BF), pltpu.VMEM((3, LC, B), BF), pltpu.VMEM((LC, B), BF), pltpu.VMEM((LC, B), F32),
            pltpu.VMEM((LC + 64, HB), BF), pltpu.VMEM((16, LC + 64), F32), pltpu.VMEM((LC + 64, 16), F32),
            DMA((SLOTS, 3)), DMA((G,)), DMA((2, G)), DMA((G,)), DMA((2,)), DMA((3,)), DMA,
        ],
        compiler_params=pltpu.CompilerParams(collective_id=0, has_side_effects=True, vmem_limit_bytes=67043328),
        cost_estimate=pl.CostEstimate(flops=30 * 10**9, bytes_accessed=400 * 10**6, transcendentals=0),
    )(x.reshape(2, 4, 2, OR, D), scale, wxt, wyt, convt, lrut, wa, wi, bx, by, cw, cb, ba, bi, sp, tok, wout, rb, w1, b1, w2, b2, wd, mb, wq, wk, wv, keep.reshape(2, HB, HD), turn.reshape(2, HB, HD))


def kernel_b(o_ref, x_ref, wo, bo_ref, sc_ref, w1, b1_ref, w2, b2_ref, wd, mb_ref, out_ref, *scratch):
    net = Links(*scratch[:NLINK])
    wu, wdb, wob, acc, h_s, us, ds, os, ls = scratch[NLINK:]
    for g in range(G):
        wide(wo, wob, os, g).start()
    slabs = Slabs([mlp_slabs(2, w1, w2, wu, us)], wu)
    slabs.begin()
    for g in range(G):
        wide(wd.at[2], wdb, ds, g).start()
    net.enter()
    net.xown[...] = x_ref[...]
    for h in range(2):
        def before(g):
            if h == 0:
                wide(wo, wob, os, g).wait()

        net.scatter(h, lambda: o_ref[h], lambda g, p: wob[:, pl.ds(pl.multiple_of(g * GC + p * 512, 512), 512)], before)
    for h in range(2):
        net.finish(h, bo_ref, 0, sc_ref[...].astype(F32)[2, 1:2, :])
    mlp(net, slabs, 0, acc, h_s, b1_ref, b2_ref, wd, wdb, ds, 2, True)
    for h in range(2):
        net.finish(h, mb_ref, 2, None)
    store = lambda h, g: pltpu.make_async_copy(net.n.at[h, :, chunk(g)], out_ref.at[h, :, chunk(g)], ls.at[h, g])
    for h in range(2):
        net.gathered(h, lambda i, g: store(h, g).start())
    for h in range(2):
        for g in range(G):
            store(h, g).wait()


def last_layer(o, x_own, wo, bo, scale, w1, b1, w2, b2, wd, mb):
    out = pl.pallas_call(
        kernel_b,
        name='last_layer',
        out_shape=jax.ShapeDtypeStruct((2, HB, D), BF),
        in_specs=[VM, VM, ANY, VM, VM, ANY, VM, ANY, VM, ANY, VM],
        out_specs=ANY,
        scratch_shapes=LINK_SCRATCH + [
            pltpu.VMEM((SLOTS, 2, SLAB, FC), BF), pltpu.VMEM((FC, D), BF), pltpu.VMEM((4 * HD, D), BF),
            pltpu.VMEM((2, HB, FC), F32), pltpu.VMEM((HB, FC), BF),
            DMA((SLOTS, 3)), DMA((G,)), DMA((G,)), DMA((2, G)),
        ],
        compiler_params=pltpu.CompilerParams(collective_id=1, has_side_effects=True, vmem_limit_bytes=67043328),
        cost_estimate=pl.CostEstimate(flops=12 * 10**9, bytes_accessed=200 * 10**6, transcendentals=0),
    )(o.reshape(2, HB, 4 * HD), x_own, wo, bo, scale, w1, b1, w2, b2, wd, mb)
    return out.reshape(B, D)


RA = 8
NB = 6
STEPS = B // RA


def attn_kernel(tok_ref, q_ref, kn_ref, vn_ref, slot_ref, k_ref, v_ref, o_ref, ko_ref, vo_ref, so_ref, kb, vb, s_s, q_s, o_s, isem, osem):
    lane = lax.broadcasted_iota(jnp.int32, (1, W), 1)
    sub = lax.broadcasted_iota(jnp.int32, (16, HD), 0)

    def copies(step, out):
        b = lax.rem(step, NB)
        rows = pl.ds(pl.multiple_of(step * RA, RA), RA)
        if out:
            return [pltpu.make_async_copy(kb.at[b], ko_ref.at[rows], osem.at[0, b]), pltpu.make_async_copy(vb.at[b], vo_ref.at[rows], osem.at[1, b])]
        return [pltpu.make_async_copy(k_ref.at[rows], kb.at[b], isem.at[0, b]), pltpu.make_async_copy(v_ref.at[rows], vb.at[b], isem.at[1, b])]

    def start(step):
        for cp in copies(step, False):
            cp.start()

    lax.fori_loop(0, NB - 2, lambda step, c: (start(step), c)[1], 0)

    def step_fn(i, carry):
        b = lax.rem(i, NB)
        rows = pl.ds(pl.multiple_of(i * RA, RA), RA)
        ahead = i + NB - 2

        @pl.when(ahead < STEPS)
        def _():
            @pl.when(ahead >= NB)
            def _():
                for cp in copies(ahead - NB, True):
                    cp.wait()
            start(ahead)

        for cp in copies(i, False):
            cp.wait()
        kn = kn_ref[rows, :].astype(F32)
        vn = vn_ref[rows, :].astype(F32)
        for h in range(4):
            q_s[pl.ds(h, RA, stride=4), :] = q_ref[rows, 128 * h:128 * h + 128].astype(F32)
        slots = slot_ref[rows, :]
        new_rows = []
        for r in range(RA):
            tp = tok_ref[i * RA + r]
            slot = lax.rem(tp, W)
            base = pl.multiple_of((slot // 16) * 16, 16)
            hit = sub == (slot - base)
            spot = pl.ds(base, 16)
            kb[b, r, spot, :] = jnp.where(hit, kn[r:r + 1], kb[b, r, spot, :].astype(F32)).astype(BF)
            vb[b, r, spot, :] = jnp.where(hit, vn[r:r + 1], vb[b, r, spot, :].astype(F32)).astype(BF)
            sn = jnp.where(lane == slot, tp, slots[r:r + 1])
            new_rows.append((tp, sn))
        for r in range(RA):
            tp, sn = new_rows[r]
            so_ref[pl.ds(i * RA + r, 1), :] = sn
            age = tp - sn
            valid = (sn >= 0) & (age >= 0) & (age < W)
            s = lax.dot_general(q_s[4 * r:4 * r + 4, :].astype(BF), kb[b, r], NT, preferred_element_type=F32) * (HD ** -0.5)
            s_s[4 * r:4 * r + 4, :] = jnp.where(valid, s, -jnp.inf)
        s = s_s[...]
        e = jnp.exp(s - jnp.max(s, axis=-1, keepdims=True))
        s_s[...] = e / jnp.sum(e, axis=-1, keepdims=True)
        for r in range(RA):
            o_s[4 * r:4 * r + 4, :] = jnp.dot(s_s[4 * r:4 * r + 4, :].astype(BF), vb[b, r], preferred_element_type=F32)
        for h in range(4):
            o_ref[rows, 128 * h:128 * h + 128] = o_s[pl.ds(h, RA, stride=4), :].astype(BF)
        for cp in copies(i, True):
            cp.start()
        return carry

    lax.fori_loop(0, STEPS, step_fn, 0)
    for step in range(STEPS - NB, STEPS):
        for cp in copies(step, True):
            cp.wait()


def attend(tok, q, kn, vn, slot_pos, kc, vc):
    return pl.pallas_call(
        attn_kernel,
        name='attend',
        in_specs=[pl.BlockSpec(memory_space=pltpu.SMEM), VM, VM, VM, VM, ANY, ANY],
        out_specs=(VM, ANY, ANY, VM),
        out_shape=(jax.ShapeDtypeStruct((B, 4 * HD), BF), jax.ShapeDtypeStruct(kc.shape, BF), jax.ShapeDtypeStruct(vc.shape, BF), jax.ShapeDtypeStruct(slot_pos.shape, jnp.int32)),
        scratch_shapes=[pltpu.VMEM((NB, RA, W, HD), BF), pltpu.VMEM((NB, RA, W, HD), BF), pltpu.VMEM((4 * RA, W), F32), pltpu.VMEM((4 * RA, HD), F32), pltpu.VMEM((4 * RA, HD), F32),
                        pltpu.SemaphoreType.DMA((2, NB)), pltpu.SemaphoreType.DMA((2, NB))],
        cost_estimate=pl.CostEstimate(flops=4 * B * 4 * W * HD, bytes_accessed=8 * B * W * HD, transcendentals=0),
    )(tok, q, kn, vn, slot_pos, kc, vc)


def rope_tables(tok_pos):
    quarter = HD // 4
    lane = lax.broadcasted_iota(jnp.int32, (1, HD), 1)
    inv_freq = ROPE_BASE ** (-(lane % quarter).astype(F32) / quarter)
    angles = tok_pos.astype(F32)[:, None] * inv_freq
    cos, sin = jnp.cos(angles), jnp.sin(angles)
    return jnp.where(lane < 2 * quarter, cos, 1.0), jnp.where(lane < quarter, -sin, jnp.where(lane < 2 * quarter, sin, 0.0))


def io_specs():
    in_specs = (P('dp', None), P('dp'), P(None, 'dp', None, 'tp'), P(None, 'dp', 'tp'), P('dp', None, None), P('dp', None, None), P('dp', None),
                P(), P(None, None, 'tp'), P(None, 'tp'), P(None, None, 'tp'), P(None, 'tp'), P(None, None, 'tp'), P(None, 'tp'),
                P(None, 'tp', None, None), P(None, 'tp'), P(None, 'tp', None, None), P(None, 'tp'), P(None, 'tp'), P(None, 'tp', None), P(),
                P(None, 'tp'), P(), P(), P('tp', None), P(),
                P(None, None, 'tp'), P(None, 'tp'), P(None, None, 'tp'), P(None, 'tp'), P(None, 'tp', None), P())
    out_specs = (P('dp', None), P(None, 'dp', None, 'tp'), P(None, 'dp', 'tp'), P('dp', None, None), P('dp', None, None), P('dp', None))
    return in_specs, out_specs


def solution(mesh):
    in_specs, out_specs = io_specs()

    def local_step(x_in, tok_pos, conv_state, lru_state, k_cache, v_cache, slot_pos, norm_scale, rec_wx, rec_bx, rec_wy, rec_by, conv_w, conv_b, gate_wa, gate_ba, gate_wi, gate_bi, a_param, rec_wout, rec_bout, attn_wq, attn_wk, attn_wv, attn_wo, attn_bo, mlp_w1, mlp_b1, mlp_w2, mlp_b2, mlp_wd, mlp_bd):
        wxt = jnp.swapaxes(rec_wx, 1, 2)
        wyt = jnp.swapaxes(rec_wy, 1, 2)
        convt = jnp.transpose(conv_state, (0, 2, 3, 1))
        lrut = jnp.swapaxes(lru_state, 1, 2)
        tok_row = tok_pos[None, :]
        tab = rope_tables(tok_pos)

        q, kn, vn, x_own, convs, lrus = first_layers(x_in, norm_scale, wxt, wyt, convt, lrut, gate_wa, gate_wi, rec_bx, rec_by, conv_w, conv_b, gate_ba, gate_bi, -8.0 * jax.nn.softplus(a_param), tok_row, rec_wout, rec_bout, mlp_w1, mlp_b1, mlp_w2, mlp_b2, mlp_wd, mlp_bd, attn_wq, attn_wk, attn_wv, *tab)
        o, k_next, v_next, slot_next = attend(tok_pos, q.reshape(B, 4 * HD), kn.reshape(B, HD), vn.reshape(B, HD), slot_pos, k_cache, v_cache)
        x = last_layer(o, x_own, attn_wo, attn_bo[None, :], norm_scale, mlp_w1, mlp_b1, mlp_w2, mlp_b2, mlp_wd, mlp_bd)
        conv_out = jnp.transpose(convs, (0, 3, 1, 2))
        lru_out = jnp.swapaxes(lrus, 1, 2)
        return (x, conv_out, lru_out, k_next, v_next, slot_next)

    return jax.shard_map(local_step, mesh=mesh, in_specs=in_specs, out_specs=out_specs, check_vma=False)
```

```python
import functools

import jax
import jax.numpy as jnp
from jax import lax
from jax.experimental import pallas as pl
from jax.experimental.pallas import tpu as pltpu
from jax.sharding import PartitionSpec as P

ROPE_BASE = 10000.0
NORM_EPS = 1e-6
MESH = pl.DeviceIdType.MESH
BF = jnp.bfloat16
F32 = jnp.float32
ANY = pl.BlockSpec(memory_space=pl.ANY)
VM = pl.BlockSpec(memory_space=pltpu.VMEM)
B = 256
D = 4096
LC = 704
FC = 1536
W = 1024
HD = 128
G = 2
HB = 128
OR = 16
GC = D // G


def rms(x, scale):
    xf = x.astype(F32)
    mean_sq = jnp.mean(xf * xf, axis=-1, keepdims=True)
    return (xf * lax.rsqrt(mean_sq + NORM_EPS) * (1.0 + scale.astype(F32))).astype(BF)


NT = (((1,), (1,)), ((), ()))
TN = (((0,), (0,)), ((), ()))
DMA = pltpu.SemaphoreType.DMA


def chunk(g):
    return pl.ds(pl.multiple_of(g * GC, GC), GC)


SLAB = 512
PER = GC // SLAB


def piece(g, e):
    return pl.ds(pl.multiple_of(g * GC + e * SLAB, SLAB), SLAB)


class Links:
    def __init__(self, part, recv1, recv2, own, n, xown, s1s, s1r, s2s, s2r, s3s, s3r, s4s, s4r, s5s, s5r):
        self.part, self.recv1, self.recv2, self.own, self.n, self.xown = part, recv1, recv2, own, n, xown
        self.s1s, self.s1r, self.s2s, self.s2r, self.s3s, self.s3r, self.s4s, self.s4r, self.s5s, self.s5r = s1s, s1r, s2s, s2r, s3s, s3r, s4s, s4r, s5s, s5r
        t = lax.axis_index('tp')
        y, x = t // 4, (t // 2) % 2
        self.c = t % 2
        self.q = 2 * y + x
        self.partner = 2 * self.q + 1 - self.c
        self.chips = [2 * y + (1 - x), 2 * (1 - y) + x, 2 * (1 - y) + (1 - x)]
        self.peers = [2 * qd + self.c for qd in self.chips]

    def enter(self):
        barrier = pltpu.get_barrier_semaphore()
        for dev in [self.partner] + self.peers:
            pl.semaphore_signal(barrier, inc=1, device_id={'tp': dev}, device_id_type=MESH)
        pl.semaphore_wait(barrier, 4)

    def remote(self, src, dst, ss, rs, dev):
        return pltpu.make_async_remote_copy(src_ref=src, dst_ref=dst, send_sem=ss, recv_sem=rs, device_id={'tp': dev}, device_id_type=MESH)

    def to_partner(self, h, g):
        return self.remote(self.part.at[h, :, 1 - self.c, :, chunk(g)], self.recv1.at[h, :, :, chunk(g)], self.s1s.at[h, g], self.s1r.at[h, g], self.partner)

    def to_owner(self, h, g, k):
        return self.remote(self.part.at[h, self.chips[k], self.c, :, chunk(g)], self.recv2.at[h, k, :, chunk(g)], self.s2s.at[h, g, k], self.s2r.at[h, g, k], self.peers[k])

    def place(self, h, dev, g):
        return self.n.at[h, pl.ds(pl.multiple_of(dev * OR, OR), OR), chunk(g)]

    def from_own(self, h, g, k):
        ref = self.place(h, 2 * self.q + self.c, g)
        return self.remote(ref, ref, self.s3s.at[h, g, k], self.s3r.at[h, g, k], self.peers[k])

    def own_pair(self, h):
        ref = self.n.at[h, pl.ds(pl.multiple_of((2 * self.q + self.c) * OR, OR), OR)]
        return self.remote(ref, ref, self.s5s.at[h], self.s5r.at[h], self.partner)

    def pass_on(self, h, g, k):
        ref = self.place(h, self.peers[k], g)
        return self.remote(ref, ref, self.s4s.at[h, g, k], self.s4r.at[h, g, k], self.partner)

    def scatter(self, h, lhs, rhs, before=None, after=None):
        c, q, chips, part = self.c, self.q, self.chips, self.part

        def pair(g):
            cols = chunk(g)
            self.to_partner(h, g).wait_recv()
            for k in (2, 0, 1):
                s = part[h, chips[k], c, :, cols].astype(F32) + self.recv1[h, chips[k], :, cols].astype(F32)
                part[h, chips[k], c, :, cols] = s.astype(BF)
                self.to_owner(h, g, k).start()
            self.own[h, :, cols] = part[h, q, c, :, cols].astype(F32) + self.recv1[h, q, :, cols].astype(F32)

        def step(g, carry):
            if before is not None:
                before(g)
            def tile(p, carry):
                cols = piece(g, p)
                out = jnp.dot(lhs(), rhs(cols), preferred_element_type=F32)
                part[h, :, :, :, cols] = out.astype(BF).reshape(4, 2, OR, SLAB)
                return carry

            lax.fori_loop(0, PER, tile, 0)
            if after is not None:
                after(g)
            self.to_partner(h, g).start()

            @pl.when(g > 0)
            def _():
                pair(g - 1)

            return carry

        lax.fori_loop(0, G, step, 0)
        pair(G - 1)

    def finish(self, h, bias_ref, layer, scale):
        def final(g, carry):
            cols = chunk(g)
            tot = self.own[h, :, cols]
            for k in range(3):
                self.to_owner(h, g, k).wait_recv()
                tot = tot + self.recv2[h, k, :, cols].astype(F32)
            bias = bias_ref[:, cols].astype(F32)[layer:layer + 1]
            self.xown[h, :, cols] = (self.xown[h, :, cols].astype(F32) + tot.astype(BF).astype(F32) + bias).astype(BF)
            return carry

        lax.fori_loop(0, G, final, 0)

        def sent(g, carry):
            self.to_partner(h, g).wait_send()
            for k in range(3):
                self.to_owner(h, g, k).wait_send()
            return carry

        lax.fori_loop(0, G, sent, 0)
        rows = self.xown[h]
        self.n[h, pl.ds(pl.multiple_of((2 * self.q + self.c) * OR, OR), OR), :] = rows if scale is None else rms(rows, scale)

        self.own_pair(h).start()

        def send(i, carry):
            for k in (2, 0, 1):
                self.from_own(h, order(h, i), k).start()
            return carry

        lax.fori_loop(0, G, send, 0)

    def gathered(self, h, use, fresh=False):
        def step(i, carry):
            if not fresh:
                @pl.when(i < G)
                def _():
                    g = order(h, i)
                    for k in range(3):
                        self.from_own(h, g, k).wait_recv()
                        self.pass_on(h, g, k).start()

            @pl.when(i > 0)
            def _():
                g = order(h, i - 1)
                if not fresh:
                    @pl.when(i == 1)
                    def _():
                        self.own_pair(h).wait_recv()

                    for k in range(3):
                        self.pass_on(h, g, k).wait_recv()
                use(i - 1, g)

            return carry

        lax.fori_loop(0, G + 1, step, 0)
        if fresh:
            return

        self.own_pair(h).wait_send()

        def sent(g, carry):
            for k in range(3):
                self.from_own(h, g, k).wait_send()
                self.pass_on(h, g, k).wait_send()
            return carry

        lax.fori_loop(0, G, sent, 0)


def order(h, i):
    return lax.rem(i + (G // 2) * h, G)


LINK_SCRATCH = [
    pltpu.VMEM((2, 4, 2, OR, D), BF), pltpu.VMEM((2, 4, OR, D), BF), pltpu.VMEM((2, 3, OR, D), BF),
    pltpu.VMEM((2, OR, D), F32), pltpu.VMEM((2, HB, D), BF), pltpu.VMEM((2, OR, D), BF),
    DMA((2, G)), DMA((2, G)), DMA((2, G, 3)), DMA((2, G, 3)), DMA((2, G, 3)), DMA((2, G, 3)), DMA((2, G, 3)), DMA((2, G, 3)), DMA((2,)), DMA((2,)),
]
NLINK = len(LINK_SCRATCH)

SLOTS = 5
LOADS = 12


class Slabs:
    def __init__(self, groups, wu):
        self.groups, self.wu = groups, wu

    def start(self, load):
        for j, group in enumerate(self.groups):
            @pl.when((load >= LOADS * j) & (load < LOADS * (j + 1)))
            def _():
                for cp in group(load - LOADS * j, load):
                    cp.start()

    def begin(self):
        def body(load, carry):
            self.start(load)
            return carry

        lax.fori_loop(0, SLOTS, body, 0)

    def use(self, h, j, i, body):
        load = LOADS * j + 4 * h + i

        @pl.when(i >= 4 * h)
        def _():
            for cp in self.groups[j](load - LOADS * j, load):
                cp.wait()

        body(lax.rem(load, SLOTS))

        @pl.when((i < 4) | (h == 1))
        def _():
            self.start(load + SLOTS)


def slab_rows(k):
    return pl.ds(pl.multiple_of(lax.rem(k, 8) * SLAB, SLAB), SLAB)


def mlp_slabs(layer, w1, w2, wu, sems):
    def group(k, load):
        s = lax.rem(load, SLOTS)
        return [pltpu.make_async_copy(w1.at[layer, slab_rows(k), :], wu.at[s, 0], sems.at[s, 0]), pltpu.make_async_copy(w2.at[layer, slab_rows(k), :], wu.at[s, 1], sems.at[s, 1])]

    return group


def qkv_slabs(wq, wk, wv, wu, sems):
    def group(k, load):
        s = lax.rem(load, SLOTS)
        return [pltpu.make_async_copy(w.at[slab_rows(k), :], wu.at[s, 0, :, lo:hi], sems.at[s, j]) for j, (w, lo, hi) in enumerate(((wq, 0, 512), (wk, 512, 640), (wv, 640, 768)))]

    return group


def wide(src, dst, sems, g):
    return pltpu.make_async_copy(src.at[:, chunk(g)], dst.at[:, chunk(g)], sems.at[g])


def mlp_up(net, h, slabs, j, acc, h_s, b1_ref, b2_ref, layer):
    acc[...] = jnp.zeros_like(acc)

    def use(i, g):
        def one(e, carry):
            def body(slot):
                ng = net.n[h, :, piece(g, e)]
                for half in range(2):
                    for lo in range(0, FC, 512):
                        acc[half, :, lo:lo + 512] += jnp.dot(ng, slabs.wu[slot, half, :, lo:lo + 512], preferred_element_type=F32)

            slabs.use(h, j, PER * i + e, body)
            return carry

        lax.fori_loop(0, PER, one, 0)

    net.gathered(h, use)
    b1 = b1_ref[...].astype(F32)[layer:layer + 1]
    b2 = b2_ref[...].astype(F32)[layer:layer + 1]
    for lo in range(0, FC, 256):
        lanes = slice(lo, lo + 256)
        h_s[:, lanes] = (jax.nn.gelu(acc[0, :, lanes] + b1[:, lanes], approximate=True) * (acc[1, :, lanes] + b2[:, lanes])).astype(BF)


def mlp(net, slabs, j, acc, h_s, b1_ref, b2_ref, wd, wdb, ds, layer, last):
    for h in range(2):
        mlp_up(net, h, slabs, j, acc, h_s, b1_ref, b2_ref, layer)

        def before(g):
            if h == 0:
                wide(wd.at[layer], wdb, ds, g).wait()

        def after(g):
            if h == 1 and not last:
                wide(wd.at[layer + 1], wdb, ds, g).start()

        net.scatter(h, lambda: h_s[...], lambda cols: wdb[:, cols], before, after)


def rope(v, keep, turn):
    lane = lax.broadcasted_iota(jnp.int32, v.shape, 1)
    return v * keep + jnp.where(lane < 32, pltpu.roll(v, 96, 1), pltpu.roll(v, 32, 1)) * turn


def kernel_a(x_ref, sc_ref, wx, wy, conv, lru, wa_ref, wi_ref, bx_ref, by_ref, cw_ref, cb_ref, ba_ref, bi_ref, sp_ref, tok_ref, wout, rb_ref, w1, b1_ref, w2, b2_ref, wd, mb_ref, wq, wk, wv, keep_ref, turn_ref,
             q_ref, k_ref, v_ref, xo_ref, conv_out, lru_out, *scratch):
    net = Links(*scratch[:NLINK])
    wu, wdb, wxb, wob, acc, accr, h_s, conv_s, xb_s, lru_s, ht_s, prow, pcol, us, ds, xs, os, ss, ts, ls = scratch[NLINK:]
    scale = lambda l, j: sc_ref[...].astype(F32)[l, j:j + 1, :]
    rec_in = lambda l, g: [pltpu.make_async_copy(w.at[l, :, chunk(g)], wxb.at[j, :, chunk(g)], xs.at[j, g]) for j, w in enumerate((wx, wy))]
    state_in = lambda l: [pltpu.make_async_copy(conv.at[l], conv_s, ss.at[0]), pltpu.make_async_copy(lru.at[l], lru_s, ss.at[1])]
    state_out = lambda l: [pltpu.make_async_copy(conv_s.at[1:3], conv_out.at[l, 0:2], ts.at[0]), pltpu.make_async_copy(xb_s, conv_out.at[l, 2], ts.at[1]), pltpu.make_async_copy(lru_s, lru_out.at[l], ts.at[2])]
    slabs = Slabs([mlp_slabs(0, w1, w2, wu, us), mlp_slabs(1, w1, w2, wu, us), qkv_slabs(wq, wk, wv, wu, us)], wu)

    load_x = pltpu.make_async_copy(x_ref, net.part, ls)
    load_x.start()

    def load_rec(l):
        for g in range(G):
            for cp in rec_in(l, g):
                cp.start()

    load_rec(0)
    for cp in state_in(0):
        cp.start()
    for g in range(G):
        wide(wout.at[0], wob, os, g).start()
    net.enter()
    load_x.wait()
    for h in range(2):
        for chip in range(4):
            net.n[h, 2 * OR * chip:2 * OR * (chip + 1), :] = rms(net.part[h, chip].reshape(2 * OR, D), scale(0, 0))
        net.xown[h] = net.part[h, net.q, net.c]
    tok = tok_ref[...]

    for layer in range(2):
        row = lambda ref: ref[...].astype(F32)[layer:layer + 1]
        cw = cw_ref[...].astype(F32)
        params = [row(bx_ref), row(by_ref)] + [cw[layer, j:j + 1, :] for j in range(4)] + [row(cb_ref), row(ba_ref), row(bi_ref), row(sp_ref)]
        for j, p in enumerate(params):
            prow[j:j + 1, 0:LC] = p
        pcol[...] = prow[...].T

        for h in range(2):
            lanes = slice(HB * h, HB * (h + 1))
            accr[...] = jnp.zeros_like(accr)

            def use(i, g):
                if h == 0:
                    for cp in rec_in(layer, g):
                        cp.wait()

                def one(e, carry):
                    cols = pl.ds(pl.multiple_of(g * GC + e * 1024, 1024), 1024)
                    for half in range(2):
                        accr[half] += lax.dot_general(wxb[half, :, cols], net.n[h, :, cols], NT, preferred_element_type=F32)
                    return carry

                lax.fori_loop(0, GC // 1024, one, 0)

            net.gathered(h, use, fresh=layer == 0)
            if h == 0:
                for cp in state_in(layer):
                    cp.wait()
            elif layer == 0:
                slabs.begin()
                for g in range(G):
                    wide(wd.at[0], wdb, ds, g).start()
            tk = tok[:, lanes]
            fresh = tk == 0
            for b in range(4):
                rows = slice(176 * b, 176 * b + 176)
                pc = pcol[rows, :]
                col = lambda k: pc[:, k:k + 1]
                xb = (accr[0, rows, :] + col(0)).astype(BF)
                yb = jax.nn.gelu(accr[1, rows, :] + col(1), approximate=True)
                xb_s[rows, lanes] = xb
                hist = jnp.zeros((176, HB), F32)
                for j in range(3):
                    hist = hist + jnp.where(tk >= 3 - j, conv_s[j, rows, lanes].astype(F32), 0.0) * col(5 - j)
                xc = (col(6) + col(2) * xb.astype(F32) + hist).astype(BF)
                rg = jax.nn.sigmoid(lax.dot_general(wa_ref[layer, b], xc, TN, preferred_element_type=F32) + col(7))
                ig = jax.nn.sigmoid(lax.dot_general(wi_ref[layer, b], xc, TN, preferred_element_type=F32) + col(8))
                a = jnp.exp(rg * col(9))
                sc = jnp.sqrt(1.0 - a * a)
                a = jnp.where(fresh, 0.0, a)
                sc = jnp.where(fresh, 1.0, sc)
                hn = a * lru_s[rows, lanes] + sc * ig * xc.astype(F32)
                lru_s[rows, lanes] = hn
                ht_s[rows, :] = (hn * yb).astype(BF)
            ht_s[LC:, :] = jnp.zeros((64, HB), BF)
            h_s[:, :LC + 64] = ht_s[...].T

            def before(g):
                if h == 0:
                    wide(wout.at[layer], wob, os, g).wait()

            net.scatter(h, lambda: h_s[:, :LC], lambda cols: wob[:, cols], before)
        for cp in state_out(layer):
            cp.start()
        if layer == 0:
            load_rec(1)
            for g in range(G):
                wide(wout.at[1], wob, os, g).start()
        for h in range(2):
            net.finish(h, rb_ref, layer, scale(layer, 1))
        for cp in state_out(layer):
            cp.wait()
        if layer == 0:
            for cp in state_in(1):
                cp.start()
        mlp(net, slabs, layer, acc, h_s, b1_ref, b2_ref, wd, wdb, ds, layer, layer == 1)
        for h in range(2):
            net.finish(h, mb_ref, layer, scale(layer + 1, 0))

    xo_ref[...] = net.xown[...]
    for h in range(2):
        acc[...] = jnp.zeros_like(acc)

        def use_q(i, g):
            def one(e, carry):
                def body(slot):
                    acc[0, :, 0:768] += jnp.dot(net.n[h, :, piece(g, e)], wu[slot, 0, :, 0:768], preferred_element_type=F32)

                slabs.use(h, 2, PER * i + e, body)
                return carry

            lax.fori_loop(0, PER, one, 0)

        net.gathered(h, use_q)
        keep, turn = keep_ref[h], turn_ref[h]
        for b in range(4):
            q_ref[h, :, HD * b:HD * (b + 1)] = rope(acc[0, :, HD * b:HD * (b + 1)], keep, turn).astype(BF)
        k_ref[h] = rope(acc[0, :, 512:640], keep, turn).astype(BF)
        v_ref[h] = acc[0, :, 640:768].astype(BF)


def first_layers(x, scale, wxt, wyt, convt, lrut, wa, wi, bx, by, cw, cb, ba, bi, sp, tok, wout, rb, w1, b1, w2, b2, wd, mb, wq, wk, wv, keep, turn):
    return pl.pallas_call(
        kernel_a,
        name='first_layers',
        out_shape=(jax.ShapeDtypeStruct((2, HB, 4 * HD), BF), jax.ShapeDtypeStruct((2, HB, HD), BF), jax.ShapeDtypeStruct((2, HB, HD), BF), jax.ShapeDtypeStruct((2, OR, D), BF),
                   jax.ShapeDtypeStruct(convt.shape, BF), jax.ShapeDtypeStruct(lrut.shape, F32)),
        in_specs=[ANY, VM, ANY, ANY, ANY, ANY, VM, VM] + [VM] * 7 + [VM, ANY, VM, ANY, VM, ANY, VM, ANY, VM, ANY, ANY, ANY, VM, VM],
        out_specs=(VM, VM, VM, VM, ANY, ANY),
        scratch_shapes=LINK_SCRATCH + [
            pltpu.VMEM((SLOTS, 2, SLAB, FC), BF), pltpu.VMEM((FC, D), BF), pltpu.VMEM((2, LC, D), BF), pltpu.VMEM((LC, D), BF),
            pltpu.VMEM((2, HB, FC), F32), pltpu.VMEM((2, LC, HB), F32), pltpu.VMEM((HB, FC), BF), pltpu.VMEM((3, LC, B), BF), pltpu.VMEM((LC, B), BF), pltpu.VMEM((LC, B), F32),
            pltpu.VMEM((LC + 64, HB), BF), pltpu.VMEM((16, LC + 64), F32), pltpu.VMEM((LC + 64, 16), F32),
            DMA((SLOTS, 3)), DMA((G,)), DMA((2, G)), DMA((G,)), DMA((2,)), DMA((3,)), DMA,
        ],
        compiler_params=pltpu.CompilerParams(collective_id=0, has_side_effects=True, vmem_limit_bytes=67043328),
        cost_estimate=pl.CostEstimate(flops=30 * 10**9, bytes_accessed=400 * 10**6, transcendentals=0),
    )(x.reshape(2, 4, 2, OR, D), scale, wxt, wyt, convt, lrut, wa, wi, bx, by, cw, cb, ba, bi, sp, tok, wout, rb, w1, b1, w2, b2, wd, mb, wq, wk, wv, keep.reshape(2, HB, HD), turn.reshape(2, HB, HD))


def kernel_b(o_ref, x_ref, wo, bo_ref, sc_ref, w1, b1_ref, w2, b2_ref, wd, mb_ref, out_ref, *scratch):
    net = Links(*scratch[:NLINK])
    wu, wdb, wob, acc, h_s, us, ds, os, ls = scratch[NLINK:]
    for g in range(G):
        wide(wo, wob, os, g).start()
    slabs = Slabs([mlp_slabs(2, w1, w2, wu, us)], wu)
    slabs.begin()
    for g in range(G):
        wide(wd.at[2], wdb, ds, g).start()
    net.enter()
    net.xown[...] = x_ref[...]
    for h in range(2):
        def before(g):
            if h == 0:
                wide(wo, wob, os, g).wait()

        net.scatter(h, lambda: o_ref[h], lambda cols: wob[:, cols], before)
    for h in range(2):
        net.finish(h, bo_ref, 0, sc_ref[...].astype(F32)[2, 1:2, :])
    mlp(net, slabs, 0, acc, h_s, b1_ref, b2_ref, wd, wdb, ds, 2, True)
    for h in range(2):
        net.finish(h, mb_ref, 2, None)
    store = lambda h, g: pltpu.make_async_copy(net.n.at[h, :, chunk(g)], out_ref.at[h, :, chunk(g)], ls.at[h, g])
    for h in range(2):
        net.gathered(h, lambda i, g: store(h, g).start())
    for h in range(2):
        for g in range(G):
            store(h, g).wait()


def last_layer(o, x_own, wo, bo, scale, w1, b1, w2, b2, wd, mb):
    out = pl.pallas_call(
        kernel_b,
        name='last_layer',
        out_shape=jax.ShapeDtypeStruct((2, HB, D), BF),
        in_specs=[VM, VM, ANY, VM, VM, ANY, VM, ANY, VM, ANY, VM],
        out_specs=ANY,
        scratch_shapes=LINK_SCRATCH + [
            pltpu.VMEM((SLOTS, 2, SLAB, FC), BF), pltpu.VMEM((FC, D), BF), pltpu.VMEM((4 * HD, D), BF),
            pltpu.VMEM((2, HB, FC), F32), pltpu.VMEM((HB, FC), BF),
            DMA((SLOTS, 3)), DMA((G,)), DMA((G,)), DMA((2, G)),
        ],
        compiler_params=pltpu.CompilerParams(collective_id=1, has_side_effects=True, vmem_limit_bytes=67043328),
        cost_estimate=pl.CostEstimate(flops=12 * 10**9, bytes_accessed=200 * 10**6, transcendentals=0),
    )(o.reshape(2, HB, 4 * HD), x_own, wo, bo, scale, w1, b1, w2, b2, wd, mb)
    return out.reshape(B, D)


RA = 8
NB = 6
STEPS = B // RA


def attn_kernel(tok_ref, q_ref, kn_ref, vn_ref, slot_ref, k_ref, v_ref, o_ref, ko_ref, vo_ref, so_ref, kb, vb, s_s, q_s, o_s, isem, osem):
    lane = lax.broadcasted_iota(jnp.int32, (1, W), 1)
    sub = lax.broadcasted_iota(jnp.int32, (16, HD), 0)

    def copies(step, out):
        b = lax.rem(step, NB)
        rows = pl.ds(pl.multiple_of(step * RA, RA), RA)
        if out:
            return [pltpu.make_async_copy(kb.at[b], ko_ref.at[rows], osem.at[0, b]), pltpu.make_async_copy(vb.at[b], vo_ref.at[rows], osem.at[1, b])]
        return [pltpu.make_async_copy(k_ref.at[rows], kb.at[b], isem.at[0, b]), pltpu.make_async_copy(v_ref.at[rows], vb.at[b], isem.at[1, b])]

    def start(step):
        for cp in copies(step, False):
            cp.start()

    lax.fori_loop(0, NB - 2, lambda step, c: (start(step), c)[1], 0)

    def step_fn(i, carry):
        b = lax.rem(i, NB)
        rows = pl.ds(pl.multiple_of(i * RA, RA), RA)
        ahead = i + NB - 2

        @pl.when(ahead < STEPS)
        def _():
            @pl.when(ahead >= NB)
            def _():
                for cp in copies(ahead - NB, True):
                    cp.wait()
            start(ahead)

        for cp in copies(i, False):
            cp.wait()
        kn = kn_ref[rows, :].astype(F32)
        vn = vn_ref[rows, :].astype(F32)
        for h in range(4):
            q_s[pl.ds(h, RA, stride=4), :] = q_ref[rows, 128 * h:128 * h + 128].astype(F32)
        slots = slot_ref[rows, :]
        new_rows = []
        for r in range(RA):
            tp = tok_ref[i * RA + r]
            slot = lax.rem(tp, W)
            base = pl.multiple_of((slot // 16) * 16, 16)
            hit = sub == (slot - base)
            spot = pl.ds(base, 16)
            kb[b, r, spot, :] = jnp.where(hit, kn[r:r + 1], kb[b, r, spot, :].astype(F32)).astype(BF)
            vb[b, r, spot, :] = jnp.where(hit, vn[r:r + 1], vb[b, r, spot, :].astype(F32)).astype(BF)
            sn = jnp.where(lane == slot, tp, slots[r:r + 1])
            new_rows.append((tp, sn))
        for r in range(RA):
            tp, sn = new_rows[r]
            so_ref[pl.ds(i * RA + r, 1), :] = sn
            age = tp - sn
            valid = (sn >= 0) & (age >= 0) & (age < W)
            s = lax.dot_general(q_s[4 * r:4 * r + 4, :].astype(BF), kb[b, r], NT, preferred_element_type=F32) * (HD ** -0.5)
            s_s[4 * r:4 * r + 4, :] = jnp.where(valid, s, -jnp.inf)
        s = s_s[...]
        e = jnp.exp(s - jnp.max(s, axis=-1, keepdims=True))
        s_s[...] = e / jnp.sum(e, axis=-1, keepdims=True)
        for r in range(RA):
            o_s[4 * r:4 * r + 4, :] = jnp.dot(s_s[4 * r:4 * r + 4, :].astype(BF), vb[b, r], preferred_element_type=F32)
        for h in range(4):
            o_ref[rows, 128 * h:128 * h + 128] = o_s[pl.ds(h, RA, stride=4), :].astype(BF)
        for cp in copies(i, True):
            cp.start()
        return carry

    lax.fori_loop(0, STEPS, step_fn, 0)
    for step in range(STEPS - NB, STEPS):
        for cp in copies(step, True):
            cp.wait()


def attend(tok, q, kn, vn, slot_pos, kc, vc):
    return pl.pallas_call(
        attn_kernel,
        name='attend',
        in_specs=[pl.BlockSpec(memory_space=pltpu.SMEM), VM, VM, VM, VM, ANY, ANY],
        out_specs=(VM, ANY, ANY, VM),
        out_shape=(jax.ShapeDtypeStruct((B, 4 * HD), BF), jax.ShapeDtypeStruct(kc.shape, BF), jax.ShapeDtypeStruct(vc.shape, BF), jax.ShapeDtypeStruct(slot_pos.shape, jnp.int32)),
        scratch_shapes=[pltpu.VMEM((NB, RA, W, HD), BF), pltpu.VMEM((NB, RA, W, HD), BF), pltpu.VMEM((4 * RA, W), F32), pltpu.VMEM((4 * RA, HD), F32), pltpu.VMEM((4 * RA, HD), F32),
                        pltpu.SemaphoreType.DMA((2, NB)), pltpu.SemaphoreType.DMA((2, NB))],
        cost_estimate=pl.CostEstimate(flops=4 * B * 4 * W * HD, bytes_accessed=8 * B * W * HD, transcendentals=0),
    )(tok, q, kn, vn, slot_pos, kc, vc)


def rope_tables(tok_pos):
    quarter = HD // 4
    lane = lax.broadcasted_iota(jnp.int32, (1, HD), 1)
    inv_freq = ROPE_BASE ** (-(lane % quarter).astype(F32) / quarter)
    angles = tok_pos.astype(F32)[:, None] * inv_freq
    cos, sin = jnp.cos(angles), jnp.sin(angles)
    return jnp.where(lane < 2 * quarter, cos, 1.0), jnp.where(lane < quarter, -sin, jnp.where(lane < 2 * quarter, sin, 0.0))


def io_specs():
    in_specs = (P('dp', None), P('dp'), P(None, 'dp', None, 'tp'), P(None, 'dp', 'tp'), P('dp', None, None), P('dp', None, None), P('dp', None),
                P(), P(None, None, 'tp'), P(None, 'tp'), P(None, None, 'tp'), P(None, 'tp'), P(None, None, 'tp'), P(None, 'tp'),
                P(None, 'tp', None, None), P(None, 'tp'), P(None, 'tp', None, None), P(None, 'tp'), P(None, 'tp'), P(None, 'tp', None), P(),
                P(None, 'tp'), P(), P(), P('tp', None), P(),
                P(None, None, 'tp'), P(None, 'tp'), P(None, None, 'tp'), P(None, 'tp'), P(None, 'tp', None), P())
    out_specs = (P('dp', None), P(None, 'dp', None, 'tp'), P(None, 'dp', 'tp'), P('dp', None, None), P('dp', None, None), P('dp', None))
    return in_specs, out_specs


def solution(mesh):
    in_specs, out_specs = io_specs()

    def local_step(x_in, tok_pos, conv_state, lru_state, k_cache, v_cache, slot_pos, norm_scale, rec_wx, rec_bx, rec_wy, rec_by, conv_w, conv_b, gate_wa, gate_ba, gate_wi, gate_bi, a_param, rec_wout, rec_bout, attn_wq, attn_wk, attn_wv, attn_wo, attn_bo, mlp_w1, mlp_b1, mlp_w2, mlp_b2, mlp_wd, mlp_bd):
        wxt = jnp.swapaxes(rec_wx, 1, 2)
        wyt = jnp.swapaxes(rec_wy, 1, 2)
        convt = jnp.transpose(conv_state, (0, 2, 3, 1))
        lrut = jnp.swapaxes(lru_state, 1, 2)
        tok_row = tok_pos[None, :]
        tab = rope_tables(tok_pos)

        q, kn, vn, x_own, convs, lrus = first_layers(x_in, norm_scale, wxt, wyt, convt, lrut, gate_wa, gate_wi, rec_bx, rec_by, conv_w, conv_b, gate_ba, gate_bi, -8.0 * jax.nn.softplus(a_param), tok_row, rec_wout, rec_bout, mlp_w1, mlp_b1, mlp_w2, mlp_b2, mlp_wd, mlp_bd, attn_wq, attn_wk, attn_wv, *tab)
        o, k_next, v_next, slot_next = attend(tok_pos, q.reshape(B, 4 * HD), kn.reshape(B, HD), vn.reshape(B, HD), slot_pos, k_cache, v_cache)
        x = last_layer(o, x_own, attn_wo, attn_bo[None, :], norm_scale, mlp_w1, mlp_b1, mlp_w2, mlp_b2, mlp_wd, mlp_bd)
        conv_out = jnp.transpose(convs, (0, 3, 1, 2))
        lru_out = jnp.swapaxes(lrus, 1, 2)
        return (x, conv_out, lru_out, k_next, v_next, slot_next)

    return jax.shard_map(local_step, mesh=mesh, in_specs=in_specs, out_specs=out_specs, check_vma=False)
```

```python
import functools

import jax
import jax.numpy as jnp
from jax import lax
from jax.experimental import pallas as pl
from jax.experimental.pallas import tpu as pltpu
from jax.sharding import PartitionSpec as P

ROPE_BASE = 10000.0
NORM_EPS = 1e-6
MESH = pl.DeviceIdType.MESH
BF = jnp.bfloat16
F32 = jnp.float32
ANY = pl.BlockSpec(memory_space=pl.ANY)
VM = pl.BlockSpec(memory_space=pltpu.VMEM)
B = 256
D = 4096
LC = 704
FC = 1536
W = 1024
HD = 128
G = 4
HB = 128
OR = 16
GC = D // G


def rms(x, scale):
    xf = x.astype(F32)
    mean_sq = jnp.mean(xf * xf, axis=-1, keepdims=True)
    return (xf * lax.rsqrt(mean_sq + NORM_EPS) * (1.0 + scale.astype(F32))).astype(BF)


NT = (((1,), (1,)), ((), ()))
TN = (((0,), (0,)), ((), ()))
DMA = pltpu.SemaphoreType.DMA


def chunk(g):
    return pl.ds(pl.multiple_of(g * GC, GC), GC)


SLAB = 512
PER = GC // SLAB


def piece(g, e):
    return pl.ds(pl.multiple_of(g * GC + e * SLAB, SLAB), SLAB)


class Links:
    def __init__(self, part, recv1, recv2, own, n, xown, s1s, s1r, s2s, s2r, s3s, s3r, s4s, s4r, s5s, s5r):
        self.part, self.recv1, self.recv2, self.own, self.n, self.xown = part, recv1, recv2, own, n, xown
        self.s1s, self.s1r, self.s2s, self.s2r, self.s3s, self.s3r, self.s4s, self.s4r, self.s5s, self.s5r = s1s, s1r, s2s, s2r, s3s, s3r, s4s, s4r, s5s, s5r
        t = lax.axis_index('tp')
        y, x = t // 4, (t // 2) % 2
        self.c = t % 2
        self.q = 2 * y + x
        self.partner = 2 * self.q + 1 - self.c
        self.chips = [2 * y + (1 - x), 2 * (1 - y) + x, 2 * (1 - y) + (1 - x)]
        self.peers = [2 * qd + self.c for qd in self.chips]

    def enter(self):
        barrier = pltpu.get_barrier_semaphore()
        for dev in [self.partner] + self.peers:
            pl.semaphore_signal(barrier, inc=1, device_id={'tp': dev}, device_id_type=MESH)
        pl.semaphore_wait(barrier, 4)

    def remote(self, src, dst, ss, rs, dev):
        return pltpu.make_async_remote_copy(src_ref=src, dst_ref=dst, send_sem=ss, recv_sem=rs, device_id={'tp': dev}, device_id_type=MESH)

    def to_partner(self, h, g):
        return self.remote(self.part.at[h, :, 1 - self.c, :, chunk(g)], self.recv1.at[h, :, :, chunk(g)], self.s1s.at[h, g], self.s1r.at[h, g], self.partner)

    def to_owner(self, h, g, k):
        return self.remote(self.part.at[h, self.chips[k], self.c, :, chunk(g)], self.recv2.at[h, k, :, chunk(g)], self.s2s.at[h, g, k], self.s2r.at[h, g, k], self.peers[k])

    def place(self, h, dev, g):
        return self.n.at[h, pl.ds(pl.multiple_of(dev * OR, OR), OR), chunk(g)]

    def from_own(self, h, g, k):
        ref = self.place(h, 2 * self.q + self.c, g)
        return self.remote(ref, ref, self.s3s.at[h, g, k], self.s3r.at[h, g, k], self.peers[k])

    def own_pair(self, h):
        ref = self.n.at[h, pl.ds(pl.multiple_of((2 * self.q + self.c) * OR, OR), OR)]
        return self.remote(ref, ref, self.s5s.at[h], self.s5r.at[h], self.partner)

    def pass_on(self, h, g, k):
        ref = self.place(h, self.peers[k], g)
        return self.remote(ref, ref, self.s4s.at[h, g, k], self.s4r.at[h, g, k], self.partner)

    def scatter(self, h, lhs, rhs, before=None, after=None):
        c, q, chips, part = self.c, self.q, self.chips, self.part

        def pair(g, carry):
            cols = chunk(g)
            self.to_partner(h, g).wait_recv()
            for k in (2, 0, 1):
                s = part[h, chips[k], c, :, cols].astype(F32) + self.recv1[h, chips[k], :, cols].astype(F32)
                part[h, chips[k], c, :, cols] = s.astype(BF)
                self.to_owner(h, g, k).start()
            self.own[h, :, cols] = part[h, q, c, :, cols].astype(F32) + self.recv1[h, q, :, cols].astype(F32)
            return carry

        def step(g, carry):
            if before is not None:
                before(g)
            def tile(p, carry):
                cols = piece(g, p)
                out = jnp.dot(lhs(), rhs(cols), preferred_element_type=F32)
                part[h, :, :, :, cols] = out.astype(BF).reshape(4, 2, OR, SLAB)
                return carry

            lax.fori_loop(0, PER, tile, 0)
            if after is not None:
                after(g)
            self.to_partner(h, g).start()
            return carry

        lax.fori_loop(0, G, step, 0)
        lax.fori_loop(0, G, pair, 0)

    def finish(self, h, bias_ref, layer, scale):
        def final(g, carry):
            cols = chunk(g)
            tot = self.own[h, :, cols]
            for k in range(3):
                self.to_owner(h, g, k).wait_recv()
                tot = tot + self.recv2[h, k, :, cols].astype(F32)
            bias = bias_ref[:, cols].astype(F32)[layer:layer + 1]
            self.xown[h, :, cols] = (self.xown[h, :, cols].astype(F32) + tot.astype(BF).astype(F32) + bias).astype(BF)
            return carry

        lax.fori_loop(0, G, final, 0)

        rows = self.xown[h]
        self.n[h, pl.ds(pl.multiple_of((2 * self.q + self.c) * OR, OR), OR), :] = rows if scale is None else rms(rows, scale)

        self.own_pair(h).start()

        def send(i, carry):
            for k in (2, 0, 1):
                self.from_own(h, order(h, i), k).start()
            return carry

        lax.fori_loop(0, G, send, 0)

        def sent(g, carry):
            self.to_partner(h, g).wait_send()
            for k in range(3):
                self.to_owner(h, g, k).wait_send()
            return carry

        lax.fori_loop(0, G, sent, 0)

    def gathered(self, h, use, fresh=False):
        def forward(i, carry):
            g = order(h, i)
            for k in range(3):
                self.from_own(h, g, k).wait_recv()
                self.pass_on(h, g, k).start()
            return carry

        if h == 1 and not fresh:
            lax.fori_loop(0, G, forward, 0)

        def step(i, carry):
            if h == 0 and not fresh:
                @pl.when(i < G)
                def _():
                    forward(i, 0)

            @pl.when(i > 0)
            def _():
                g = order(h, i - 1)
                if not fresh:
                    @pl.when(i == 1)
                    def _():
                        self.own_pair(h).wait_recv()

                    for k in range(3):
                        self.pass_on(h, g, k).wait_recv()
                use(i - 1, g)

            return carry

        lax.fori_loop(0, G + 1, step, 0)
        if fresh:
            return

        self.own_pair(h).wait_send()

        def sent(g, carry):
            for k in range(3):
                self.from_own(h, g, k).wait_send()
                self.pass_on(h, g, k).wait_send()
            return carry

        lax.fori_loop(0, G, sent, 0)


def order(h, i):
    return lax.rem(i + (G // 2) * h, G)


LINK_SCRATCH = [
    pltpu.VMEM((2, 4, 2, OR, D), BF), pltpu.VMEM((2, 4, OR, D), BF), pltpu.VMEM((2, 3, OR, D), BF),
    pltpu.VMEM((2, OR, D), F32), pltpu.VMEM((2, HB, D), BF), pltpu.VMEM((2, OR, D), BF),
    DMA((2, G)), DMA((2, G)), DMA((2, G, 3)), DMA((2, G, 3)), DMA((2, G, 3)), DMA((2, G, 3)), DMA((2, G, 3)), DMA((2, G, 3)), DMA((2,)), DMA((2,)),
]
NLINK = len(LINK_SCRATCH)

SLOTS = 5
LOADS = 12


class Slabs:
    def __init__(self, groups, wu):
        self.groups, self.wu = groups, wu

    def start(self, load):
        for j, group in enumerate(self.groups):
            @pl.when((load >= LOADS * j) & (load < LOADS * (j + 1)))
            def _():
                for cp in group(load - LOADS * j, load):
                    cp.start()

    def begin(self):
        def body(load, carry):
            self.start(load)
            return carry

        lax.fori_loop(0, SLOTS, body, 0)

    def use(self, h, j, i, body):
        load = LOADS * j + 4 * h + i

        @pl.when(i >= 4 * h)
        def _():
            for cp in self.groups[j](load - LOADS * j, load):
                cp.wait()

        body(lax.rem(load, SLOTS))

        @pl.when((i < 4) | (h == 1))
        def _():
            self.start(load + SLOTS)


def slab_rows(k):
    return pl.ds(pl.multiple_of(lax.rem(k, 8) * SLAB, SLAB), SLAB)


def mlp_slabs(layer, w1, w2, wu, sems):
    def group(k, load):
        s = lax.rem(load, SLOTS)
        return [pltpu.make_async_copy(w1.at[layer, slab_rows(k), :], wu.at[s, 0], sems.at[s, 0]), pltpu.make_async_copy(w2.at[layer, slab_rows(k), :], wu.at[s, 1], sems.at[s, 1])]

    return group


def qkv_slabs(wq, wk, wv, wu, sems):
    def group(k, load):
        s = lax.rem(load, SLOTS)
        return [pltpu.make_async_copy(w.at[slab_rows(k), :], wu.at[s, 0, :, lo:hi], sems.at[s, j]) for j, (w, lo, hi) in enumerate(((wq, 0, 512), (wk, 512, 640), (wv, 640, 768)))]

    return group


def wide(src, dst, sems, g):
    return pltpu.make_async_copy(src.at[:, chunk(g)], dst.at[:, chunk(g)], sems.at[g])


def mlp_up(net, h, slabs, j, acc, h_s, b1_ref, b2_ref, layer):
    acc[...] = jnp.zeros_like(acc)

    def use(i, g):
        def one(e, carry):
            def body(slot):
                ng = net.n[h, :, piece(g, e)]
                for half in range(2):
                    for lo in range(0, FC, 512):
                        acc[half, :, lo:lo + 512] += jnp.dot(ng, slabs.wu[slot, half, :, lo:lo + 512], preferred_element_type=F32)

            slabs.use(h, j, PER * i + e, body)
            return carry

        lax.fori_loop(0, PER, one, 0)

    net.gathered(h, use)
    b1 = b1_ref[...].astype(F32)[layer:layer + 1]
    b2 = b2_ref[...].astype(F32)[layer:layer + 1]
    for lo in range(0, FC, 256):
        lanes = slice(lo, lo + 256)
        h_s[:, lanes] = (jax.nn.gelu(acc[0, :, lanes] + b1[:, lanes], approximate=True) * (acc[1, :, lanes] + b2[:, lanes])).astype(BF)


def mlp(net, slabs, j, acc, h_s, b1_ref, b2_ref, wd, wdb, ds, layer, last):
    for h in range(2):
        mlp_up(net, h, slabs, j, acc, h_s, b1_ref, b2_ref, layer)

        def before(g):
            if h == 0:
                wide(wd.at[layer], wdb, ds, g).wait()

        def after(g):
            if h == 1 and not last:
                wide(wd.at[layer + 1], wdb, ds, g).start()

        net.scatter(h, lambda: h_s[...], lambda cols: wdb[:, cols], before, after)


def rope(v, keep, turn):
    lane = lax.broadcasted_iota(jnp.int32, v.shape, 1)
    return v * keep + jnp.where(lane < 32, pltpu.roll(v, 96, 1), pltpu.roll(v, 32, 1)) * turn


def kernel_a(x_ref, sc_ref, wx, wy, conv, lru, wa_ref, wi_ref, bx_ref, by_ref, cw_ref, cb_ref, ba_ref, bi_ref, sp_ref, tok_ref, wout, rb_ref, w1, b1_ref, w2, b2_ref, wd, mb_ref, wq, wk, wv, keep_ref, turn_ref,
             q_ref, k_ref, v_ref, xo_ref, conv_out, lru_out, *scratch):
    net = Links(*scratch[:NLINK])
    wu, wdb, wxb, wob, acc, accr, h_s, conv_s, xb_s, lru_s, ht_s, prow, pcol, us, ds, xs, os, ss, ts, ls = scratch[NLINK:]
    scale = lambda l, j: sc_ref[...].astype(F32)[l, j:j + 1, :]
    rec_in = lambda l, g: [pltpu.make_async_copy(w.at[l, :, chunk(g)], wxb.at[j, :, chunk(g)], xs.at[j, g]) for j, w in enumerate((wx, wy))]
    state_in = lambda l: [pltpu.make_async_copy(conv.at[l], conv_s, ss.at[0]), pltpu.make_async_copy(lru.at[l], lru_s, ss.at[1])]
    state_out = lambda l: [pltpu.make_async_copy(conv_s.at[1:3], conv_out.at[l, 0:2], ts.at[0]), pltpu.make_async_copy(xb_s, conv_out.at[l, 2], ts.at[1]), pltpu.make_async_copy(lru_s, lru_out.at[l], ts.at[2])]
    slabs = Slabs([mlp_slabs(0, w1, w2, wu, us), mlp_slabs(1, w1, w2, wu, us), qkv_slabs(wq, wk, wv, wu, us)], wu)

    load_x = pltpu.make_async_copy(x_ref, net.part, ls)
    load_x.start()

    def load_rec(l):
        for g in range(G):
            for cp in rec_in(l, g):
                cp.start()

    load_rec(0)
    for cp in state_in(0):
        cp.start()
    for g in range(G):
        wide(wout.at[0], wob, os, g).start()
    net.enter()
    load_x.wait()
    for h in range(2):
        for chip in range(4):
            net.n[h, 2 * OR * chip:2 * OR * (chip + 1), :] = rms(net.part[h, chip].reshape(2 * OR, D), scale(0, 0))
        net.xown[h] = net.part[h, net.q, net.c]
    tok = tok_ref[...]

    for layer in range(2):
        row = lambda ref: ref[...].astype(F32)[layer:layer + 1]
        cw = cw_ref[...].astype(F32)
        params = [row(bx_ref), row(by_ref)] + [cw[layer, j:j + 1, :] for j in range(4)] + [row(cb_ref), row(ba_ref), row(bi_ref), row(sp_ref)]
        for j, p in enumerate(params):
            prow[j:j + 1, 0:LC] = p
        pcol[...] = prow[...].T

        for h in range(2):
            lanes = slice(HB * h, HB * (h + 1))
            accr[...] = jnp.zeros_like(accr)

            def use(i, g):
                if h == 0:
                    for cp in rec_in(layer, g):
                        cp.wait()

                def one(e, carry):
                    cols = pl.ds(pl.multiple_of(g * GC + e * 1024, 1024), 1024)
                    for half in range(2):
                        accr[half] += lax.dot_general(wxb[half, :, cols], net.n[h, :, cols], NT, preferred_element_type=F32)
                    return carry

                lax.fori_loop(0, GC // 1024, one, 0)

            net.gathered(h, use, fresh=layer == 0)
            if h == 0:
                for cp in state_in(layer):
                    cp.wait()
            elif layer == 0:
                slabs.begin()
                for g in range(G):
                    wide(wd.at[0], wdb, ds, g).start()
            tk = tok[:, lanes]
            fresh = tk == 0
            for b in range(4):
                rows = slice(176 * b, 176 * b + 176)
                pc = pcol[rows, :]
                col = lambda k: pc[:, k:k + 1]
                xb = (accr[0, rows, :] + col(0)).astype(BF)
                yb = jax.nn.gelu(accr[1, rows, :] + col(1), approximate=True)
                xb_s[rows, lanes] = xb
                hist = jnp.zeros((176, HB), F32)
                for j in range(3):
                    hist = hist + jnp.where(tk >= 3 - j, conv_s[j, rows, lanes].astype(F32), 0.0) * col(5 - j)
                xc = (col(6) + col(2) * xb.astype(F32) + hist).astype(BF)
                rg = jax.nn.sigmoid(lax.dot_general(wa_ref[layer, b], xc, TN, preferred_element_type=F32) + col(7))
                ig = jax.nn.sigmoid(lax.dot_general(wi_ref[layer, b], xc, TN, preferred_element_type=F32) + col(8))
                a = jnp.exp(rg * col(9))
                sc = jnp.sqrt(1.0 - a * a)
                a = jnp.where(fresh, 0.0, a)
                sc = jnp.where(fresh, 1.0, sc)
                hn = a * lru_s[rows, lanes] + sc * ig * xc.astype(F32)
                lru_s[rows, lanes] = hn
                ht_s[rows, :] = (hn * yb).astype(BF)
            ht_s[LC:, :] = jnp.zeros((64, HB), BF)
            h_s[:, :LC + 64] = ht_s[...].T

            def before(g):
                if h == 0:
                    wide(wout.at[layer], wob, os, g).wait()

            net.scatter(h, lambda: h_s[:, :LC], lambda cols: wob[:, cols], before)
        for cp in state_out(layer):
            cp.start()
        if layer == 0:
            load_rec(1)
            for g in range(G):
                wide(wout.at[1], wob, os, g).start()
        for h in range(2):
            net.finish(h, rb_ref, layer, scale(layer, 1))
        for cp in state_out(layer):
            cp.wait()
        if layer == 0:
            for cp in state_in(1):
                cp.start()
        mlp(net, slabs, layer, acc, h_s, b1_ref, b2_ref, wd, wdb, ds, layer, layer == 1)
        for h in range(2):
            net.finish(h, mb_ref, layer, scale(layer + 1, 0))

    xo_ref[...] = net.xown[...]
    for h in range(2):
        acc[...] = jnp.zeros_like(acc)

        def use_q(i, g):
            def one(e, carry):
                def body(slot):
                    acc[0, :, 0:768] += jnp.dot(net.n[h, :, piece(g, e)], wu[slot, 0, :, 0:768], preferred_element_type=F32)

                slabs.use(h, 2, PER * i + e, body)
                return carry

            lax.fori_loop(0, PER, one, 0)

        net.gathered(h, use_q)
        keep, turn = keep_ref[h], turn_ref[h]
        for b in range(4):
            q_ref[h, :, HD * b:HD * (b + 1)] = rope(acc[0, :, HD * b:HD * (b + 1)], keep, turn).astype(BF)
        k_ref[h] = rope(acc[0, :, 512:640], keep, turn).astype(BF)
        v_ref[h] = acc[0, :, 640:768].astype(BF)


def first_layers(x, scale, wxt, wyt, convt, lrut, wa, wi, bx, by, cw, cb, ba, bi, sp, tok, wout, rb, w1, b1, w2, b2, wd, mb, wq, wk, wv, keep, turn):
    return pl.pallas_call(
        kernel_a,
        name='first_layers',
        out_shape=(jax.ShapeDtypeStruct((2, HB, 4 * HD), BF), jax.ShapeDtypeStruct((2, HB, HD), BF), jax.ShapeDtypeStruct((2, HB, HD), BF), jax.ShapeDtypeStruct((2, OR, D), BF),
                   jax.ShapeDtypeStruct(convt.shape, BF), jax.ShapeDtypeStruct(lrut.shape, F32)),
        in_specs=[ANY, VM, ANY, ANY, ANY, ANY, VM, VM] + [VM] * 7 + [VM, ANY, VM, ANY, VM, ANY, VM, ANY, VM, ANY, ANY, ANY, VM, VM],
        out_specs=(VM, VM, VM, VM, ANY, ANY),
        scratch_shapes=LINK_SCRATCH + [
            pltpu.VMEM((SLOTS, 2, SLAB, FC), BF), pltpu.VMEM((FC, D), BF), pltpu.VMEM((2, LC, D), BF), pltpu.VMEM((LC, D), BF),
            pltpu.VMEM((2, HB, FC), F32), pltpu.VMEM((2, LC, HB), F32), pltpu.VMEM((HB, FC), BF), pltpu.VMEM((3, LC, B), BF), pltpu.VMEM((LC, B), BF), pltpu.VMEM((LC, B), F32),
            pltpu.VMEM((LC + 64, HB), BF), pltpu.VMEM((16, LC + 64), F32), pltpu.VMEM((LC + 64, 16), F32),
            DMA((SLOTS, 3)), DMA((G,)), DMA((2, G)), DMA((G,)), DMA((2,)), DMA((3,)), DMA,
        ],
        compiler_params=pltpu.CompilerParams(collective_id=0, has_side_effects=True, vmem_limit_bytes=67043328),
        cost_estimate=pl.CostEstimate(flops=30 * 10**9, bytes_accessed=400 * 10**6, transcendentals=0),
    )(x.reshape(2, 4, 2, OR, D), scale, wxt, wyt, convt, lrut, wa, wi, bx, by, cw, cb, ba, bi, sp, tok, wout, rb, w1, b1, w2, b2, wd, mb, wq, wk, wv, keep.reshape(2, HB, HD), turn.reshape(2, HB, HD))


def kernel_b(o_ref, x_ref, wo, bo_ref, sc_ref, w1, b1_ref, w2, b2_ref, wd, mb_ref, out_ref, *scratch):
    net = Links(*scratch[:NLINK])
    wu, wdb, wob, acc, h_s, us, ds, os, ls = scratch[NLINK:]
    for g in range(G):
        wide(wo, wob, os, g).start()
    slabs = Slabs([mlp_slabs(2, w1, w2, wu, us)], wu)
    slabs.begin()
    for g in range(G):
        wide(wd.at[2], wdb, ds, g).start()
    net.enter()
    net.xown[...] = x_ref[...]
    for h in range(2):
        def before(g):
            if h == 0:
                wide(wo, wob, os, g).wait()

        net.scatter(h, lambda: o_ref[h], lambda cols: wob[:, cols], before)
    for h in range(2):
        net.finish(h, bo_ref, 0, sc_ref[...].astype(F32)[2, 1:2, :])
    mlp(net, slabs, 0, acc, h_s, b1_ref, b2_ref, wd, wdb, ds, 2, True)
    for h in range(2):
        net.finish(h, mb_ref, 2, None)
    store = lambda h, g: pltpu.make_async_copy(net.n.at[h, :, chunk(g)], out_ref.at[h, :, chunk(g)], ls.at[h, g])
    for h in range(2):
        net.gathered(h, lambda i, g: store(h, g).start())
    for h in range(2):
        for g in range(G):
            store(h, g).wait()


def last_layer(o, x_own, wo, bo, scale, w1, b1, w2, b2, wd, mb):
    out = pl.pallas_call(
        kernel_b,
        name='last_layer',
        out_shape=jax.ShapeDtypeStruct((2, HB, D), BF),
        in_specs=[VM, VM, ANY, VM, VM, ANY, VM, ANY, VM, ANY, VM],
        out_specs=ANY,
        scratch_shapes=LINK_SCRATCH + [
            pltpu.VMEM((SLOTS, 2, SLAB, FC), BF), pltpu.VMEM((FC, D), BF), pltpu.VMEM((4 * HD, D), BF),
            pltpu.VMEM((2, HB, FC), F32), pltpu.VMEM((HB, FC), BF),
            DMA((SLOTS, 3)), DMA((G,)), DMA((G,)), DMA((2, G)),
        ],
        compiler_params=pltpu.CompilerParams(collective_id=1, has_side_effects=True, vmem_limit_bytes=67043328),
        cost_estimate=pl.CostEstimate(flops=12 * 10**9, bytes_accessed=200 * 10**6, transcendentals=0),
    )(o.reshape(2, HB, 4 * HD), x_own, wo, bo, scale, w1, b1, w2, b2, wd, mb)
    return out.reshape(B, D)


RA = 8
NB = 6
STEPS = B // RA


def attn_kernel(tok_ref, q_ref, kn_ref, vn_ref, slot_ref, k_ref, v_ref, o_ref, ko_ref, vo_ref, so_ref, kb, vb, s_s, q_s, o_s, isem, osem):
    lane = lax.broadcasted_iota(jnp.int32, (1, W), 1)
    sub = lax.broadcasted_iota(jnp.int32, (16, HD), 0)

    def copies(step, out):
        b = lax.rem(step, NB)
        rows = pl.ds(pl.multiple_of(step * RA, RA), RA)
        if out:
            return [pltpu.make_async_copy(kb.at[b], ko_ref.at[rows], osem.at[0, b]), pltpu.make_async_copy(vb.at[b], vo_ref.at[rows], osem.at[1, b])]
        return [pltpu.make_async_copy(k_ref.at[rows], kb.at[b], isem.at[0, b]), pltpu.make_async_copy(v_ref.at[rows], vb.at[b], isem.at[1, b])]

    def start(step):
        for cp in copies(step, False):
            cp.start()

    lax.fori_loop(0, NB - 2, lambda step, c: (start(step), c)[1], 0)

    def step_fn(i, carry):
        b = lax.rem(i, NB)
        rows = pl.ds(pl.multiple_of(i * RA, RA), RA)
        ahead = i + NB - 2

        @pl.when(ahead < STEPS)
        def _():
            @pl.when(ahead >= NB)
            def _():
                for cp in copies(ahead - NB, True):
                    cp.wait()
            start(ahead)

        for cp in copies(i, False):
            cp.wait()
        kn = kn_ref[rows, :].astype(F32)
        vn = vn_ref[rows, :].astype(F32)
        for h in range(4):
            q_s[pl.ds(h, RA, stride=4), :] = q_ref[rows, 128 * h:128 * h + 128].astype(F32)
        slots = slot_ref[rows, :]
        new_rows = []
        for r in range(RA):
            tp = tok_ref[i * RA + r]
            slot = lax.rem(tp, W)
            base = pl.multiple_of((slot // 16) * 16, 16)
            hit = sub == (slot - base)
            spot = pl.ds(base, 16)
            kb[b, r, spot, :] = jnp.where(hit, kn[r:r + 1], kb[b, r, spot, :].astype(F32)).astype(BF)
            vb[b, r, spot, :] = jnp.where(hit, vn[r:r + 1], vb[b, r, spot, :].astype(F32)).astype(BF)
            sn = jnp.where(lane == slot, tp, slots[r:r + 1])
            new_rows.append((tp, sn))
        for r in range(RA):
            tp, sn = new_rows[r]
            so_ref[pl.ds(i * RA + r, 1), :] = sn
            age = tp - sn
            valid = (sn >= 0) & (age >= 0) & (age < W)
            s = lax.dot_general(q_s[4 * r:4 * r + 4, :].astype(BF), kb[b, r], NT, preferred_element_type=F32) * (HD ** -0.5)
            s_s[4 * r:4 * r + 4, :] = jnp.where(valid, s, -jnp.inf)
        s = s_s[...]
        e = jnp.exp(s - jnp.max(s, axis=-1, keepdims=True))
        s_s[...] = e / jnp.sum(e, axis=-1, keepdims=True)
        for r in range(RA):
            o_s[4 * r:4 * r + 4, :] = jnp.dot(s_s[4 * r:4 * r + 4, :].astype(BF), vb[b, r], preferred_element_type=F32)
        for h in range(4):
            o_ref[rows, 128 * h:128 * h + 128] = o_s[pl.ds(h, RA, stride=4), :].astype(BF)
        for cp in copies(i, True):
            cp.start()
        return carry

    lax.fori_loop(0, STEPS, step_fn, 0)
    for step in range(STEPS - NB, STEPS):
        for cp in copies(step, True):
            cp.wait()


def attend(tok, q, kn, vn, slot_pos, kc, vc):
    return pl.pallas_call(
        attn_kernel,
        name='attend',
        in_specs=[pl.BlockSpec(memory_space=pltpu.SMEM), VM, VM, VM, VM, ANY, ANY],
        out_specs=(VM, ANY, ANY, VM),
        out_shape=(jax.ShapeDtypeStruct((B, 4 * HD), BF), jax.ShapeDtypeStruct(kc.shape, BF), jax.ShapeDtypeStruct(vc.shape, BF), jax.ShapeDtypeStruct(slot_pos.shape, jnp.int32)),
        scratch_shapes=[pltpu.VMEM((NB, RA, W, HD), BF), pltpu.VMEM((NB, RA, W, HD), BF), pltpu.VMEM((4 * RA, W), F32), pltpu.VMEM((4 * RA, HD), F32), pltpu.VMEM((4 * RA, HD), F32),
                        pltpu.SemaphoreType.DMA((2, NB)), pltpu.SemaphoreType.DMA((2, NB))],
        cost_estimate=pl.CostEstimate(flops=4 * B * 4 * W * HD, bytes_accessed=8 * B * W * HD, transcendentals=0),
    )(tok, q, kn, vn, slot_pos, kc, vc)


def rope_tables(tok_pos):
    quarter = HD // 4
    lane = lax.broadcasted_iota(jnp.int32, (1, HD), 1)
    inv_freq = ROPE_BASE ** (-(lane % quarter).astype(F32) / quarter)
    angles = tok_pos.astype(F32)[:, None] * inv_freq
    cos, sin = jnp.cos(angles), jnp.sin(angles)
    return jnp.where(lane < 2 * quarter, cos, 1.0), jnp.where(lane < quarter, -sin, jnp.where(lane < 2 * quarter, sin, 0.0))


def io_specs():
    in_specs = (P('dp', None), P('dp'), P(None, 'dp', None, 'tp'), P(None, 'dp', 'tp'), P('dp', None, None), P('dp', None, None), P('dp', None),
                P(), P(None, None, 'tp'), P(None, 'tp'), P(None, None, 'tp'), P(None, 'tp'), P(None, None, 'tp'), P(None, 'tp'),
                P(None, 'tp', None, None), P(None, 'tp'), P(None, 'tp', None, None), P(None, 'tp'), P(None, 'tp'), P(None, 'tp', None), P(),
                P(None, 'tp'), P(), P(), P('tp', None), P(),
                P(None, None, 'tp'), P(None, 'tp'), P(None, None, 'tp'), P(None, 'tp'), P(None, 'tp', None), P())
    out_specs = (P('dp', None), P(None, 'dp', None, 'tp'), P(None, 'dp', 'tp'), P('dp', None, None), P('dp', None, None), P('dp', None))
    return in_specs, out_specs


def solution(mesh):
    in_specs, out_specs = io_specs()

    def local_step(x_in, tok_pos, conv_state, lru_state, k_cache, v_cache, slot_pos, norm_scale, rec_wx, rec_bx, rec_wy, rec_by, conv_w, conv_b, gate_wa, gate_ba, gate_wi, gate_bi, a_param, rec_wout, rec_bout, attn_wq, attn_wk, attn_wv, attn_wo, attn_bo, mlp_w1, mlp_b1, mlp_w2, mlp_b2, mlp_wd, mlp_bd):
        wxt = jnp.swapaxes(rec_wx, 1, 2)
        wyt = jnp.swapaxes(rec_wy, 1, 2)
        convt = jnp.transpose(conv_state, (0, 2, 3, 1))
        lrut = jnp.swapaxes(lru_state, 1, 2)
        tok_row = tok_pos[None, :]
        tab = rope_tables(tok_pos)

        q, kn, vn, x_own, convs, lrus = first_layers(x_in, norm_scale, wxt, wyt, convt, lrut, gate_wa, gate_wi, rec_bx, rec_by, conv_w, conv_b, gate_ba, gate_bi, -8.0 * jax.nn.softplus(a_param), tok_row, rec_wout, rec_bout, mlp_w1, mlp_b1, mlp_w2, mlp_b2, mlp_wd, mlp_bd, attn_wq, attn_wk, attn_wv, *tab)
        o, k_next, v_next, slot_next = attend(tok_pos, q.reshape(B, 4 * HD), kn.reshape(B, HD), vn.reshape(B, HD), slot_pos, k_cache, v_cache)
        x = last_layer(o, x_own, attn_wo, attn_bo[None, :], norm_scale, mlp_w1, mlp_b1, mlp_w2, mlp_b2, mlp_wd, mlp_bd)
        conv_out = jnp.transpose(convs, (0, 3, 1, 2))
        lru_out = jnp.swapaxes(lrus, 1, 2)
        return (x, conv_out, lru_out, k_next, v_next, slot_next)

    return jax.shard_map(local_step, mesh=mesh, in_specs=in_specs, out_specs=out_specs, check_vma=False)
```

```python
import functools

import jax
import jax.numpy as jnp
from jax import lax
from jax.experimental import pallas as pl
from jax.experimental.pallas import tpu as pltpu
from jax.sharding import PartitionSpec as P

ROPE_BASE = 10000.0
NORM_EPS = 1e-6
MESH = pl.DeviceIdType.MESH
BF = jnp.bfloat16
F32 = jnp.float32
ANY = pl.BlockSpec(memory_space=pl.ANY)
VM = pl.BlockSpec(memory_space=pltpu.VMEM)
B = 256
D = 4096
LC = 704
FC = 1536
W = 1024
HD = 128
G = 4
HB = 128
OR = 16
GC = D // G


def rms(x, scale):
    xf = x.astype(F32)
    mean_sq = jnp.mean(xf * xf, axis=-1, keepdims=True)
    return (xf * lax.rsqrt(mean_sq + NORM_EPS) * (1.0 + scale.astype(F32))).astype(BF)


NT = (((1,), (1,)), ((), ()))
TN = (((0,), (0,)), ((), ()))
DMA = pltpu.SemaphoreType.DMA


def chunk(g):
    return pl.ds(pl.multiple_of(g * GC, GC), GC)


SLAB = 512
PER = GC // SLAB


def unrolled(count, body):
    for e in range(count):
        body(e, None)


def piece(g, e):
    return pl.ds(pl.multiple_of(g * GC + e * SLAB, SLAB), SLAB)


class Links:
    def __init__(self, part, recv1, recv2, own, n, xown, s1s, s1r, s2s, s2r, s3s, s3r, s4s, s4r, s5s, s5r):
        self.part, self.recv1, self.recv2, self.own, self.n, self.xown = part, recv1, recv2, own, n, xown
        self.s1s, self.s1r, self.s2s, self.s2r, self.s3s, self.s3r, self.s4s, self.s4r, self.s5s, self.s5r = s1s, s1r, s2s, s2r, s3s, s3r, s4s, s4r, s5s, s5r
        t = lax.axis_index('tp')
        y, x = t // 4, (t // 2) % 2
        self.c = t % 2
        self.q = 2 * y + x
        self.partner = 2 * self.q + 1 - self.c
        self.chips = [2 * y + (1 - x), 2 * (1 - y) + x, 2 * (1 - y) + (1 - x)]
        self.peers = [2 * qd + self.c for qd in self.chips]

    def enter(self):
        barrier = pltpu.get_barrier_semaphore()
        for dev in [self.partner] + self.peers:
            pl.semaphore_signal(barrier, inc=1, device_id={'tp': dev}, device_id_type=MESH)
        pl.semaphore_wait(barrier, 4)

    def remote(self, src, dst, ss, rs, dev):
        return pltpu.make_async_remote_copy(src_ref=src, dst_ref=dst, send_sem=ss, recv_sem=rs, device_id={'tp': dev}, device_id_type=MESH)

    def to_partner(self, h, g):
        return self.remote(self.part.at[h, :, 1 - self.c, :, chunk(g)], self.recv1.at[h, :, :, chunk(g)], self.s1s.at[h, g], self.s1r.at[h, g], self.partner)

    def to_owner(self, h, g, k):
        return self.remote(self.part.at[h, self.chips[k], self.c, :, chunk(g)], self.recv2.at[h, k, :, chunk(g)], self.s2s.at[h, g, k], self.s2r.at[h, g, k], self.peers[k])

    def place(self, h, dev, g):
        return self.n.at[h, pl.ds(pl.multiple_of(dev * OR, OR), OR), chunk(g)]

    def from_own(self, h, g, k):
        ref = self.place(h, 2 * self.q + self.c, g)
        return self.remote(ref, ref, self.s3s.at[h, g, k], self.s3r.at[h, g, k], self.peers[k])

    def own_pair(self, h):
        ref = self.n.at[h, pl.ds(pl.multiple_of((2 * self.q + self.c) * OR, OR), OR)]
        return self.remote(ref, ref, self.s5s.at[h], self.s5r.at[h], self.partner)

    def pass_on(self, h, g, k):
        ref = self.place(h, self.peers[k], g)
        return self.remote(ref, ref, self.s4s.at[h, g, k], self.s4r.at[h, g, k], self.partner)

    def scatter(self, h, lhs, rhs, before=None, after=None):
        c, q, chips, part = self.c, self.q, self.chips, self.part

        def pair(g, carry):
            cols = chunk(g)
            self.to_partner(h, g).wait_recv()
            for k in (2, 0, 1):
                s = part[h, chips[k], c, :, cols].astype(F32) + self.recv1[h, chips[k], :, cols].astype(F32)
                part[h, chips[k], c, :, cols] = s.astype(BF)
                self.to_owner(h, g, k).start()
            self.own[h, :, cols] = part[h, q, c, :, cols].astype(F32) + self.recv1[h, q, :, cols].astype(F32)
            return carry

        def step(g, carry):
            if before is not None:
                before(g)
            def tile(p, carry):
                cols = piece(g, p)
                out = jnp.dot(lhs(), rhs(cols), preferred_element_type=F32)
                part[h, :, :, :, cols] = out.astype(BF).reshape(4, 2, OR, SLAB)
                return carry

            unrolled(PER, tile)
            if after is not None:
                after(g)
            self.to_partner(h, g).start()
            return carry

        lax.fori_loop(0, G, step, 0)
        lax.fori_loop(0, G, pair, 0)

    def finish(self, h, bias_ref, layer, scale):
        def final(g, carry):
            cols = chunk(g)
            tot = self.own[h, :, cols]
            for k in range(3):
                self.to_owner(h, g, k).wait_recv()
                tot = tot + self.recv2[h, k, :, cols].astype(F32)
            bias = bias_ref[:, cols].astype(F32)[layer:layer + 1]
            self.xown[h, :, cols] = (self.xown[h, :, cols].astype(F32) + tot.astype(BF).astype(F32) + bias).astype(BF)
            return carry

        lax.fori_loop(0, G, final, 0)

        rows = self.xown[h]
        self.n[h, pl.ds(pl.multiple_of((2 * self.q + self.c) * OR, OR), OR), :] = rows if scale is None else rms(rows, scale)

        self.own_pair(h).start()

        def send(i, carry):
            for k in (2, 0, 1):
                self.from_own(h, order(h, i), k).start()
            return carry

        lax.fori_loop(0, G, send, 0)

        def sent(g, carry):
            self.to_partner(h, g).wait_send()
            for k in range(3):
                self.to_owner(h, g, k).wait_send()
            return carry

        lax.fori_loop(0, G, sent, 0)

    def gathered(self, h, use, fresh=False):
        def forward(i, carry):
            g = order(h, i)
            for k in range(3):
                self.from_own(h, g, k).wait_recv()
                self.pass_on(h, g, k).start()
            return carry

        def step(i, carry):
            if not fresh:
                @pl.when(i < G)
                def _():
                    forward(i, 0)

            @pl.when(i > 0)
            def _():
                g = order(h, i - 1)
                if not fresh:
                    @pl.when(i == 1)
                    def _():
                        self.own_pair(h).wait_recv()

                    for k in range(3):
                        self.pass_on(h, g, k).wait_recv()
                use(i - 1, g)

            return carry

        lax.fori_loop(0, G + 1, step, 0)
        if fresh:
            return

        self.own_pair(h).wait_send()

        def sent(g, carry):
            for k in range(3):
                self.from_own(h, g, k).wait_send()
                self.pass_on(h, g, k).wait_send()
            return carry

        lax.fori_loop(0, G, sent, 0)


def order(h, i):
    return lax.rem(i + (G // 2) * h, G)


LINK_SCRATCH = [
    pltpu.VMEM((2, 4, 2, OR, D), BF), pltpu.VMEM((2, 4, OR, D), BF), pltpu.VMEM((2, 3, OR, D), BF),
    pltpu.VMEM((2, OR, D), F32), pltpu.VMEM((2, HB, D), BF), pltpu.VMEM((2, OR, D), BF),
    DMA((2, G)), DMA((2, G)), DMA((2, G, 3)), DMA((2, G, 3)), DMA((2, G, 3)), DMA((2, G, 3)), DMA((2, G, 3)), DMA((2, G, 3)), DMA((2,)), DMA((2,)),
]
NLINK = len(LINK_SCRATCH)

SLOTS = 5
LOADS = 12


class Slabs:
    def __init__(self, groups, wu):
        self.groups, self.wu = groups, wu

    def start(self, load):
        for j, group in enumerate(self.groups):
            @pl.when((load >= LOADS * j) & (load < LOADS * (j + 1)))
            def _():
                for cp in group(load - LOADS * j, load):
                    cp.start()

    def begin(self):
        def body(load, carry):
            self.start(load)
            return carry

        lax.fori_loop(0, SLOTS, body, 0)

    def use(self, h, j, i, body):
        load = LOADS * j + 4 * h + i

        @pl.when(i >= 4 * h)
        def _():
            for cp in self.groups[j](load - LOADS * j, load):
                cp.wait()

        body(lax.rem(load, SLOTS))

        @pl.when((i < 4) | (h == 1))
        def _():
            self.start(load + SLOTS)


def slab_rows(k):
    return pl.ds(pl.multiple_of(lax.rem(k, 8) * SLAB, SLAB), SLAB)


def mlp_slabs(layer, w1, w2, wu, sems):
    def group(k, load):
        s = lax.rem(load, SLOTS)
        return [pltpu.make_async_copy(w1.at[layer, slab_rows(k), :], wu.at[s, 0], sems.at[s, 0]), pltpu.make_async_copy(w2.at[layer, slab_rows(k), :], wu.at[s, 1], sems.at[s, 1])]

    return group


def qkv_slabs(wq, wk, wv, wu, sems):
    def group(k, load):
        s = lax.rem(load, SLOTS)
        return [pltpu.make_async_copy(w.at[slab_rows(k), :], wu.at[s, 0, :, lo:hi], sems.at[s, j]) for j, (w, lo, hi) in enumerate(((wq, 0, 512), (wk, 512, 640), (wv, 640, 768)))]

    return group


def wide(src, dst, sems, g):
    return pltpu.make_async_copy(src.at[:, chunk(g)], dst.at[:, chunk(g)], sems.at[g])


def mlp_up(net, h, slabs, j, acc, h_s, b1_ref, b2_ref, layer):
    acc[...] = jnp.zeros_like(acc)

    def use(i, g):
        def one(e, carry):
            def body(slot):
                ng = net.n[h, :, piece(g, e)]
                for half in range(2):
                    for lo in range(0, FC, 512):
                        acc[half, :, lo:lo + 512] += jnp.dot(ng, slabs.wu[slot, half, :, lo:lo + 512], preferred_element_type=F32)

            slabs.use(h, j, PER * i + e, body)
            return carry

        unrolled(PER, one)

    net.gathered(h, use)
    b1 = b1_ref[...].astype(F32)[layer:layer + 1]
    b2 = b2_ref[...].astype(F32)[layer:layer + 1]
    for lo in range(0, FC, 256):
        lanes = slice(lo, lo + 256)
        h_s[:, lanes] = (jax.nn.gelu(acc[0, :, lanes] + b1[:, lanes], approximate=True) * (acc[1, :, lanes] + b2[:, lanes])).astype(BF)


def mlp(net, slabs, j, acc, h_s, b1_ref, b2_ref, wd, wdb, ds, layer, last):
    for h in range(2):
        mlp_up(net, h, slabs, j, acc, h_s, b1_ref, b2_ref, layer)

        def before(g):
            if h == 0:
                wide(wd.at[layer], wdb, ds, g).wait()

        def after(g):
            if h == 1 and not last:
                wide(wd.at[layer + 1], wdb, ds, g).start()

        net.scatter(h, lambda: h_s[...], lambda cols: wdb[:, cols], before, after)


def rope(v, keep, turn):
    lane = lax.broadcasted_iota(jnp.int32, v.shape, 1)
    return v * keep + jnp.where(lane < 32, pltpu.roll(v, 96, 1), pltpu.roll(v, 32, 1)) * turn


def kernel_a(x_ref, sc_ref, wx, wy, conv, lru, wa_ref, wi_ref, bx_ref, by_ref, cw_ref, cb_ref, ba_ref, bi_ref, sp_ref, tok_ref, wout, rb_ref, w1, b1_ref, w2, b2_ref, wd, mb_ref, wq, wk, wv, keep_ref, turn_ref,
             q_ref, k_ref, v_ref, xo_ref, conv_out, lru_out, *scratch):
    net = Links(*scratch[:NLINK])
    wu, wdb, wxb, wob, acc, accr, h_s, conv_s, xb_s, lru_s, ht_s, prow, pcol, us, ds, xs, os, ss, ts, ls = scratch[NLINK:]
    scale = lambda l, j: sc_ref[...].astype(F32)[l, j:j + 1, :]
    rec_in = lambda l, g: [pltpu.make_async_copy(w.at[l, :, chunk(g)], wxb.at[j, :, chunk(g)], xs.at[j, g]) for j, w in enumerate((wx, wy))]
    state_in = lambda l: [pltpu.make_async_copy(conv.at[l], conv_s, ss.at[0]), pltpu.make_async_copy(lru.at[l], lru_s, ss.at[1])]
    state_out = lambda l: [pltpu.make_async_copy(conv_s.at[1:3], conv_out.at[l, 0:2], ts.at[0]), pltpu.make_async_copy(xb_s, conv_out.at[l, 2], ts.at[1]), pltpu.make_async_copy(lru_s, lru_out.at[l], ts.at[2])]
    slabs = Slabs([mlp_slabs(0, w1, w2, wu, us), mlp_slabs(1, w1, w2, wu, us), qkv_slabs(wq, wk, wv, wu, us)], wu)

    load_x = pltpu.make_async_copy(x_ref, net.part, ls)
    load_x.start()

    def load_rec(l):
        for g in range(G):
            for cp in rec_in(l, g):
                cp.start()

    load_rec(0)
    for cp in state_in(0):
        cp.start()
    for g in range(G):
        wide(wout.at[0], wob, os, g).start()
    net.enter()
    load_x.wait()
    for h in range(2):
        for chip in range(4):
            net.n[h, 2 * OR * chip:2 * OR * (chip + 1), :] = rms(net.part[h, chip].reshape(2 * OR, D), scale(0, 0))
        net.xown[h] = net.part[h, net.q, net.c]
    tok = tok_ref[...]

    for layer in range(2):
        row = lambda ref: ref[...].astype(F32)[layer:layer + 1]
        cw = cw_ref[...].astype(F32)
        params = [row(bx_ref), row(by_ref)] + [cw[layer, j:j + 1, :] for j in range(4)] + [row(cb_ref), row(ba_ref), row(bi_ref), row(sp_ref)]
        for j, p in enumerate(params):
            prow[j:j + 1, 0:LC] = p
        pcol[...] = prow[...].T

        for h in range(2):
            lanes = slice(HB * h, HB * (h + 1))
            accr[...] = jnp.zeros_like(accr)

            def use(i, g):
                if h == 0:
                    for cp in rec_in(layer, g):
                        cp.wait()

                def one(e, carry):
                    cols = pl.ds(pl.multiple_of(g * GC + e * 1024, 1024), 1024)
                    for half in range(2):
                        accr[half] += lax.dot_general(wxb[half, :, cols], net.n[h, :, cols], NT, preferred_element_type=F32)
                    return carry

                unrolled(GC // 1024, one)

            net.gathered(h, use, fresh=layer == 0)
            if h == 0:
                for cp in state_in(layer):
                    cp.wait()
            elif layer == 0:
                slabs.begin()
                for g in range(G):
                    wide(wd.at[0], wdb, ds, g).start()
            tk = tok[:, lanes]
            fresh = tk == 0
            for b in range(4):
                rows = slice(176 * b, 176 * b + 176)
                pc = pcol[rows, :]
                col = lambda k: pc[:, k:k + 1]
                xb = (accr[0, rows, :] + col(0)).astype(BF)
                yb = jax.nn.gelu(accr[1, rows, :] + col(1), approximate=True)
                xb_s[rows, lanes] = xb
                hist = jnp.zeros((176, HB), F32)
                for j in range(3):
                    hist = hist + jnp.where(tk >= 3 - j, conv_s[j, rows, lanes].astype(F32), 0.0) * col(5 - j)
                xc = (col(6) + col(2) * xb.astype(F32) + hist).astype(BF)
                rg = jax.nn.sigmoid(lax.dot_general(wa_ref[layer, b], xc, TN, preferred_element_type=F32) + col(7))
                ig = jax.nn.sigmoid(lax.dot_general(wi_ref[layer, b], xc, TN, preferred_element_type=F32) + col(8))
                a = jnp.exp(rg * col(9))
                sc = jnp.sqrt(1.0 - a * a)
                a = jnp.where(fresh, 0.0, a)
                sc = jnp.where(fresh, 1.0, sc)
                hn = a * lru_s[rows, lanes] + sc * ig * xc.astype(F32)
                lru_s[rows, lanes] = hn
                ht_s[rows, :] = (hn * yb).astype(BF)
            ht_s[LC:, :] = jnp.zeros((64, HB), BF)
            h_s[:, :LC + 64] = ht_s[...].T

            def before(g):
                if h == 0:
                    wide(wout.at[layer], wob, os, g).wait()

            net.scatter(h, lambda: h_s[:, :LC], lambda cols: wob[:, cols], before)
        for cp in state_out(layer):
            cp.start()
        if layer == 0:
            load_rec(1)
            for g in range(G):
                wide(wout.at[1], wob, os, g).start()
        for h in range(2):
            net.finish(h, rb_ref, layer, scale(layer, 1))
        for cp in state_out(layer):
            cp.wait()
        if layer == 0:
            for cp in state_in(1):
                cp.start()
        mlp(net, slabs, layer, acc, h_s, b1_ref, b2_ref, wd, wdb, ds, layer, layer == 1)
        for h in range(2):
            net.finish(h, mb_ref, layer, scale(layer + 1, 0))

    xo_ref[...] = net.xown[...]
    for h in range(2):
        acc[...] = jnp.zeros_like(acc)

        def use_q(i, g):
            def one(e, carry):
                def body(slot):
                    acc[0, :, 0:768] += jnp.dot(net.n[h, :, piece(g, e)], wu[slot, 0, :, 0:768], preferred_element_type=F32)

                slabs.use(h, 2, PER * i + e, body)
                return carry

            unrolled(PER, one)

        net.gathered(h, use_q)
        keep, turn = keep_ref[h], turn_ref[h]
        for b in range(4):
            q_ref[h, :, HD * b:HD * (b + 1)] = rope(acc[0, :, HD * b:HD * (b + 1)], keep, turn).astype(BF)
        k_ref[h] = rope(acc[0, :, 512:640], keep, turn).astype(BF)
        v_ref[h] = acc[0, :, 640:768].astype(BF)


def first_layers(x, scale, wxt, wyt, convt, lrut, wa, wi, bx, by, cw, cb, ba, bi, sp, tok, wout, rb, w1, b1, w2, b2, wd, mb, wq, wk, wv, keep, turn):
    return pl.pallas_call(
        kernel_a,
        name='first_layers',
        out_shape=(jax.ShapeDtypeStruct((2, HB, 4 * HD), BF), jax.ShapeDtypeStruct((2, HB, HD), BF), jax.ShapeDtypeStruct((2, HB, HD), BF), jax.ShapeDtypeStruct((2, OR, D), BF),
                   jax.ShapeDtypeStruct(convt.shape, BF), jax.ShapeDtypeStruct(lrut.shape, F32)),
        in_specs=[ANY, VM, ANY, ANY, ANY, ANY, VM, VM] + [VM] * 7 + [VM, ANY, VM, ANY, VM, ANY, VM, ANY, VM, ANY, ANY, ANY, VM, VM],
        out_specs=(VM, VM, VM, VM, ANY, ANY),
        scratch_shapes=LINK_SCRATCH + [
            pltpu.VMEM((SLOTS, 2, SLAB, FC), BF), pltpu.VMEM((FC, D), BF), pltpu.VMEM((2, LC, D), BF), pltpu.VMEM((LC, D), BF),
            pltpu.VMEM((2, HB, FC), F32), pltpu.VMEM((2, LC, HB), F32), pltpu.VMEM((HB, FC), BF), pltpu.VMEM((3, LC, B), BF), pltpu.VMEM((LC, B), BF), pltpu.VMEM((LC, B), F32),
            pltpu.VMEM((LC + 64, HB), BF), pltpu.VMEM((16, LC + 64), F32), pltpu.VMEM((LC + 64, 16), F32),
            DMA((SLOTS, 3)), DMA((G,)), DMA((2, G)), DMA((G,)), DMA((2,)), DMA((3,)), DMA,
        ],
        compiler_params=pltpu.CompilerParams(collective_id=0, has_side_effects=True, vmem_limit_bytes=67043328),
        cost_estimate=pl.CostEstimate(flops=30 * 10**9, bytes_accessed=400 * 10**6, transcendentals=0),
    )(x.reshape(2, 4, 2, OR, D), scale, wxt, wyt, convt, lrut, wa, wi, bx, by, cw, cb, ba, bi, sp, tok, wout, rb, w1, b1, w2, b2, wd, mb, wq, wk, wv, keep.reshape(2, HB, HD), turn.reshape(2, HB, HD))


def kernel_b(o_ref, x_ref, wo, bo_ref, sc_ref, w1, b1_ref, w2, b2_ref, wd, mb_ref, out_ref, *scratch):
    net = Links(*scratch[:NLINK])
    wu, wdb, wob, acc, h_s, us, ds, os, ls = scratch[NLINK:]
    for g in range(G):
        wide(wo, wob, os, g).start()
    slabs = Slabs([mlp_slabs(2, w1, w2, wu, us)], wu)
    slabs.begin()
    for g in range(G):
        wide(wd.at[2], wdb, ds, g).start()
    net.enter()
    net.xown[...] = x_ref[...]
    for h in range(2):
        def before(g):
            if h == 0:
                wide(wo, wob, os, g).wait()

        net.scatter(h, lambda: o_ref[h], lambda cols: wob[:, cols], before)
    for h in range(2):
        net.finish(h, bo_ref, 0, sc_ref[...].astype(F32)[2, 1:2, :])
    mlp(net, slabs, 0, acc, h_s, b1_ref, b2_ref, wd, wdb, ds, 2, True)
    for h in range(2):
        net.finish(h, mb_ref, 2, None)
    store = lambda h, g: pltpu.make_async_copy(net.n.at[h, :, chunk(g)], out_ref.at[h, :, chunk(g)], ls.at[h, g])
    for h in range(2):
        net.gathered(h, lambda i, g: store(h, g).start())
    for h in range(2):
        for g in range(G):
            store(h, g).wait()


def last_layer(o, x_own, wo, bo, scale, w1, b1, w2, b2, wd, mb):
    out = pl.pallas_call(
        kernel_b,
        name='last_layer',
        out_shape=jax.ShapeDtypeStruct((2, HB, D), BF),
        in_specs=[VM, VM, ANY, VM, VM, ANY, VM, ANY, VM, ANY, VM],
        out_specs=ANY,
        scratch_shapes=LINK_SCRATCH + [
            pltpu.VMEM((SLOTS, 2, SLAB, FC), BF), pltpu.VMEM((FC, D), BF), pltpu.VMEM((4 * HD, D), BF),
            pltpu.VMEM((2, HB, FC), F32), pltpu.VMEM((HB, FC), BF),
            DMA((SLOTS, 3)), DMA((G,)), DMA((G,)), DMA((2, G)),
        ],
        compiler_params=pltpu.CompilerParams(collective_id=1, has_side_effects=True, vmem_limit_bytes=67043328),
        cost_estimate=pl.CostEstimate(flops=12 * 10**9, bytes_accessed=200 * 10**6, transcendentals=0),
    )(o.reshape(2, HB, 4 * HD), x_own, wo, bo, scale, w1, b1, w2, b2, wd, mb)
    return out.reshape(B, D)


RA = 8
NB = 6
STEPS = B // RA


def attn_kernel(tok_ref, q_ref, kn_ref, vn_ref, slot_ref, k_ref, v_ref, o_ref, ko_ref, vo_ref, so_ref, kb, vb, s_s, q_s, o_s, isem, osem):
    lane = lax.broadcasted_iota(jnp.int32, (1, W), 1)
    sub = lax.broadcasted_iota(jnp.int32, (16, HD), 0)

    def copies(step, out):
        b = lax.rem(step, NB)
        rows = pl.ds(pl.multiple_of(step * RA, RA), RA)
        if out:
            return [pltpu.make_async_copy(kb.at[b], ko_ref.at[rows], osem.at[0, b]), pltpu.make_async_copy(vb.at[b], vo_ref.at[rows], osem.at[1, b])]
        return [pltpu.make_async_copy(k_ref.at[rows], kb.at[b], isem.at[0, b]), pltpu.make_async_copy(v_ref.at[rows], vb.at[b], isem.at[1, b])]

    def start(step):
        for cp in copies(step, False):
            cp.start()

    lax.fori_loop(0, NB - 2, lambda step, c: (start(step), c)[1], 0)

    def step_fn(i, carry):
        b = lax.rem(i, NB)
        rows = pl.ds(pl.multiple_of(i * RA, RA), RA)
        ahead = i + NB - 2

        @pl.when(ahead < STEPS)
        def _():
            @pl.when(ahead >= NB)
            def _():
                for cp in copies(ahead - NB, True):
                    cp.wait()
            start(ahead)

        for cp in copies(i, False):
            cp.wait()
        kn = kn_ref[rows, :].astype(F32)
        vn = vn_ref[rows, :].astype(F32)
        for h in range(4):
            q_s[pl.ds(h, RA, stride=4), :] = q_ref[rows, 128 * h:128 * h + 128].astype(F32)
        slots = slot_ref[rows, :]
        new_rows = []
        for r in range(RA):
            tp = tok_ref[i * RA + r]
            slot = lax.rem(tp, W)
            base = pl.multiple_of((slot // 16) * 16, 16)
            hit = sub == (slot - base)
            spot = pl.ds(base, 16)
            kb[b, r, spot, :] = jnp.where(hit, kn[r:r + 1], kb[b, r, spot, :].astype(F32)).astype(BF)
            vb[b, r, spot, :] = jnp.where(hit, vn[r:r + 1], vb[b, r, spot, :].astype(F32)).astype(BF)
            sn = jnp.where(lane == slot, tp, slots[r:r + 1])
            new_rows.append((tp, sn))
        for r in range(RA):
            tp, sn = new_rows[r]
            so_ref[pl.ds(i * RA + r, 1), :] = sn
            age = tp - sn
            valid = (sn >= 0) & (age >= 0) & (age < W)
            s = lax.dot_general(q_s[4 * r:4 * r + 4, :].astype(BF), kb[b, r], NT, preferred_element_type=F32) * (HD ** -0.5)
            s_s[4 * r:4 * r + 4, :] = jnp.where(valid, s, -jnp.inf)
        s = s_s[...]
        e = jnp.exp(s - jnp.max(s, axis=-1, keepdims=True))
        s_s[...] = e / jnp.sum(e, axis=-1, keepdims=True)
        for r in range(RA):
            o_s[4 * r:4 * r + 4, :] = jnp.dot(s_s[4 * r:4 * r + 4, :].astype(BF), vb[b, r], preferred_element_type=F32)
        for h in range(4):
            o_ref[rows, 128 * h:128 * h + 128] = o_s[pl.ds(h, RA, stride=4), :].astype(BF)
        for cp in copies(i, True):
            cp.start()
        return carry

    lax.fori_loop(0, STEPS, step_fn, 0)
    for step in range(STEPS - NB, STEPS):
        for cp in copies(step, True):
            cp.wait()


def attend(tok, q, kn, vn, slot_pos, kc, vc):
    return pl.pallas_call(
        attn_kernel,
        name='attend',
        in_specs=[pl.BlockSpec(memory_space=pltpu.SMEM), VM, VM, VM, VM, ANY, ANY],
        out_specs=(VM, ANY, ANY, VM),
        out_shape=(jax.ShapeDtypeStruct((B, 4 * HD), BF), jax.ShapeDtypeStruct(kc.shape, BF), jax.ShapeDtypeStruct(vc.shape, BF), jax.ShapeDtypeStruct(slot_pos.shape, jnp.int32)),
        scratch_shapes=[pltpu.VMEM((NB, RA, W, HD), BF), pltpu.VMEM((NB, RA, W, HD), BF), pltpu.VMEM((4 * RA, W), F32), pltpu.VMEM((4 * RA, HD), F32), pltpu.VMEM((4 * RA, HD), F32),
                        pltpu.SemaphoreType.DMA((2, NB)), pltpu.SemaphoreType.DMA((2, NB))],
        cost_estimate=pl.CostEstimate(flops=4 * B * 4 * W * HD, bytes_accessed=8 * B * W * HD, transcendentals=0),
    )(tok, q, kn, vn, slot_pos, kc, vc)


def rope_tables(tok_pos):
    quarter = HD // 4
    lane = lax.broadcasted_iota(jnp.int32, (1, HD), 1)
    inv_freq = ROPE_BASE ** (-(lane % quarter).astype(F32) / quarter)
    angles = tok_pos.astype(F32)[:, None] * inv_freq
    cos, sin = jnp.cos(angles), jnp.sin(angles)
    return jnp.where(lane < 2 * quarter, cos, 1.0), jnp.where(lane < quarter, -sin, jnp.where(lane < 2 * quarter, sin, 0.0))


def io_specs():
    in_specs = (P('dp', None), P('dp'), P(None, 'dp', None, 'tp'), P(None, 'dp', 'tp'), P('dp', None, None), P('dp', None, None), P('dp', None),
                P(), P(None, None, 'tp'), P(None, 'tp'), P(None, None, 'tp'), P(None, 'tp'), P(None, None, 'tp'), P(None, 'tp'),
                P(None, 'tp', None, None), P(None, 'tp'), P(None, 'tp', None, None), P(None, 'tp'), P(None, 'tp'), P(None, 'tp', None), P(),
                P(None, 'tp'), P(), P(), P('tp', None), P(),
                P(None, None, 'tp'), P(None, 'tp'), P(None, None, 'tp'), P(None, 'tp'), P(None, 'tp', None), P())
    out_specs = (P('dp', None), P(None, 'dp', None, 'tp'), P(None, 'dp', 'tp'), P('dp', None, None), P('dp', None, None), P('dp', None))
    return in_specs, out_specs


def solution(mesh):
    in_specs, out_specs = io_specs()

    def local_step(x_in, tok_pos, conv_state, lru_state, k_cache, v_cache, slot_pos, norm_scale, rec_wx, rec_bx, rec_wy, rec_by, conv_w, conv_b, gate_wa, gate_ba, gate_wi, gate_bi, a_param, rec_wout, rec_bout, attn_wq, attn_wk, attn_wv, attn_wo, attn_bo, mlp_w1, mlp_b1, mlp_w2, mlp_b2, mlp_wd, mlp_bd):
        wxt = jnp.swapaxes(rec_wx, 1, 2)
        wyt = jnp.swapaxes(rec_wy, 1, 2)
        convt = jnp.transpose(conv_state, (0, 2, 3, 1))
        lrut = jnp.swapaxes(lru_state, 1, 2)
        tok_row = tok_pos[None, :]
        tab = rope_tables(tok_pos)

        q, kn, vn, x_own, convs, lrus = first_layers(x_in, norm_scale, wxt, wyt, convt, lrut, gate_wa, gate_wi, rec_bx, rec_by, conv_w, conv_b, gate_ba, gate_bi, -8.0 * jax.nn.softplus(a_param), tok_row, rec_wout, rec_bout, mlp_w1, mlp_b1, mlp_w2, mlp_b2, mlp_wd, mlp_bd, attn_wq, attn_wk, attn_wv, *tab)
        o, k_next, v_next, slot_next = attend(tok_pos, q.reshape(B, 4 * HD), kn.reshape(B, HD), vn.reshape(B, HD), slot_pos, k_cache, v_cache)
        x = last_layer(o, x_own, attn_wo, attn_bo[None, :], norm_scale, mlp_w1, mlp_b1, mlp_w2, mlp_b2, mlp_wd, mlp_bd)
        conv_out = jnp.transpose(convs, (0, 3, 1, 2))
        lru_out = jnp.swapaxes(lrus, 1, 2)
        return (x, conv_out, lru_out, k_next, v_next, slot_next)

    return jax.shard_map(local_step, mesh=mesh, in_specs=in_specs, out_specs=out_specs, check_vma=False)
```

```python
import functools

import jax
import jax.numpy as jnp
from jax import lax
from jax.experimental import pallas as pl
from jax.experimental.pallas import tpu as pltpu
from jax.sharding import PartitionSpec as P

ROPE_BASE = 10000.0
NORM_EPS = 1e-6
MESH = pl.DeviceIdType.MESH
BF = jnp.bfloat16
F32 = jnp.float32
ANY = pl.BlockSpec(memory_space=pl.ANY)
VM = pl.BlockSpec(memory_space=pltpu.VMEM)
B = 256
D = 4096
LC = 704
FC = 1536
W = 1024
HD = 128
G = 4
HB = 128
OR = 16
GC = D // G


def rms(x, scale):
    xf = x.astype(F32)
    mean_sq = jnp.mean(xf * xf, axis=-1, keepdims=True)
    return (xf * lax.rsqrt(mean_sq + NORM_EPS) * (1.0 + scale.astype(F32))).astype(BF)


NT = (((1,), (1,)), ((), ()))
TN = (((0,), (0,)), ((), ()))
DMA = pltpu.SemaphoreType.DMA


def chunk(g):
    return pl.ds(pl.multiple_of(g * GC, GC), GC)


SLAB = 512
PER = GC // SLAB


def unrolled(count, body):
    for e in range(count):
        body(e, None)


def piece(g, e):
    return pl.ds(pl.multiple_of(g * GC + e * SLAB, SLAB), SLAB)


class Links:
    def __init__(self, part, recv1, recv2, own, n, xown, s1s, s1r, s2s, s2r, s3s, s3r, s4s, s4r, s5s, s5r):
        self.part, self.recv1, self.recv2, self.own, self.n, self.xown = part, recv1, recv2, own, n, xown
        self.s1s, self.s1r, self.s2s, self.s2r, self.s3s, self.s3r, self.s4s, self.s4r, self.s5s, self.s5r = s1s, s1r, s2s, s2r, s3s, s3r, s4s, s4r, s5s, s5r
        t = lax.axis_index('tp')
        y, x = t // 4, (t // 2) % 2
        self.c = t % 2
        self.q = 2 * y + x
        self.partner = 2 * self.q + 1 - self.c
        self.chips = [2 * y + (1 - x), 2 * (1 - y) + x, 2 * (1 - y) + (1 - x)]
        self.peers = [2 * qd + self.c for qd in self.chips]

    def enter(self):
        barrier = pltpu.get_barrier_semaphore()
        for dev in [self.partner] + self.peers:
            pl.semaphore_signal(barrier, inc=1, device_id={'tp': dev}, device_id_type=MESH)
        pl.semaphore_wait(barrier, 4)

    def remote(self, src, dst, ss, rs, dev):
        return pltpu.make_async_remote_copy(src_ref=src, dst_ref=dst, send_sem=ss, recv_sem=rs, device_id={'tp': dev}, device_id_type=MESH)

    def to_partner(self, h, g):
        return self.remote(self.part.at[h, :, 1 - self.c, :, chunk(g)], self.recv1.at[h, :, :, chunk(g)], self.s1s.at[h, g], self.s1r.at[h, g], self.partner)

    def to_owner(self, h, g, k):
        return self.remote(self.part.at[h, self.chips[k], self.c, :, chunk(g)], self.recv2.at[h, k, :, chunk(g)], self.s2s.at[h, g, k], self.s2r.at[h, g, k], self.peers[k])

    def place(self, h, dev, g):
        return self.n.at[h, pl.ds(pl.multiple_of(dev * OR, OR), OR), chunk(g)]

    def from_own(self, h, g, k):
        ref = self.place(h, 2 * self.q + self.c, g)
        return self.remote(ref, ref, self.s3s.at[h, g, k], self.s3r.at[h, g, k], self.peers[k])

    def own_pair(self, h):
        ref = self.n.at[h, pl.ds(pl.multiple_of((2 * self.q + self.c) * OR, OR), OR)]
        return self.remote(ref, ref, self.s5s.at[h], self.s5r.at[h], self.partner)

    def pass_on(self, h, g, k):
        ref = self.place(h, self.peers[k], g)
        return self.remote(ref, ref, self.s4s.at[h, g, k], self.s4r.at[h, g, k], self.partner)

    def scatter(self, h, lhs, rhs, before=None, after=None):
        c, q, chips, part = self.c, self.q, self.chips, self.part

        def pair(g, carry):
            cols = chunk(g)
            self.to_partner(h, g).wait_recv()
            for k in (2, 0, 1):
                s = part[h, chips[k], c, :, cols].astype(F32) + self.recv1[h, chips[k], :, cols].astype(F32)
                part[h, chips[k], c, :, cols] = s.astype(BF)
                self.to_owner(h, g, k).start()
            self.own[h, :, cols] = part[h, q, c, :, cols].astype(F32) + self.recv1[h, q, :, cols].astype(F32)
            return carry

        def step(g, carry):
            if before is not None:
                before(g)
            def tile(p, carry):
                cols = piece(g, p)
                out = jnp.dot(lhs(), rhs(cols), preferred_element_type=F32)
                part[h, :, :, :, cols] = out.astype(BF).reshape(4, 2, OR, SLAB)
                return carry

            unrolled(PER, tile)
            if after is not None:
                after(g)
            self.to_partner(h, g).start()
            return carry

        lax.fori_loop(0, G, step, 0)
        lax.fori_loop(0, G, pair, 0)

    def finish(self, h, bias_ref, layer, scale):
        def final(g, carry):
            cols = chunk(g)
            tot = self.own[h, :, cols]
            for k in range(3):
                self.to_owner(h, g, k).wait_recv()
                tot = tot + self.recv2[h, k, :, cols].astype(F32)
            bias = bias_ref[:, cols].astype(F32)[layer:layer + 1]
            self.xown[h, :, cols] = (self.xown[h, :, cols].astype(F32) + tot.astype(BF).astype(F32) + bias).astype(BF)
            return carry

        lax.fori_loop(0, G, final, 0)

        rows = self.xown[h]
        self.n[h, pl.ds(pl.multiple_of((2 * self.q + self.c) * OR, OR), OR), :] = rows if scale is None else rms(rows, scale)

        self.own_pair(h).start()

        def send(i, carry):
            for k in (2, 0, 1):
                self.from_own(h, order(h, i), k).start()
            return carry

        lax.fori_loop(0, G, send, 0)

        def sent(g, carry):
            self.to_partner(h, g).wait_send()
            for k in range(3):
                self.to_owner(h, g, k).wait_send()
            return carry

        lax.fori_loop(0, G, sent, 0)

    def gathered(self, h, use):
        def forward(i, carry):
            g = order(h, i)
            for k in range(3):
                self.from_own(h, g, k).wait_recv()
                self.pass_on(h, g, k).start()
            return carry

        def step(i, carry):
            @pl.when(i < G)
            def _():
                forward(i, 0)

            @pl.when(i > 0)
            def _():
                g = order(h, i - 1)

                @pl.when(i == 1)
                def _():
                    self.own_pair(h).wait_recv()

                for k in range(3):
                    self.pass_on(h, g, k).wait_recv()
                use(i - 1, g)

            return carry

        lax.fori_loop(0, G + 1, step, 0)
        self.own_pair(h).wait_send()

        def sent(g, carry):
            for k in range(3):
                self.from_own(h, g, k).wait_send()
                self.pass_on(h, g, k).wait_send()
            return carry

        lax.fori_loop(0, G, sent, 0)


def order(h, i):
    return lax.rem(i + (G // 2) * h, G)


LINK_SCRATCH = [
    pltpu.VMEM((2, 4, 2, OR, D), BF), pltpu.VMEM((2, 4, OR, D), BF), pltpu.VMEM((2, 3, OR, D), BF),
    pltpu.VMEM((2, OR, D), F32), pltpu.VMEM((2, HB, D), BF), pltpu.VMEM((2, OR, D), BF),
    DMA((2, G)), DMA((2, G)), DMA((2, G, 3)), DMA((2, G, 3)), DMA((2, G, 3)), DMA((2, G, 3)), DMA((2, G, 3)), DMA((2, G, 3)), DMA((2,)), DMA((2,)),
]
NLINK = len(LINK_SCRATCH)

SLOTS = 5
LOADS = 12


class Slabs:
    def __init__(self, groups, wu):
        self.groups, self.wu = groups, wu

    def start(self, load):
        for j, group in enumerate(self.groups):
            @pl.when((load >= LOADS * j) & (load < LOADS * (j + 1)))
            def _():
                for cp in group(load - LOADS * j, load):
                    cp.start()

    def begin(self):
        def body(load, carry):
            self.start(load)
            return carry

        lax.fori_loop(0, SLOTS, body, 0)

    def use(self, h, j, i, body):
        load = LOADS * j + 4 * h + i

        @pl.when(i >= 4 * h)
        def _():
            for cp in self.groups[j](load - LOADS * j, load):
                cp.wait()

        body(lax.rem(load, SLOTS))

        @pl.when((i < 4) | (h == 1))
        def _():
            self.start(load + SLOTS)


def slab_rows(k):
    return pl.ds(pl.multiple_of(lax.rem(k, 8) * SLAB, SLAB), SLAB)


def mlp_slabs(layer, w1, w2, wu, sems):
    def group(k, load):
        s = lax.rem(load, SLOTS)
        return [pltpu.make_async_copy(w1.at[layer, slab_rows(k), :], wu.at[s, 0], sems.at[s, 0]), pltpu.make_async_copy(w2.at[layer, slab_rows(k), :], wu.at[s, 1], sems.at[s, 1])]

    return group


def qkv_slabs(wq, wk, wv, wu, sems):
    def group(k, load):
        s = lax.rem(load, SLOTS)
        return [pltpu.make_async_copy(w.at[slab_rows(k), :], wu.at[s, 0, :, lo:hi], sems.at[s, j]) for j, (w, lo, hi) in enumerate(((wq, 0, 512), (wk, 512, 640), (wv, 640, 768)))]

    return group


def wide(src, dst, sems, g):
    return pltpu.make_async_copy(src.at[:, chunk(g)], dst.at[:, chunk(g)], sems.at[g])


def mlp_up(net, h, slabs, j, acc, h_s, b1_ref, b2_ref, layer):
    acc[...] = jnp.zeros_like(acc)

    def use(i, g):
        def one(e, carry):
            def body(slot):
                ng = net.n[h, :, piece(g, e)]
                for half in range(2):
                    for lo in range(0, FC, 512):
                        acc[half, :, lo:lo + 512] += jnp.dot(ng, slabs.wu[slot, half, :, lo:lo + 512], preferred_element_type=F32)

            slabs.use(h, j, PER * i + e, body)
            return carry

        unrolled(PER, one)

    net.gathered(h, use)
    b1 = b1_ref[...].astype(F32)[layer:layer + 1]
    b2 = b2_ref[...].astype(F32)[layer:layer + 1]
    for lo in range(0, FC, 256):
        lanes = slice(lo, lo + 256)
        h_s[:, lanes] = (jax.nn.gelu(acc[0, :, lanes] + b1[:, lanes], approximate=True) * (acc[1, :, lanes] + b2[:, lanes])).astype(BF)


def mlp(net, slabs, j, acc, h_s, b1_ref, b2_ref, wd, wdb, ds, layer, last):
    for h in range(2):
        mlp_up(net, h, slabs, j, acc, h_s, b1_ref, b2_ref, layer)

        def before(g):
            if h == 0:
                wide(wd.at[layer], wdb, ds, g).wait()

        def after(g):
            if h == 1 and not last:
                wide(wd.at[layer + 1], wdb, ds, g).start()

        net.scatter(h, lambda: h_s[...], lambda cols: wdb[:, cols], before, after)


def rope(v, keep, turn):
    lane = lax.broadcasted_iota(jnp.int32, v.shape, 1)
    return v * keep + jnp.where(lane < 32, pltpu.roll(v, 96, 1), pltpu.roll(v, 32, 1)) * turn


def kernel_a(x_ref, sc_ref, wx, wy, conv, lru, wa_ref, wi_ref, bx_ref, by_ref, cw_ref, cb_ref, ba_ref, bi_ref, sp_ref, tok_ref, wout, rb_ref, w1, b1_ref, w2, b2_ref, wd, mb_ref, wq, wk, wv, keep_ref, turn_ref,
             q_ref, k_ref, v_ref, xo_ref, conv_out, lru_out, *scratch):
    net = Links(*scratch[:NLINK])
    wu, wdb, wxb, wob, acc, accr, h_s, conv_s, xb_s, lru_s, ht_s, prow, pcol, us, ds, xs, os, ss, ts, ls = scratch[NLINK:]
    scale = lambda l, j: sc_ref[...].astype(F32)[l, j:j + 1, :]
    rec_in = lambda l, g: [pltpu.make_async_copy(w.at[l, :, chunk(g)], wxb.at[j, :, chunk(g)], xs.at[j, g]) for j, w in enumerate((wx, wy))]
    state_in = lambda l: [pltpu.make_async_copy(conv.at[l], conv_s, ss.at[0]), pltpu.make_async_copy(lru.at[l], lru_s, ss.at[1])]
    state_out = lambda l: [pltpu.make_async_copy(conv_s.at[1:3], conv_out.at[l, 0:2], ts.at[0]), pltpu.make_async_copy(xb_s, conv_out.at[l, 2], ts.at[1]), pltpu.make_async_copy(lru_s, lru_out.at[l], ts.at[2])]
    slabs = Slabs([mlp_slabs(0, w1, w2, wu, us), mlp_slabs(1, w1, w2, wu, us), qkv_slabs(wq, wk, wv, wu, us)], wu)

    load_x = pltpu.make_async_copy(x_ref, net.part, ls)
    load_x.start()

    def load_rec(l):
        for g in range(G):
            for cp in rec_in(l, g):
                cp.start()

    load_rec(0)
    for cp in state_in(0):
        cp.start()
    for g in range(G):
        wide(wout.at[0], wob, os, g).start()
    net.enter()
    load_x.wait()
    for h in range(2):
        for chip in range(4):
            net.n[h, 2 * OR * chip:2 * OR * (chip + 1), :] = rms(net.part[h, chip].reshape(2 * OR, D), scale(0, 0))
        net.xown[h] = net.part[h, net.q, net.c]
    tok = tok_ref[...]

    for layer in range(2):
        row = lambda ref: ref[...].astype(F32)[layer:layer + 1]
        cw = cw_ref[...].astype(F32)
        params = [row(bx_ref), row(by_ref)] + [cw[layer, j:j + 1, :] for j in range(4)] + [row(cb_ref), row(ba_ref), row(bi_ref), row(sp_ref)]
        for j, p in enumerate(params):
            prow[j:j + 1, 0:LC] = p
        pcol[...] = prow[...].T
        accr[...] = jnp.zeros_like(accr)

        def use_both(g, carry):
            for cp in rec_in(layer, g):
                cp.wait()
            ng = net.n[:, :, chunk(g)].reshape(B, GC)
            for half in range(2):
                r = lax.dot_general(wxb[half, :, chunk(g)], ng, NT, preferred_element_type=F32)
                accr[0, half] += r[:, :HB]
                accr[1, half] += r[:, HB:]
            return carry

        if layer == 0:
            lax.fori_loop(0, G, use_both, 0)
            slabs.begin()
            for g in range(G):
                wide(wd.at[0], wdb, ds, g).start()

        for h in range(2):
            lanes = slice(HB * h, HB * (h + 1))

            def use(i, g):
                if h == 0:
                    for cp in rec_in(layer, g):
                        cp.wait()
                for half in range(2):
                    accr[h, half] += lax.dot_general(wxb[half, :, chunk(g)], net.n[h, :, chunk(g)], NT, preferred_element_type=F32)

            if layer == 1:
                net.gathered(h, use)
            if h == 0:
                for cp in state_in(layer):
                    cp.wait()
            tk = tok[:, lanes]
            fresh = tk == 0
            for b in range(4):
                rows = slice(176 * b, 176 * b + 176)
                pc = pcol[rows, :]
                col = lambda k: pc[:, k:k + 1]
                xb = (accr[h, 0, rows, :] + col(0)).astype(BF)
                yb = jax.nn.gelu(accr[h, 1, rows, :] + col(1), approximate=True)
                xb_s[rows, lanes] = xb
                hist = jnp.zeros((176, HB), F32)
                for j in range(3):
                    hist = hist + jnp.where(tk >= 3 - j, conv_s[j, rows, lanes].astype(F32), 0.0) * col(5 - j)
                xc = (col(6) + col(2) * xb.astype(F32) + hist).astype(BF)
                rg = jax.nn.sigmoid(lax.dot_general(wa_ref[layer, b], xc, TN, preferred_element_type=F32) + col(7))
                ig = jax.nn.sigmoid(lax.dot_general(wi_ref[layer, b], xc, TN, preferred_element_type=F32) + col(8))
                a = jnp.exp(rg * col(9))
                sc = jnp.sqrt(1.0 - a * a)
                a = jnp.where(fresh, 0.0, a)
                sc = jnp.where(fresh, 1.0, sc)
                hn = a * lru_s[rows, lanes] + sc * ig * xc.astype(F32)
                lru_s[rows, lanes] = hn
                ht_s[rows, :] = (hn * yb).astype(BF)
            ht_s[LC:, :] = jnp.zeros((64, HB), BF)
            h_s[:, :LC + 64] = ht_s[...].T

            def before(g):
                if h == 0:
                    wide(wout.at[layer], wob, os, g).wait()

            net.scatter(h, lambda: h_s[:, :LC], lambda cols: wob[:, cols], before)
        for cp in state_out(layer):
            cp.start()
        if layer == 0:
            load_rec(1)
            for g in range(G):
                wide(wout.at[1], wob, os, g).start()
        for h in range(2):
            net.finish(h, rb_ref, layer, scale(layer, 1))
        for cp in state_out(layer):
            cp.wait()
        if layer == 0:
            for cp in state_in(1):
                cp.start()
        mlp(net, slabs, layer, acc, h_s, b1_ref, b2_ref, wd, wdb, ds, layer, layer == 1)
        for h in range(2):
            net.finish(h, mb_ref, layer, scale(layer + 1, 0))

    xo_ref[...] = net.xown[...]
    for h in range(2):
        acc[...] = jnp.zeros_like(acc)

        def use_q(i, g):
            def one(e, carry):
                def body(slot):
                    acc[0, :, 0:768] += jnp.dot(net.n[h, :, piece(g, e)], wu[slot, 0, :, 0:768], preferred_element_type=F32)

                slabs.use(h, 2, PER * i + e, body)
                return carry

            unrolled(PER, one)

        net.gathered(h, use_q)
        keep, turn = keep_ref[h], turn_ref[h]
        for b in range(4):
            q_ref[h, :, HD * b:HD * (b + 1)] = rope(acc[0, :, HD * b:HD * (b + 1)], keep, turn).astype(BF)
        k_ref[h] = rope(acc[0, :, 512:640], keep, turn).astype(BF)
        v_ref[h] = acc[0, :, 640:768].astype(BF)


def first_layers(x, scale, wxt, wyt, convt, lrut, wa, wi, bx, by, cw, cb, ba, bi, sp, tok, wout, rb, w1, b1, w2, b2, wd, mb, wq, wk, wv, keep, turn):
    return pl.pallas_call(
        kernel_a,
        name='first_layers',
        out_shape=(jax.ShapeDtypeStruct((2, HB, 4 * HD), BF), jax.ShapeDtypeStruct((2, HB, HD), BF), jax.ShapeDtypeStruct((2, HB, HD), BF), jax.ShapeDtypeStruct((2, OR, D), BF),
                   jax.ShapeDtypeStruct(convt.shape, BF), jax.ShapeDtypeStruct(lrut.shape, F32)),
        in_specs=[ANY, VM, ANY, ANY, ANY, ANY, VM, VM] + [VM] * 7 + [VM, ANY, VM, ANY, VM, ANY, VM, ANY, VM, ANY, ANY, ANY, VM, VM],
        out_specs=(VM, VM, VM, VM, ANY, ANY),
        scratch_shapes=LINK_SCRATCH + [
            pltpu.VMEM((SLOTS, 2, SLAB, FC), BF), pltpu.VMEM((FC, D), BF), pltpu.VMEM((2, LC, D), BF), pltpu.VMEM((LC, D), BF),
            pltpu.VMEM((2, HB, FC), F32), pltpu.VMEM((2, 2, LC, HB), F32), pltpu.VMEM((HB, FC), BF), pltpu.VMEM((3, LC, B), BF), pltpu.VMEM((LC, B), BF), pltpu.VMEM((LC, B), F32),
            pltpu.VMEM((LC + 64, HB), BF), pltpu.VMEM((16, LC + 64), F32), pltpu.VMEM((LC + 64, 16), F32),
            DMA((SLOTS, 3)), DMA((G,)), DMA((2, G)), DMA((G,)), DMA((2,)), DMA((3,)), DMA,
        ],
        compiler_params=pltpu.CompilerParams(collective_id=0, has_side_effects=True, vmem_limit_bytes=67043328),
        cost_estimate=pl.CostEstimate(flops=30 * 10**9, bytes_accessed=400 * 10**6, transcendentals=0),
    )(x.reshape(2, 4, 2, OR, D), scale, wxt, wyt, convt, lrut, wa, wi, bx, by, cw, cb, ba, bi, sp, tok, wout, rb, w1, b1, w2, b2, wd, mb, wq, wk, wv, keep.reshape(2, HB, HD), turn.reshape(2, HB, HD))


def kernel_b(o_ref, x_ref, wo, bo_ref, sc_ref, w1, b1_ref, w2, b2_ref, wd, mb_ref, out_ref, *scratch):
    net = Links(*scratch[:NLINK])
    wu, wdb, wob, acc, h_s, us, ds, os, ls = scratch[NLINK:]
    for g in range(G):
        wide(wo, wob, os, g).start()
    slabs = Slabs([mlp_slabs(2, w1, w2, wu, us)], wu)
    slabs.begin()
    for g in range(G):
        wide(wd.at[2], wdb, ds, g).start()
    net.enter()
    net.xown[...] = x_ref[...]
    for h in range(2):
        def before(g):
            if h == 0:
                wide(wo, wob, os, g).wait()

        net.scatter(h, lambda: o_ref[h], lambda cols: wob[:, cols], before)
    for h in range(2):
        net.finish(h, bo_ref, 0, sc_ref[...].astype(F32)[2, 1:2, :])
    mlp(net, slabs, 0, acc, h_s, b1_ref, b2_ref, wd, wdb, ds, 2, True)
    for h in range(2):
        net.finish(h, mb_ref, 2, None)
    store = lambda h, g: pltpu.make_async_copy(net.n.at[h, :, chunk(g)], out_ref.at[h, :, chunk(g)], ls.at[h, g])
    for h in range(2):
        net.gathered(h, lambda i, g: store(h, g).start())
    for h in range(2):
        for g in range(G):
            store(h, g).wait()


def last_layer(o, x_own, wo, bo, scale, w1, b1, w2, b2, wd, mb):
    out = pl.pallas_call(
        kernel_b,
        name='last_layer',
        out_shape=jax.ShapeDtypeStruct((2, HB, D), BF),
        in_specs=[VM, VM, ANY, VM, VM, ANY, VM, ANY, VM, ANY, VM],
        out_specs=ANY,
        scratch_shapes=LINK_SCRATCH + [
            pltpu.VMEM((SLOTS, 2, SLAB, FC), BF), pltpu.VMEM((FC, D), BF), pltpu.VMEM((4 * HD, D), BF),
            pltpu.VMEM((2, HB, FC), F32), pltpu.VMEM((HB, FC), BF),
            DMA((SLOTS, 3)), DMA((G,)), DMA((G,)), DMA((2, G)),
        ],
        compiler_params=pltpu.CompilerParams(collective_id=1, has_side_effects=True, vmem_limit_bytes=67043328),
        cost_estimate=pl.CostEstimate(flops=12 * 10**9, bytes_accessed=200 * 10**6, transcendentals=0),
    )(o.reshape(2, HB, 4 * HD), x_own, wo, bo, scale, w1, b1, w2, b2, wd, mb)
    return out.reshape(B, D)


RA = 8
NB = 6
STEPS = B // RA


def attn_kernel(tok_ref, q_ref, kn_ref, vn_ref, slot_ref, k_ref, v_ref, o_ref, ko_ref, vo_ref, so_ref, kb, vb, s_s, q_s, o_s, isem, osem):
    lane = lax.broadcasted_iota(jnp.int32, (1, W), 1)
    sub = lax.broadcasted_iota(jnp.int32, (16, HD), 0)

    def copies(step, out):
        b = lax.rem(step, NB)
        rows = pl.ds(pl.multiple_of(step * RA, RA), RA)
        if out:
            return [pltpu.make_async_copy(kb.at[b], ko_ref.at[rows], osem.at[0, b]), pltpu.make_async_copy(vb.at[b], vo_ref.at[rows], osem.at[1, b])]
        return [pltpu.make_async_copy(k_ref.at[rows], kb.at[b], isem.at[0, b]), pltpu.make_async_copy(v_ref.at[rows], vb.at[b], isem.at[1, b])]

    def start(step):
        for cp in copies(step, False):
            cp.start()

    lax.fori_loop(0, NB - 2, lambda step, c: (start(step), c)[1], 0)

    def step_fn(i, carry):
        b = lax.rem(i, NB)
        rows = pl.ds(pl.multiple_of(i * RA, RA), RA)
        ahead = i + NB - 2

        @pl.when(ahead < STEPS)
        def _():
            @pl.when(ahead >= NB)
            def _():
                for cp in copies(ahead - NB, True):
                    cp.wait()
            start(ahead)

        for cp in copies(i, False):
            cp.wait()
        kn = kn_ref[rows, :].astype(F32)
        vn = vn_ref[rows, :].astype(F32)
        for h in range(4):
            q_s[pl.ds(h, RA, stride=4), :] = q_ref[rows, 128 * h:128 * h + 128].astype(F32)
        slots = slot_ref[rows, :]
        new_rows = []
        for r in range(RA):
            tp = tok_ref[i * RA + r]
            slot = lax.rem(tp, W)
            base = pl.multiple_of((slot // 16) * 16, 16)
            hit = sub == (slot - base)
            spot = pl.ds(base, 16)
            kb[b, r, spot, :] = jnp.where(hit, kn[r:r + 1], kb[b, r, spot, :].astype(F32)).astype(BF)
            vb[b, r, spot, :] = jnp.where(hit, vn[r:r + 1], vb[b, r, spot, :].astype(F32)).astype(BF)
            sn = jnp.where(lane == slot, tp, slots[r:r + 1])
            new_rows.append((tp, sn))
        for r in range(RA):
            tp, sn = new_rows[r]
            so_ref[pl.ds(i * RA + r, 1), :] = sn
            age = tp - sn
            valid = (sn >= 0) & (age >= 0) & (age < W)
            s = lax.dot_general(q_s[4 * r:4 * r + 4, :].astype(BF), kb[b, r], NT, preferred_element_type=F32) * (HD ** -0.5)
            s_s[4 * r:4 * r + 4, :] = jnp.where(valid, s, -jnp.inf)
        s = s_s[...]
        e = jnp.exp(s - jnp.max(s, axis=-1, keepdims=True))
        s_s[...] = e / jnp.sum(e, axis=-1, keepdims=True)
        for r in range(RA):
            o_s[4 * r:4 * r + 4, :] = jnp.dot(s_s[4 * r:4 * r + 4, :].astype(BF), vb[b, r], preferred_element_type=F32)
        for h in range(4):
            o_ref[rows, 128 * h:128 * h + 128] = o_s[pl.ds(h, RA, stride=4), :].astype(BF)
        for cp in copies(i, True):
            cp.start()
        return carry

    lax.fori_loop(0, STEPS, step_fn, 0)
    for step in range(STEPS - NB, STEPS):
        for cp in copies(step, True):
            cp.wait()


def attend(tok, q, kn, vn, slot_pos, kc, vc):
    return pl.pallas_call(
        attn_kernel,
        name='attend',
        in_specs=[pl.BlockSpec(memory_space=pltpu.SMEM), VM, VM, VM, VM, ANY, ANY],
        out_specs=(VM, ANY, ANY, VM),
        out_shape=(jax.ShapeDtypeStruct((B, 4 * HD), BF), jax.ShapeDtypeStruct(kc.shape, BF), jax.ShapeDtypeStruct(vc.shape, BF), jax.ShapeDtypeStruct(slot_pos.shape, jnp.int32)),
        scratch_shapes=[pltpu.VMEM((NB, RA, W, HD), BF), pltpu.VMEM((NB, RA, W, HD), BF), pltpu.VMEM((4 * RA, W), F32), pltpu.VMEM((4 * RA, HD), F32), pltpu.VMEM((4 * RA, HD), F32),
                        pltpu.SemaphoreType.DMA((2, NB)), pltpu.SemaphoreType.DMA((2, NB))],
        cost_estimate=pl.CostEstimate(flops=4 * B * 4 * W * HD, bytes_accessed=8 * B * W * HD, transcendentals=0),
    )(tok, q, kn, vn, slot_pos, kc, vc)


def rope_tables(tok_pos):
    quarter = HD // 4
    lane = lax.broadcasted_iota(jnp.int32, (1, HD), 1)
    inv_freq = ROPE_BASE ** (-(lane % quarter).astype(F32) / quarter)
    angles = tok_pos.astype(F32)[:, None] * inv_freq
    cos, sin = jnp.cos(angles), jnp.sin(angles)
    return jnp.where(lane < 2 * quarter, cos, 1.0), jnp.where(lane < quarter, -sin, jnp.where(lane < 2 * quarter, sin, 0.0))


def io_specs():
    in_specs = (P('dp', None), P('dp'), P(None, 'dp', None, 'tp'), P(None, 'dp', 'tp'), P('dp', None, None), P('dp', None, None), P('dp', None),
                P(), P(None, None, 'tp'), P(None, 'tp'), P(None, None, 'tp'), P(None, 'tp'), P(None, None, 'tp'), P(None, 'tp'),
                P(None, 'tp', None, None), P(None, 'tp'), P(None, 'tp', None, None), P(None, 'tp'), P(None, 'tp'), P(None, 'tp', None), P(),
                P(None, 'tp'), P(), P(), P('tp', None), P(),
                P(None, None, 'tp'), P(None, 'tp'), P(None, None, 'tp'), P(None, 'tp'), P(None, 'tp', None), P())
    out_specs = (P('dp', None), P(None, 'dp', None, 'tp'), P(None, 'dp', 'tp'), P('dp', None, None), P('dp', None, None), P('dp', None))
    return in_specs, out_specs


def solution(mesh):
    in_specs, out_specs = io_specs()

    def local_step(x_in, tok_pos, conv_state, lru_state, k_cache, v_cache, slot_pos, norm_scale, rec_wx, rec_bx, rec_wy, rec_by, conv_w, conv_b, gate_wa, gate_ba, gate_wi, gate_bi, a_param, rec_wout, rec_bout, attn_wq, attn_wk, attn_wv, attn_wo, attn_bo, mlp_w1, mlp_b1, mlp_w2, mlp_b2, mlp_wd, mlp_bd):
        wxt = jnp.swapaxes(rec_wx, 1, 2)
        wyt = jnp.swapaxes(rec_wy, 1, 2)
        convt = jnp.transpose(conv_state, (0, 2, 3, 1))
        lrut = jnp.swapaxes(lru_state, 1, 2)
        tok_row = tok_pos[None, :]
        tab = rope_tables(tok_pos)

        q, kn, vn, x_own, convs, lrus = first_layers(x_in, norm_scale, wxt, wyt, convt, lrut, gate_wa, gate_wi, rec_bx, rec_by, conv_w, conv_b, gate_ba, gate_bi, -8.0 * jax.nn.softplus(a_param), tok_row, rec_wout, rec_bout, mlp_w1, mlp_b1, mlp_w2, mlp_b2, mlp_wd, mlp_bd, attn_wq, attn_wk, attn_wv, *tab)
        o, k_next, v_next, slot_next = attend(tok_pos, q.reshape(B, 4 * HD), kn.reshape(B, HD), vn.reshape(B, HD), slot_pos, k_cache, v_cache)
        x = last_layer(o, x_own, attn_wo, attn_bo[None, :], norm_scale, mlp_w1, mlp_b1, mlp_w2, mlp_b2, mlp_wd, mlp_bd)
        conv_out = jnp.transpose(convs, (0, 3, 1, 2))
        lru_out = jnp.swapaxes(lrus, 1, 2)
        return (x, conv_out, lru_out, k_next, v_next, slot_next)

    return jax.shard_map(local_step, mesh=mesh, in_specs=in_specs, out_specs=out_specs, check_vma=False)
```
